32 devices in a mesh: dp: 1 (over z), tp: 4 (over y), sp: 8 (over x, core).
Axes of the slice: x: 4, y: 4, z: 1, core: 2. Of those that a mesh axis runs over, the one named last changes fastest.
The devices are a block of a 4x4x8 slice.
Arguments:
- x: bfloat16 [4096, 3584], P(('dp', 'sp'))
- pos: int32 [4096], P(('dp', 'sp'))
- k_hist: bfloat16 [2, 8192, 4, 128], P(None, ('dp', 'sp'), 'tp')
- v_hist: bfloat16 [2, 8192, 4, 128], P(None, ('dp', 'sp'), 'tp')
- wq: bfloat16 [2, 3584, 3584], P(None, None, 'tp')
- wk: bfloat16 [2, 3584, 512], P(None, None, 'tp')
- wv: bfloat16 [2, 3584, 512], P(None, None, 'tp')
- wo: bfloat16 [2, 3584, 3584], P(None, 'tp')
- wg: bfloat16 [2, 3584, 18944], P(None, None, 'tp')
- wu: bfloat16 [2, 3584, 18944], P(None, None, 'tp')
- wd: bfloat16 [2, 18944, 3584], P(None, 'tp')
- g1: bfloat16 [2, 3584], replicated
- g2: bfloat16 [2, 3584], replicated
Outputs:
- output 1: bfloat16 [4096, 3584], P(('dp', 'sp'))
- output 2: bfloat16 [2, 4096, 4, 128], P(None, ('dp', 'sp'), 'tp')
- output 3: bfloat16 [2, 4096, 4, 128], P(None, ('dp', 'sp'), 'tp')
All inputs are finite; a program needn't handle non-finite values.
Results may differ from the reference program's by a relative error of at most 0.02.
Values are sent between devices in bfloat16 or wider.
A program may use at most 768 MiB of HBM per device.

```python
import jax
import jax.numpy as jnp
from jax import lax

D = 3584
HEADS = 28
KV_HEADS = 4
HEAD = 128
FF = 18944
S = 4096
HIST = 8192
LAYERS = 2
QBLK = 32
EPS = 1e-5
ROPE_THETA = 500000.0


def setup_inputs(seed: int = 0, part: int = 0) -> dict:
    key = jax.random.PRNGKey(seed)
    ks = jax.random.split(key, 9)
    kp = jax.random.split(jax.random.fold_in(key, part), 4)
    f32 = jnp.float32

    def w(k, shape, fan_in, gain=1.0):
        return (jax.random.normal(k, shape, f32) * (gain * fan_in ** -0.5)).astype(jnp.bfloat16)

    off = jax.random.randint(kp[1], (), 0, 1024)
    kvshape = (LAYERS, HIST, KV_HEADS, HEAD)
    return {
        'x': jax.random.normal(kp[0], (S, D), f32).astype(jnp.bfloat16),
        'pos': (HIST + off + jnp.arange(S)).astype(jnp.int32),
        'k_hist': jax.random.normal(kp[2], kvshape, f32).astype(jnp.bfloat16),
        'v_hist': jax.random.normal(kp[3], kvshape, f32).astype(jnp.bfloat16),
        'wq': w(ks[0], (LAYERS, D, HEADS * HEAD), D, 3.0),
        'wk': w(ks[1], (LAYERS, D, KV_HEADS * HEAD), D),
        'wv': w(ks[2], (LAYERS, D, KV_HEADS * HEAD), D),
        'wo': w(ks[3], (LAYERS, HEADS * HEAD, D), HEADS * HEAD),
        'wg': w(ks[4], (LAYERS, D, FF), D),
        'wu': w(ks[5], (LAYERS, D, FF), D),
        'wd': w(ks[6], (LAYERS, FF, D), FF),
        'g1': (1.0 + 0.2 * jax.random.normal(ks[7], (LAYERS, D), f32)).astype(jnp.bfloat16),
        'g2': (1.0 + 0.2 * jax.random.normal(ks[8], (LAYERS, D), f32)).astype(jnp.bfloat16),
    }


def rmsnorm(x, g):
    xf = x.astype(jnp.float32)
    r = lax.rsqrt(jnp.mean(xf * xf, axis=-1, keepdims=True) + EPS)
    return (xf * r * g.astype(jnp.float32)).astype(jnp.bfloat16)


def rope(t, pos):
    half = t.shape[-1] // 2
    inv = ROPE_THETA ** (-(jnp.arange(half, dtype=jnp.float32) * (2.0 / t.shape[-1])))
    ang = pos.astype(jnp.float32)[..., None] * inv
    c = jnp.cos(ang)[..., None, :]
    s = jnp.sin(ang)[..., None, :]
    tf = t.astype(jnp.float32)
    t1 = tf[..., :half]
    t2 = tf[..., half:]
    return jnp.concatenate([t1 * c - t2 * s, t2 * c + t1 * s], axis=-1).astype(jnp.bfloat16)


def attention(q, k, v):
    g = HEADS // KV_HEADS
    kf = k.astype(jnp.float32)
    vf = v.astype(jnp.float32)
    qb = q.reshape(S // QBLK, QBLK, KV_HEADS, g, HEAD)
    kidx = jnp.arange(HIST + S)

    def blk(args):
        i, qq = args
        s = jnp.einsum('qkgd,tkd->qkgt', qq.astype(jnp.float32), kf) * HEAD ** -0.5
        qidx = HIST + i * QBLK + jnp.arange(QBLK)
        mask = (kidx[None, :] <= qidx[:, None])[:, None, None, :]
        s = jnp.where(mask, s, -jnp.inf)
        p = jax.nn.softmax(s, axis=-1).astype(jnp.bfloat16)
        o = jnp.einsum('qkgt,tkd->qkgd', p.astype(jnp.float32), vf)
        return o.astype(jnp.bfloat16)

    o = lax.map(blk, (jnp.arange(S // QBLK), qb))
    return o.reshape(S, HEADS * HEAD)


def reference(x, pos, k_hist, v_hist, wq, wk, wv, wo, wg, wu, wd, g1, g2):
    def layer(x, w):
        kh, vh, wq_, wk_, wv_, wo_, wg_, wu_, wd_, g1_, g2_ = w
        h = rmsnorm(x, g1_)
        q = jnp.dot(h, wq_, preferred_element_type=jnp.float32).astype(jnp.bfloat16).reshape(S, HEADS, HEAD)
        k = jnp.dot(h, wk_, preferred_element_type=jnp.float32).astype(jnp.bfloat16).reshape(S, KV_HEADS, HEAD)
        v = jnp.dot(h, wv_, preferred_element_type=jnp.float32).astype(jnp.bfloat16).reshape(S, KV_HEADS, HEAD)
        q = rope(q, pos)
        k = rope(k, pos)
        a = attention(q, jnp.concatenate([kh, k], axis=0), jnp.concatenate([vh, v], axis=0))
        x = x + jnp.dot(a, wo_, preferred_element_type=jnp.float32).astype(jnp.bfloat16)
        h2 = rmsnorm(x, g2_)
        ga = jnp.dot(h2, wg_, preferred_element_type=jnp.float32).astype(jnp.bfloat16)
        up = jnp.dot(h2, wu_, preferred_element_type=jnp.float32).astype(jnp.bfloat16)
        u = (jax.nn.silu(ga.astype(jnp.float32)) * up.astype(jnp.float32)).astype(jnp.bfloat16)
        x = x + jnp.dot(u, wd_, preferred_element_type=jnp.float32).astype(jnp.bfloat16)
        return x, (k, v)

    x, (kn, vn) = lax.scan(layer, x, (k_hist, v_hist, wq, wk, wv, wo, wg, wu, wd, g1, g2))
    return x, kn, vn
```

```python
import functools

import jax
import jax.numpy as jnp
from jax import lax
from jax.experimental import pallas as pl
from jax.experimental.pallas import tpu as pltpu
from jax.sharding import PartitionSpec as P

EPS = 1e-5
ROPE_THETA = 500000.0
LOG2E = 1.4426950408889634


def rmsnorm(x, g):
    xf = x.astype(jnp.float32)
    r = lax.rsqrt(jnp.mean(xf * xf, axis=-1, keepdims=True) + EPS)
    return (xf * r * g.astype(jnp.float32)).astype(jnp.bfloat16)


def rope(t, pos):
    half = t.shape[-1] // 2
    inv = ROPE_THETA ** (-(jnp.arange(half, dtype=jnp.float32) * (2.0 / t.shape[-1])))
    ang = pos.astype(jnp.float32)[..., None] * inv
    c = jnp.cos(ang)[..., None, :]
    s = jnp.sin(ang)[..., None, :]
    tf = t.astype(jnp.float32)
    t1 = tf[..., :half]
    t2 = tf[..., half:]
    return jnp.concatenate([t1 * c - t2 * s, t2 * c + t1 * s], axis=-1).astype(jnp.bfloat16)


def mm(a, b):
    return jnp.dot(a, b, preferred_element_type=jnp.float32)


def attn_kernel(sp, layer, q_ref, hist_ref, new_ref, o_ref, hkv, nkv, m_ref, l_ref, acc_ref, hsem, nsem):
    n, w = q_ref.shape
    dh = hkv.shape[-1]
    heads = w // dh
    hc = hkv.shape[2]
    nc = nkv.shape[2]
    rows_t = min(256, n)
    nt = n // rows_t
    c = dh ** -0.5 * LOG2E
    me = lax.axis_index("sp")
    for b in range(sp):
        for j in range(2):
            pltpu.make_async_copy(hist_ref.at[b, 2 * layer + j], hkv.at[b, j], hsem.at[b, j]).start()
    for b in range(sp):
        pltpu.make_async_copy(new_ref.at[b], nkv.at[b], nsem.at[b]).start()
    m_ref[...] = jnp.full(m_ref.shape, -1e30, jnp.float32)
    l_ref[...] = jnp.zeros_like(l_ref)
    acc_ref[...] = jnp.zeros_like(acc_ref)

    def block(t, k_of, v_of, cols, mask):
        rows = pl.ds(pl.multiple_of(t * rows_t, rows_t), rows_t)

        def qk(g):
            return lax.dot_general(q_ref[rows, g * dh:(g + 1) * dh], k_of(), (((1,), (1,)), ((), ())),
                                   preferred_element_type=jnp.float32)

        s = qk(0)
        pend = None

        def pv(g, p, alpha):
            acc_ref[g, rows, :] = acc_ref[g, rows, :] * alpha + mm(p, v_of())

        for g in range(heads):
            s_next = qk(g + 1) if g + 1 < heads else None
            if pend is not None:
                pv(*pend)
            if mask is not None:
                s = jnp.where(mask, s, -jnp.inf)
            m_old = m_ref[g, rows, :]
            m_new = jnp.maximum(m_old, jnp.max(s, axis=1, keepdims=True) * c)
            alpha = jnp.exp2(m_old - m_new)
            p = jnp.exp2(s * c - m_new[:, :1])
            ls = p[:, :dh]
            for j in range(1, cols // dh):
                ls = ls + p[:, j * dh:(j + 1) * dh]
            l_ref[g, rows, :] = l_ref[g, rows, :] * alpha + ls
            m_ref[g, rows, :] = m_new
            pend = (g, p.astype(jnp.bfloat16), alpha)
            s = s_next
        pv(*pend)

    def hist_body(i, carry):
        b = i // nt
        t = i % nt

        @pl.when(t == 0)
        def _():
            for j in range(2):
                pltpu.make_async_copy(hist_ref.at[b, 2 * layer + j], hkv.at[b, j], hsem.at[b, j]).wait()

        block(t, lambda: hkv[b, 0], lambda: hkv[b, 1], hc, None)
        return carry

    lax.fori_loop(0, sp * nt, hist_body, 0)
    for b in range(sp):
        pltpu.make_async_copy(new_ref.at[b], nkv.at[b], nsem.at[b]).wait()

    def new_body(i, carry):
        b = i // nt
        block(i % nt, lambda: nkv[b, 0], lambda: nkv[b, 1], nc, None)
        return carry

    lax.fori_loop(0, me * nt, new_body, 0)

    def diag_body(t, carry):
        r = lax.broadcasted_iota(jnp.int32, (rows_t, nc), 0) + t * rows_t
        col = lax.broadcasted_iota(jnp.int32, (rows_t, nc), 1)
        block(t, lambda: nkv[me, 0], lambda: nkv[me, 1], nc, col <= r)
        return carry

    lax.fori_loop(0, nt, diag_body, 0)
    for g in range(heads):
        l = jnp.sum(l_ref[g], axis=1, keepdims=True)
        o_ref[:, g * dh:(g + 1) * dh] = (acc_ref[g] / l).astype(jnp.bfloat16)


def attention(sp, layer, q, hist, new):
    n, w = q.shape
    _, _, hc, dh = hist.shape
    heads = w // dh
    keys = sp * hc + sp * n // 2
    return pl.pallas_call(
        functools.partial(attn_kernel, sp, layer),
        out_shape=jax.ShapeDtypeStruct((n, w), jnp.bfloat16),
        in_specs=[pl.BlockSpec(memory_space=pltpu.VMEM), pl.BlockSpec(memory_space=pl.ANY),
                  pl.BlockSpec(memory_space=pl.ANY)],
        out_specs=pl.BlockSpec(memory_space=pltpu.VMEM),
        scratch_shapes=[
            pltpu.VMEM((sp, 2, hc, dh), jnp.bfloat16),
            pltpu.VMEM((sp, 2, n, dh), jnp.bfloat16),
            pltpu.VMEM((heads, n, dh), jnp.float32),
            pltpu.VMEM((heads, n, dh), jnp.float32),
            pltpu.VMEM((heads, n, dh), jnp.float32),
            pltpu.SemaphoreType.DMA((sp, 2)),
            pltpu.SemaphoreType.DMA((sp,)),
        ],
        compiler_params=pltpu.CompilerParams(vmem_limit_bytes=40 * 2 ** 20),
        cost_estimate=pl.CostEstimate(flops=4 * n * w * keys, bytes_accessed=4 * keys * dh, transcendentals=n * heads * keys),
        name="attention",
    )(q, hist, new)


def solution(mesh):
    sp = mesh.shape['sp']
    tp = mesh.shape['tp']
    row = ('dp', 'sp')
    kv_spec = P(None, row, 'tp', None)
    col = P(None, None, 'tp')
    rowsplit = P(None, 'tp', None)

    def body(x, pos, k_hist, v_hist, wq, wk, wv, wo, wg, wu, wd, g1, g2):
        n, d = x.shape
        layers, hc, kvl, dh = k_hist.shape
        hql = wq.shape[-1] // dh
        dt = d // tp
        my = lax.axis_index('tp') * dt
        kv = jnp.stack([k_hist[:, :, 0], v_hist[:, :, 0]], axis=1).reshape(2 * layers, hc, dh)
        hist = lax.all_gather(kv, 'sp', axis=0)
        ks, vs = [], []

        def reduce_add(x, part):
            red = lax.psum_scatter(part, 'tp', scatter_dimension=1, tiled=True)
            xc = lax.dynamic_slice_in_dim(x, my, dt, axis=1) + red.astype(jnp.bfloat16)
            return lax.all_gather(xc, 'tp', axis=1, tiled=True)

        for l in range(layers):
            h = rmsnorm(x, g1[l])
            k = rope(mm(h, wk[l]).astype(jnp.bfloat16).reshape(n, kvl, dh), pos)
            v = mm(h, wv[l]).astype(jnp.bfloat16).reshape(n, kvl, dh)
            ks.append(k)
            vs.append(v)
            new = lax.all_gather(jnp.stack([k[:, 0], v[:, 0]]), 'sp', axis=0)
            q = rope(mm(h, wq[l]).astype(jnp.bfloat16).reshape(n, hql, dh), pos)
            attn = attention(sp, l, q.reshape(n, hql * dh), hist, new)
            x = reduce_add(x, mm(attn, wo[l]))
            h2 = rmsnorm(x, g2[l])
            a = mm(h2, wg[l]).astype(jnp.bfloat16)
            b = mm(h2, wu[l]).astype(jnp.bfloat16)
            u = (jax.nn.silu(a.astype(jnp.float32)) * b.astype(jnp.float32)).astype(jnp.bfloat16)
            x = reduce_add(x, mm(u, wd[l]))
        return x, jnp.stack(ks), jnp.stack(vs)

    in_specs = (P(row, None), P(row), kv_spec, kv_spec, col, col, col, rowsplit, col, col, rowsplit, P(), P())
    out_specs = (P(row, None), kv_spec, kv_spec)
    return jax.shard_map(body, mesh=mesh, in_specs=in_specs, out_specs=out_specs, check_vma=False)
```

```python
import functools

import jax
import jax.numpy as jnp
from jax import lax
from jax.experimental import pallas as pl
from jax.experimental.pallas import tpu as pltpu
from jax.sharding import PartitionSpec as P

EPS = 1e-5
ROPE_THETA = 500000.0
LOG2E = 1.4426950408889634


def rmsnorm(x, g):
    xf = x.astype(jnp.float32)
    r = lax.rsqrt(jnp.mean(xf * xf, axis=-1, keepdims=True) + EPS)
    return (xf * r * g.astype(jnp.float32)).astype(jnp.bfloat16)


def rope(t, pos):
    half = t.shape[-1] // 2
    inv = ROPE_THETA ** (-(jnp.arange(half, dtype=jnp.float32) * (2.0 / t.shape[-1])))
    ang = pos.astype(jnp.float32)[..., None] * inv
    c = jnp.cos(ang)[..., None, :]
    s = jnp.sin(ang)[..., None, :]
    tf = t.astype(jnp.float32)
    t1 = tf[..., :half]
    t2 = tf[..., half:]
    return jnp.concatenate([t1 * c - t2 * s, t2 * c + t1 * s], axis=-1).astype(jnp.bfloat16)


def mm(a, b):
    return jnp.dot(a, b, preferred_element_type=jnp.float32)


def attn_kernel(sp, layer, q_ref, hist_ref, new_ref, o_ref, hkv, nkv, m_ref, l_ref, acc_ref, hsem, nsem):
    n, w = q_ref.shape
    dh = hkv.shape[-1]
    heads = w // dh
    hc = hkv.shape[2]
    nc = nkv.shape[2]
    rows_t = min(256, n)
    nt = n // rows_t
    c = dh ** -0.5 * LOG2E
    me = lax.axis_index("sp")
    for b in range(sp):
        for j in range(2):
            pltpu.make_async_copy(hist_ref.at[b, 2 * layer + j], hkv.at[b, j], hsem.at[b, j]).start()
    for b in range(sp):
        pltpu.make_async_copy(new_ref.at[b], nkv.at[b], nsem.at[b]).start()
    m_ref[...] = jnp.full(m_ref.shape, -1e30, jnp.float32)
    l_ref[...] = jnp.zeros_like(l_ref)
    acc_ref[...] = jnp.zeros_like(acc_ref)

    def block(t, k_of, v_of, cols, mask):
        rows = pl.ds(pl.multiple_of(t * rows_t, rows_t), rows_t)

        def qk(g):
            return lax.dot_general(q_ref[rows, g * dh:(g + 1) * dh], k_of(), (((1,), (1,)), ((), ())),
                                   preferred_element_type=jnp.float32)

        s = qk(0)
        pend = None

        def pv(g, p, alpha):
            acc_ref[g, rows, :] = acc_ref[g, rows, :] * alpha + mm(p, v_of())

        for g in range(heads):
            s_next = qk(g + 1) if g + 1 < heads else None
            if pend is not None:
                pv(*pend)
            if mask is not None:
                s = jnp.where(mask, s, -jnp.inf)
            m_old = m_ref[g, rows, :]
            m_new = jnp.maximum(m_old, jnp.max(s, axis=1, keepdims=True) * c)
            alpha = jnp.exp2(m_old - m_new)
            p = jnp.exp2(s * c - m_new[:, :1])
            ls = p[:, :dh]
            for j in range(1, cols // dh):
                ls = ls + p[:, j * dh:(j + 1) * dh]
            l_ref[g, rows, :] = l_ref[g, rows, :] * alpha + ls
            m_ref[g, rows, :] = m_new
            pend = (g, p.astype(jnp.bfloat16), alpha)
            s = s_next
        pv(*pend)

    def hist_body(i, carry):
        b = i // nt
        t = i % nt

        @pl.when(t == 0)
        def _():
            for j in range(2):
                pltpu.make_async_copy(hist_ref.at[b, 2 * layer + j], hkv.at[b, j], hsem.at[b, j]).wait()

        block(t, lambda: hkv[b, 0], lambda: hkv[b, 1], hc, None)
        return carry

    lax.fori_loop(0, sp * nt, hist_body, 0)
    for b in range(sp):
        pltpu.make_async_copy(new_ref.at[b], nkv.at[b], nsem.at[b]).wait()

    def new_body(i, carry):
        b = i // nt
        block(i % nt, lambda: nkv[b, 0], lambda: nkv[b, 1], nc, None)
        return carry

    lax.fori_loop(0, me * nt, new_body, 0)

    def diag_body(t, carry):
        r = lax.broadcasted_iota(jnp.int32, (rows_t, nc), 0) + t * rows_t
        col = lax.broadcasted_iota(jnp.int32, (rows_t, nc), 1)
        block(t, lambda: nkv[me, 0], lambda: nkv[me, 1], nc, col <= r)
        return carry

    lax.fori_loop(0, nt, diag_body, 0)
    for g in range(heads):
        l = jnp.sum(l_ref[g], axis=1, keepdims=True)
        o_ref[:, g * dh:(g + 1) * dh] = (acc_ref[g] / l).astype(jnp.bfloat16)


def attention(sp, layer, q, hist, new):
    n, w = q.shape
    _, _, hc, dh = hist.shape
    heads = w // dh
    keys = sp * hc + sp * n // 2
    return pl.pallas_call(
        functools.partial(attn_kernel, sp, layer),
        out_shape=jax.ShapeDtypeStruct((n, w), jnp.bfloat16),
        in_specs=[pl.BlockSpec(memory_space=pltpu.VMEM), pl.BlockSpec(memory_space=pltpu.HBM),
                  pl.BlockSpec(memory_space=pltpu.HBM)],
        out_specs=pl.BlockSpec(memory_space=pltpu.VMEM),
        scratch_shapes=[
            pltpu.VMEM((sp, 2, hc, dh), jnp.bfloat16),
            pltpu.VMEM((sp, 2, n, dh), jnp.bfloat16),
            pltpu.VMEM((heads, n, dh), jnp.float32),
            pltpu.VMEM((heads, n, dh), jnp.float32),
            pltpu.VMEM((heads, n, dh), jnp.float32),
            pltpu.SemaphoreType.DMA((sp, 2)),
            pltpu.SemaphoreType.DMA((sp,)),
        ],
        compiler_params=pltpu.CompilerParams(vmem_limit_bytes=60 * 2 ** 20),
        cost_estimate=pl.CostEstimate(flops=4 * n * w * keys, bytes_accessed=4 * keys * dh, transcendentals=n * heads * keys),
        name="attention",
    )(q, hist, new)


MESH = pl.DeviceIdType.MESH
LN = 128


def mlp_kernel(T, layer, attn_ref, x_ref, wo_ref, g_ref, wg_ref, wu_ref, wd_ref, out_ref,
               acc, ring, H, U, wdb, RA, RB, RD, RU, XF, xm, st, strv,
               ags, agr, rss, rsr, sts, strs, lsem, wsem, wosem, dsem):
    n, d = XF.shape
    dt = d // T
    KP = dt // LN
    NP = T * KP
    NG = NP // 4
    F = U.shape[1]
    FP = F // LN
    t = lax.axis_index("tp")
    up = lax.rem(t + 1, T)
    dn = lax.rem(t + 3, T)
    op = lax.rem(t + 2, T)
    hf = n // 2
    ALL, A, B = pl.ds(0, n), pl.ds(0, hf), pl.ds(hf, hf)

    barrier = pltpu.get_barrier_semaphore()
    for dev in (up, dn, op):
        pl.semaphore_signal(barrier, inc=1, device_id={"tp": dev}, device_id_type=MESH)
    pl.semaphore_wait(barrier, 3)

    def rcopy(src, dst, ss, rs, dev):
        return pltpu.make_async_remote_copy(src_ref=src, dst_ref=dst, send_sem=ss, recv_sem=rs,
                                            device_id={"tp": dev}, device_id_type=MESH)

    def pos_of(kind, k):
        return {'own': k, 'up': KP + 2 * k, 'dn': KP + 2 * k + 1, 'op': 3 * KP + k}[kind]

    order = [None] * NP
    for kind in ('own', 'up', 'dn', 'op'):
        for k in range(KP):
            order[pos_of(kind, k)] = (kind, k)
    owner_of = {'own': t, 'up': up, 'dn': dn, 'op': op}

    def hloc(kind, owner, k, rows):
        p = pos_of(kind, k)
        return H.at[p // 4, rows, pl.ds((p % 4) * LN, LN)]

    def xloc(kind, owner, k, rows):
        return XF.at[rows, pl.ds(pl.multiple_of(owner * dt + k * LN, LN), LN)]

    class Gather:
        def __init__(self, loc):
            self.loc = loc

        def c_up(self, k):
            return rcopy(self.loc('own', t, k, ALL), self.loc('dn', t, k, ALL), ags.at[0, k], agr.at[0, k], up)

        def c_dn(self, k):
            return rcopy(self.loc('own', t, k, ALL), self.loc('up', t, k, ALL), ags.at[1, k], agr.at[1, k], dn)

        def r_up(self, k):
            return rcopy(self.loc('dn', dn, k, A), self.loc('op', dn, k, A), ags.at[2, k], agr.at[2, k], up)

        def r_dn(self, k):
            return rcopy(self.loc('up', up, k, B), self.loc('op', up, k, B), ags.at[3, k], agr.at[3, k], dn)

        def send(self, k):
            self.c_up(k).start()
            self.c_dn(k).start()

        def wait(self, kind, k):
            if kind == 'dn':
                rcopy(self.loc('dn', dn, k, ALL), self.loc('dn', dn, k, ALL), ags.at[0, k], agr.at[0, k], up).wait_recv()
                self.r_up(k).start()
            elif kind == 'up':
                rcopy(self.loc('up', up, k, ALL), self.loc('up', up, k, ALL), ags.at[1, k], agr.at[1, k], dn).wait_recv()
                self.r_dn(k).start()
            elif kind == 'op':
                rcopy(self.loc('op', op, k, A), self.loc('op', op, k, A), ags.at[2, k], agr.at[2, k], up).wait_recv()
                rcopy(self.loc('op', op, k, B), self.loc('op', op, k, B), ags.at[3, k], agr.at[3, k], dn).wait_recv()

        def done(self):
            for k in range(KP):
                self.c_up(k).wait_send()
                self.c_dn(k).wait_send()
                self.r_up(k).wait_send()
                self.r_dn(k).wait_send()

    gh = Gather(hloc)
    gx = Gather(xloc)

    def wait_group(gather, j):
        for kind, k in order[4 * j:4 * j + 4]:
            gather.wait(kind, k)

    def own_in(k):
        return pltpu.make_async_copy(attn_ref.at[:, pl.ds(k * LN, LN)], hloc('own', t, k, ALL), lsem.at[0])

    for k in range(KP):
        own_in(k).start()
    xin = pltpu.make_async_copy(x_ref.at[:, pl.ds(pl.multiple_of(t * dt, LN), dt)], xm, lsem.at[1])
    xin.start()
    for k in range(KP):
        own_in(k).wait()
    for k in range(KP):
        gh.send(k)

    per = F // dt
    SR = wo_ref.shape[4]
    NS = wo_ref.shape[0]

    def wo_copy(p, s):
        kind, k = order[p]
        j = p // 4
        return pltpu.make_async_copy(
            wo_ref.at[s, owner_of[kind], layer, k],
            ring.at[j // per, pl.ds((p % 4) * LN + s * SR, SR), pl.ds((j % per) * dt, dt)], wosem.at[j])

    for p in range(NP):
        for s in range(NS):
            wo_copy(p, s).start()

    def w_copy(i, q, slot):
        p = (i // 2) * 4 + q
        own = p < KP
        pair = jnp.logical_and(p >= KP, p < 3 * KP)
        k = jnp.where(own, p, jnp.where(pair, (p - KP) // 2, p - 3 * KP))
        who = jnp.where(own, t, jnp.where(pair, jnp.where(lax.rem(p - KP, 2) == 0, up, dn), op))
        row = pl.multiple_of(who * dt + k * LN, LN)
        src = wg_ref if False else None
        return row

    def w_start(i, slot):
        for q in range(4):
            row = w_copy(i, q, slot)
            dst = ring.at[slot, pl.ds(q * LN, LN), :]

            @pl.when(lax.rem(i, 2) == 0)
            def _():
                pltpu.make_async_copy(wg_ref.at[layer, pl.ds(row, LN), :], dst, wsem.at[slot]).start()

            @pl.when(lax.rem(i, 2) == 1)
            def _():
                pltpu.make_async_copy(wu_ref.at[layer, pl.ds(row, LN), :], dst, wsem.at[slot]).start()

    def w_wait(slot):
        pltpu.make_async_copy(wg_ref.at[layer, pl.ds(0, 4 * LN), :], ring.at[slot], wsem.at[slot]).wait()

    NSLOT = ring.shape[0]
    free = list(range((NG + per - 1) // per, NSLOT))
    for s in free:
        w_start(jnp.int32(s), s)

    def zero(j, c):
        acc[j] = jnp.zeros(acc.shape[1:], acc.dtype)
        return c

    lax.fori_loop(0, 2 * FP, zero, 0)

    def wo_step(j, c):
        for jj in range(NG):
            @pl.when(j == jj)
            def _():
                wait_group(gh, jj)
                pltpu.make_async_copy(wo_ref.at[0, 0, layer, 0], ring.at[0, pl.ds(0, SR), pl.ds(0, dt)],
                                      wosem.at[jj]) if False else None
                for q in range(4):
                    for s in range(NS):
                        wo_copy(4 * jj + q, s).wait()
        w = ring[j // per, :, pl.ds(pl.multiple_of(lax.rem(j, per) * dt, LN), dt)]
        r = mm(H[j], w)
        for k in range(KP):
            acc[k] += r[:, k * LN:(k + 1) * LN]
        return c

    lax.fori_loop(0, NG, wo_step, 0)
    for s in range(min(NSLOT, 2 * NG)):
        if s not in free:
            w_start(jnp.int32(s), s)
    gh.done()
    xin.wait()
    ss = jnp.zeros((n, LN), jnp.float32)
    for k in range(KP):
        v = xm[:, k * LN:(k + 1) * LN] + acc[k].astype(jnp.bfloat16)
        xm[:, k * LN:(k + 1) * LN] = v
        vf = v.astype(jnp.float32)
        ss = ss + vf * vf
        acc[k] = jnp.zeros(acc.shape[1:], acc.dtype)
    sb = jnp.broadcast_to(jnp.sum(ss, axis=1, keepdims=True), (n, LN))
    st[...] = jnp.swapaxes(sb, 0, 1)[:8]

    def s_copy(j, dev):
        return rcopy(st, strv.at[j], sts.at[j], strs.at[j], dev)

    peers = ((0, up), (1, dn), (2, op))
    for j, dev in peers:
        s_copy(j, dev).start()
    for j, dev in peers:
        s_copy(j, dev).wait_recv()
    tot = st[...] + strv[0] + strv[1] + strv[2]
    r8 = lax.rsqrt(tot / d + EPS)
    rb = jnp.swapaxes(jnp.concatenate([r8] * (LN // 8), axis=0), 0, 1)
    for k in range(KP):
        gk = g_ref[0, pl.ds(pl.multiple_of(t * dt + k * LN, LN), LN)].astype(jnp.float32)
        hv = (xm[:, k * LN:(k + 1) * LN].astype(jnp.float32) * rb * gk[None, :]).astype(jnp.bfloat16)
        H[k // 4, :, (k % 4) * LN:(k % 4 + 1) * LN] = hv
    for k in range(KP):
        gh.send(k)
    for j, dev in peers:
        s_copy(j, dev).wait_send()

    def gu_step(i, c):
        j = i // 2
        slot = lax.rem(i, NSLOT)
        for jj in range(NG):
            @pl.when(i == 2 * jj)
            def _():
                wait_group(gh, jj)
        w_wait(slot)
        base = lax.rem(i, 2) * FP
        for f in range(0, FP, 4):
            m = min(4, FP - f)
            r = mm(H[j], ring[slot, :, f * LN:(f + m) * LN])
            for q in range(m):
                acc[base + f + q] += r[:, q * LN:(q + 1) * LN]

        @pl.when(i + NSLOT < 2 * NG)
        def _():
            w_start(i + NSLOT, slot)
        return c

    def d_col(p):
        c = p // KP
        who = jnp.where(c == 0, op, jnp.where(c == 1, up, jnp.where(c == 2, dn, t)))
        return pl.multiple_of(who * dt + lax.rem(p, KP) * LN, LN)

    def d_start(i, slot):
        for q in range(2):
            pltpu.make_async_copy(wd_ref.at[layer, :, pl.ds(d_col(2 * i + q), LN)],
                                  wdb.at[slot, :, pl.ds(q * LN, LN)], dsem.at[slot]).start()

    def d_wait(slot):
        pltpu.make_async_copy(wd_ref.at[layer, :, pl.ds(0, 2 * LN)], wdb.at[slot], dsem.at[slot]).wait()

    d_start(jnp.int32(0), 0)
    d_start(jnp.int32(1), 1)
    lax.fori_loop(0, 2 * NG, gu_step, 0)

    def silu(f, c):
        a = acc[f].astype(jnp.bfloat16).astype(jnp.float32)
        b = acc[FP + f].astype(jnp.bfloat16).astype(jnp.float32)
        U[:, pl.ds(pl.multiple_of(f * LN, LN), LN)] = (a * (1.0 / (1.0 + jnp.exp(-a))) * b).astype(jnp.bfloat16)
        return c

    lax.fori_loop(0, FP, silu, 0)
    gh.done()

    def c_opA(k):
        return rcopy(acc.at[k, A, :], RA.at[k], rss.at[0, k], rsr.at[0, k], up)

    def c_opB(k):
        return rcopy(acc.at[k, B, :], RB.at[k], rss.at[1, k], rsr.at[1, k], dn)

    def c_upB(k):
        return rcopy(acc.at[KP + k, B, :], RD.at[k, B, :], rss.at[2, k], rsr.at[2, k], up)

    def c_dnA(k):
        return rcopy(acc.at[2 * KP + k, A, :], RU.at[k, A, :], rss.at[3, k], rsr.at[3, k], dn)

    def c_upA(k):
        return rcopy(acc.at[KP + k, A, :], RD.at[k, A, :], rss.at[4, k], rsr.at[4, k], up)

    def c_dnB(k):
        return rcopy(acc.at[2 * KP + k, B, :], RU.at[k, B, :], rss.at[5, k], rsr.at[5, k], dn)

    def rs_send(p):
        c = p // KP
        k = lax.rem(p, KP)

        @pl.when(c == 0)
        def _():
            c_opA(k).start()
            c_opB(k).start()

        @pl.when(c == 1)
        def _():
            c_upB(k).start()

        @pl.when(c == 2)
        def _():
            c_dnA(k).start()

    def down(i, c):
        slot = lax.rem(i, 2)
        d_wait(slot)

        @pl.when(i > 0)
        def _():
            rs_send(2 * i - 2)
            rs_send(2 * i - 1)

        r = mm(U[...], wdb[slot])
        for q in range(2):
            acc[2 * i + q] = r[:, q * LN:(q + 1) * LN]

        @pl.when(i + 2 < NP // 2)
        def _():
            d_start(i + 2, slot)
        return c

    lax.fori_loop(0, NP // 2, down, 0)

    def add(k, c):
        c_opA(k).wait_recv()
        acc[KP + k, 0:hf, :] += RA[k]
        c_upA(k).start()
        c_opB(k).wait_recv()
        acc[2 * KP + k, hf:n, :] += RB[k]
        c_dnB(k).start()
        return c

    lax.fori_loop(0, KP, add, 0)

    for k in range(KP):
        c_upB(k).wait_recv()
        c_dnA(k).wait_recv()
        c_upA(k).wait_recv()
        c_dnB(k).wait_recv()
        s = acc[3 * KP + k] + RD[k] + RU[k]
        v = xm[:, k * LN:(k + 1) * LN] + s.astype(jnp.bfloat16)
        XF[:, pl.ds(pl.multiple_of(t * dt + k * LN, LN), LN)] = v
        gx.send(k)
    for k in range(KP):
        gx.wait('up', k)
        gx.wait('dn', k)
    for k in range(KP):
        gx.wait('op', k)
    o = pltpu.make_async_copy(XF, out_ref, lsem.at[0])
    o.start()
    gx.done()
    for k in range(KP):
        for cp in (c_opA, c_opB, c_upB, c_dnA, c_upA, c_dnB):
            cp(k).wait_send()
    o.wait()


def mlp(T, layer, attn, x, wo_g, g, wg, wu, wd, cid):
    n, d = x.shape
    F = wg.shape[2]
    dt = d // T
    KP = dt // LN
    FP = F // LN
    hf = n // 2
    NG = T * KP // 4
    f32, bf = jnp.float32, jnp.bfloat16
    anyspec = pl.BlockSpec(memory_space=pltpu.HBM)
    D = pltpu.SemaphoreType.DMA
    return pl.pallas_call(
        functools.partial(mlp_kernel, T, layer),
        out_shape=jax.ShapeDtypeStruct((n, d), bf),
        in_specs=[anyspec, anyspec, anyspec, pl.BlockSpec(memory_space=pltpu.VMEM), anyspec, anyspec, anyspec],
        out_specs=anyspec,
        scratch_shapes=[
            pltpu.VMEM((2 * FP, n, LN), f32),
            pltpu.VMEM((3, 4 * LN, F), bf),
            pltpu.VMEM((NG, n, 4 * LN), bf),
            pltpu.VMEM((n, F), bf),
            pltpu.VMEM((2, F, 2 * LN), bf),
            pltpu.VMEM((KP, hf, LN), f32),
            pltpu.VMEM((KP, hf, LN), f32),
            pltpu.VMEM((KP, n, LN), f32),
            pltpu.VMEM((KP, n, LN), f32),
            pltpu.VMEM((n, d), bf),
            pltpu.VMEM((n, dt), bf),
            pltpu.VMEM((8, n), f32),
            pltpu.VMEM((3, 8, n), f32),
            D((4, KP)), D((4, KP)), D((6, KP)), D((6, KP)), D((3,)), D((3,)),
            D((2,)), D((3,)), D((NG,)), D((2,)),
        ],
        compiler_params=pltpu.CompilerParams(vmem_limit_bytes=61 * 2 ** 20, collective_id=cid, has_side_effects=True),
        cost_estimate=pl.CostEstimate(flops=2 * n * d * (3 * F + dt), bytes_accessed=2 * d * (3 * F + dt), transcendentals=n * F),
        name="mlp",
    )(attn, x, wo_g, g, wg, wu, wd)


def solution(mesh):
    sp = mesh.shape['sp']
    tp = mesh.shape['tp']
    row = ('dp', 'sp')
    kv_spec = P(None, row, 'tp', None)
    col = P(None, None, 'tp')
    rowsplit = P(None, 'tp', None)

    def body(x, pos, k_hist, v_hist, wq, wk, wv, wo, wg, wu, wd, g1, g2):
        n, d = x.shape
        layers, hc, kvl, dh = k_hist.shape
        hql = wq.shape[-1] // dh
        dt = d // tp
        tt, ss = lax.axis_index('tp'), lax.axis_index('sp')
        kp = dt // LN
        sr = LN // sp
        wr = lax.dynamic_index_in_dim(wo.reshape(layers, kp, sp, sr, d), ss, axis=2, keepdims=False)

        def wcols(t):
            return lax.dynamic_slice_in_dim(wr, t * dt, dt, axis=3)

        parts = jnp.zeros((tp,) + wcols(0).shape, wo.dtype)
        parts = lax.dynamic_update_index_in_dim(parts, wcols(tt), tt, 0)
        for j in range(1, tp):
            got = lax.ppermute(wcols(lax.rem(tt + j, tp)), 'tp', [(i, (i + j) % tp) for i in range(tp)])
            parts = lax.dynamic_update_index_in_dim(parts, got, lax.rem(tt + tp - j, tp), 0)
        kv = jnp.stack([k_hist[:, :, 0], v_hist[:, :, 0]], axis=1).reshape(2 * layers, hc, dh)
        hist = lax.all_gather(kv, 'sp', axis=0)
        ks, vs = [], []
        wo_g = None

        for l in range(layers):
            h = rmsnorm(x, g1[l])
            k = rope(mm(h, wk[l]).astype(jnp.bfloat16).reshape(n, kvl, dh), pos)
            v = mm(h, wv[l]).astype(jnp.bfloat16).reshape(n, kvl, dh)
            ks.append(k)
            vs.append(v)
            new = lax.all_gather(jnp.stack([k[:, 0], v[:, 0]]), 'sp', axis=0)
            if wo_g is None:
                wo_g = lax.all_gather(parts, 'sp', axis=0)
            q = rope(mm(h, wq[l]).astype(jnp.bfloat16).reshape(n, hql, dh), pos)
            attn = attention(sp, l, q.reshape(n, hql * dh), hist, new)
            x = mlp(tp, l, attn, x, wo_g, g2[l:l + 1], wg, wu, wd, l)
        return x, jnp.stack(ks), jnp.stack(vs)

    in_specs = (P(row, None), P(row), kv_spec, kv_spec, col, col, col, rowsplit, col, col, rowsplit, P(), P())
    out_specs = (P(row, None), kv_spec, kv_spec)
    return jax.shard_map(body, mesh=mesh, in_specs=in_specs, out_specs=out_specs, check_vma=False)
```

```python
import functools

import jax
import jax.numpy as jnp
from jax import lax
from jax.experimental import pallas as pl
from jax.experimental.pallas import tpu as pltpu
from jax.sharding import PartitionSpec as P

EPS = 1e-5
ROPE_THETA = 500000.0
LOG2E = 1.4426950408889634
MESH = pl.DeviceIdType.MESH
LN = 128


def mm(a, b):
    return jnp.dot(a, b, preferred_element_type=jnp.float32)


def attn_kernel(T, SP, layer, x_ref, cos_ref, sin_ref, kh_ref, vh_ref, wq_ref, wk_ref, wv_ref, g_ref,
                out_ref, ko_ref, vo_ref,
                xb, wb, kv, qb, m_ref, l_ref, acc_ref, ga,
                kvs, kvr, gas, gar, lsem, hsem, wsem):
    n, d = xb.shape
    w = qb.shape[1]
    dh = kv.shape[3]
    heads = w // dh
    X = SP // 2
    C = kv.shape[2]
    hc = C // 2
    R = min(128, n)
    nt = n // R
    scale = dh ** -0.5 * LOG2E
    me = lax.axis_index("sp")
    t = lax.axis_index("tp")
    c = lax.rem(me, 2)
    xx = me // 2
    lx, rx, ox = lax.rem(xx + X - 1, X), lax.rem(xx + 1, X), lax.rem(xx + 2, X)
    left, right, part = lx * 2 + c, rx * 2 + c, xx * 2 + 1 - c
    up, dn = lax.rem(t + 1, T), lax.rem(t + T - 1, T)

    barrier = pltpu.get_barrier_semaphore()
    for dev in ({"sp": left}, {"sp": right}, {"sp": part}, {"tp": up}, {"tp": dn}):
        pl.semaphore_signal(barrier, inc=1, device_id=dev, device_id_type=MESH)

    def hist_in(j):
        return pltpu.make_async_copy((kh_ref, vh_ref)[j].at[layer], kv.at[xx, j, pl.ds(c * hc, hc), :], hsem)

    for j in range(2):
        hist_in(j).start()
    xin = pltpu.make_async_copy(x_ref, xb, lsem.at[0])
    xin.start()
    win = [pltpu.make_async_copy(wk_ref.at[layer], wb.at[:, 0:dh], wsem.at[0]),
           pltpu.make_async_copy(wv_ref.at[layer], wb.at[:, dh:2 * dh], wsem.at[0]),
           pltpu.make_async_copy(wq_ref.at[layer], wb.at[:, 2 * dh:], wsem.at[1])]
    for cp in win:
        cp.start()

    def region(kind, chip, core, half):
        if kind == 0:
            blk, base, ln = chip, core * hc, hc
        else:
            blk, base, ln = X + chip // 2, lax.rem(chip, 2) * (2 * n) + core * n, n
        if half is not None:
            ln = ln // 2
            base = base + half * ln
        return kv.at[blk, :, pl.ds(pl.multiple_of(base, ln), ln), :]

    sent = [(xx, c, None, right), (xx, c, None, left), (xx, c, None, part), (lx, c, 0, right), (rx, c, 1, left),
            (lx, c, None, part), (rx, c, None, part), (ox, c, 0, part), (ox, c, 1, part)]
    got = [(lx, c, None), (rx, c, None), (xx, 1 - c, None), (ox, c, 0), (ox, c, 1),
           (lx, 1 - c, None), (rx, 1 - c, None), (ox, 1 - c, 0), (ox, 1 - c, 1)]

    def tx(kind, i):
        chip, core, half, dev = sent[i]
        r = region(kind, chip, core, half)
        return pltpu.make_async_remote_copy(src_ref=r, dst_ref=r, send_sem=kvs.at[kind, i], recv_sem=kvr.at[kind, i],
                                            device_id={"sp": dev}, device_id_type=MESH)

    def rx_wait(kind, i):
        chip, core, half = got[i]
        r = region(kind, chip, core, half)
        pltpu.make_async_remote_copy(src_ref=r, dst_ref=r, send_sem=kvs.at[kind, i], recv_sem=kvr.at[kind, i],
                                     device_id={"sp": part}, device_id_type=MESH).wait_recv()

    def send_own(kind):
        for i in (0, 1, 2):
            tx(kind, i).start()

    def pass_near(kind):
        rx_wait(kind, 0)
        tx(kind, 3).start()
        tx(kind, 5).start()
        rx_wait(kind, 1)
        tx(kind, 4).start()
        tx(kind, 6).start()

    def pass_far(kind):
        rx_wait(kind, 3)
        tx(kind, 7).start()
        rx_wait(kind, 4)
        tx(kind, 8).start()

    pl.semaphore_wait(barrier, 5)
    for j in range(2):
        hist_in(j).wait()
    send_own(0)

    xin.wait()
    g = g_ref[...].astype(jnp.float32)
    NR = min(32, n)

    def norm(i, carry):
        rows = pl.ds(pl.multiple_of(i * NR, NR), NR)
        xf = xb[rows, :].astype(jnp.float32)
        r = lax.rsqrt(jnp.sum(xf * xf, axis=1, keepdims=True) / d + EPS)
        xb[rows, :] = (xf * r * g).astype(jnp.bfloat16)
        return carry

    lax.fori_loop(0, n // NR, norm, 0)

    def rope(a):
        a = a.astype(jnp.bfloat16).astype(jnp.float32)
        return (a * cos_ref[...] + pltpu.roll(a, dh // 2, 1) * sin_ref[...]).astype(jnp.bfloat16)

    win[0].wait()
    win[1].wait()
    r = mm(xb[...], wb[:, :2 * dh])
    own = pl.ds(pl.multiple_of(lax.rem(xx, 2) * (2 * n) + c * n, n), n)
    kv[X + xx // 2, 0, own, :] = rope(r[:, :dh])
    kv[X + xx // 2, 1, own, :] = r[:, dh:].astype(jnp.bfloat16)
    win[2].wait()

    def qpair(i, carry):
        @pl.when(i == 1)
        def _():
            send_own(1)

        r = mm(xb[...], wb[:, pl.ds(pl.multiple_of((i + 1) * 2 * dh, 2 * dh), 2 * dh)])
        for j in range(2):
            qb[:, pl.ds(pl.multiple_of((2 * i + j) * dh, dh), dh)] = rope(r[:, j * dh:(j + 1) * dh])
        return carry

    lax.fori_loop(0, heads // 2, qpair, 0)
    if heads // 2 < 2:
        send_own(1)
    if heads % 2:
        qb[:, (heads - 1) * dh:] = rope(mm(xb[...], wb[:, (heads + 1) * dh:]))

    def kv_out(j):
        return pltpu.make_async_copy(kv.at[X + xx // 2, j, own, :], (ko_ref, vo_ref)[j], hsem)

    for j in range(2):
        kv_out(j).start()

    def init(i, carry):
        rows = pl.ds(pl.multiple_of(i * R, R), R)
        for h in range(heads):
            m_ref[h, rows, :] = jnp.full((R, LN), -1e30, jnp.float32)
            l_ref[h, rows, :] = jnp.zeros((R, LN), jnp.float32)
            acc_ref[h, rows, :] = jnp.zeros((R, dh), jnp.float32)
        return carry

    lax.fori_loop(0, nt, init, 0)

    def unit(tile, blk, mask):
        rows = pl.ds(pl.multiple_of(tile * R, R), R)

        def qk(h):
            return lax.dot_general(qb[rows, h * dh:(h + 1) * dh], kv[blk, 0], (((1,), (1,)), ((), ())),
                                   preferred_element_type=jnp.float32)

        def pv(h, p, alpha):
            acc_ref[h, rows, :] = acc_ref[h, rows, :] * alpha + mm(p, kv[blk, 1])

        s = qk(0)
        pend = None
        for h in range(heads):
            s_next = qk(h + 1) if h + 1 < heads else None
            if pend is not None:
                pv(*pend)
            if mask is not None:
                s = jnp.where(mask, s, -jnp.inf)
            m_old = m_ref[h, rows, :]
            m_new = jnp.maximum(m_old, jnp.max(s, axis=1, keepdims=True) * scale)
            alpha = jnp.exp2(m_old - m_new)
            p = jnp.exp2(s * scale - m_new[:, :1])
            ls = p[:, :LN]
            for j in range(1, C // LN):
                ls = ls + p[:, j * LN:(j + 1) * LN]
            l_ref[h, rows, :] = l_ref[h, rows, :] * alpha + ls
            m_ref[h, rows, :] = m_new
            pend = (h, p.astype(jnp.bfloat16), alpha)
            s = s_next
        pv(*pend)

    hR = R // 2

    def gx(i, tile):
        base = pl.multiple_of(tile * R, R)
        owner, off, ln, dev = ((t, 0, R, up), (t, 0, R, dn), (dn, 0, hR, up), (up, hR, hR, dn))[i]
        ref = ga.at[owner, pl.ds(pl.multiple_of(base + off, hR), ln), :]
        return pltpu.make_async_remote_copy(src_ref=ref, dst_ref=ref, send_sem=gas.at[i, tile], recv_sem=gar.at[i, tile],
                                            device_id={"tp": dev}, device_id_type=MESH)

    def g_wait(i, tile):
        base = pl.multiple_of(tile * R, R)
        far = lax.rem(t + 2, T)
        owner, off, ln = ((dn, 0, R), (up, 0, R), (far, 0, hR), (far, hR, hR))[i]
        ref = ga.at[owner, pl.ds(pl.multiple_of(base + off, hR), ln), :]
        pltpu.make_async_remote_copy(src_ref=ref, dst_ref=ref, send_sem=gas.at[i, tile], recv_sem=gar.at[i, tile],
                                     device_id={"tp": up}, device_id_type=MESH).wait_recv()

    def g_pass(tile):
        g_wait(0, tile)
        gx(2, tile).start()
        g_wait(1, tile)
        gx(3, tile).start()

    def finish(tile):
        rows = pl.ds(pl.multiple_of(tile * R, R), R)
        for h in range(heads):
            l = jnp.sum(l_ref[h, rows, :], axis=1, keepdims=True)
            ga[t, rows, h * dh:(h + 1) * dh] = (acc_ref[h, rows, :] / l).astype(jnp.bfloat16)

    rx_wait(0, 2)
    first = 3 * nt
    per = 1 + xx // 2
    pts = [2, nt, 2 * nt - 2, 2 * nt] if nt >= 4 else [0, 1, 2, 3]

    def step(i, carry):
        for at, fn, kind in zip(pts, (pass_near, pass_near, pass_far, pass_far), (0, 1, 0, 1)):
            @pl.when(i == at)
            def _():
                fn(kind)

        for chip_at, gid in ((nt, 5), (2 * nt, 6)):
            @pl.when(i == chip_at)
            def _():
                rx_wait(0, gid)

        @pl.when(i == first)
        def _():
            rx_wait(0, 7)
            rx_wait(0, 8)
            for gid in (2, 5, 6, 7, 8):
                rx_wait(1, gid)

        late = i >= first
        i2 = jnp.maximum(i - first, 0)
        m = lax.rem(i2, per)
        tile = jnp.where(late, i2 // per, lax.rem(i, nt))
        early = jnp.where(i < nt, xx, jnp.where(i < 2 * nt, lx, rx))
        blk = jnp.where(late, jnp.where(m == 0, ox, X + m - 1), early)
        unit(tile, blk, None)

        @pl.when(jnp.logical_and(late, jnp.logical_and(m == 0, tile >= 2)))
        def _():
            g_pass(tile - 2)

        @pl.when(jnp.logical_and(late, m == per - 1))
        def _():
            off = lax.rem(xx, 2) * (2 * n) + c * n + tile * R
            row = lax.broadcasted_iota(jnp.int32, (R, C), 0) + off
            unit(tile, X + xx // 2, lax.broadcasted_iota(jnp.int32, (R, C), 1) <= row)
            finish(tile)
            gx(0, tile).start()
            gx(1, tile).start()
        return carry

    lax.fori_loop(0, first + nt * per, step, 0)
    for tile in range(max(nt - 2, 0), nt):
        g_pass(tile)
    for tile in range(nt):
        g_wait(2, tile)
        g_wait(3, tile)
    o = pltpu.make_async_copy(ga, out_ref, lsem.at[0])
    o.start()
    for tile in range(nt):
        for i in range(4):
            gx(i, tile).wait_send()
    for kind in range(2):
        for i in range(9):
            tx(kind, i).wait_send()
    for j in range(2):
        kv_out(j).wait()
    o.wait()


def attention(T, SP, layer, x, cos, sin, kh, vh, wq, wk, wv, g, cid):
    n, d = x.shape
    w = wq.shape[2]
    hc, dh = kh.shape[1], kh.shape[2]
    heads = w // dh
    X = SP // 2
    assert 2 * hc == 4 * n and wk.shape[2] == dh
    R = min(128, n)
    f32, bf = jnp.float32, jnp.bfloat16
    hbm = pl.BlockSpec(memory_space=pltpu.HBM)
    vm = pl.BlockSpec(memory_space=pltpu.VMEM)
    D = pltpu.SemaphoreType.DMA
    keys = SP * (hc + n // 2)
    return pl.pallas_call(
        functools.partial(attn_kernel, T, SP, layer),
        out_shape=[jax.ShapeDtypeStruct((T, n, w), bf), jax.ShapeDtypeStruct((n, dh), bf), jax.ShapeDtypeStruct((n, dh), bf)],
        in_specs=[hbm, vm, vm, hbm, hbm, hbm, hbm, hbm, vm],
        out_specs=[hbm, hbm, hbm],
        scratch_shapes=[
            pltpu.VMEM((n, d), bf),
            pltpu.VMEM((d, w + 2 * dh), bf),
            pltpu.VMEM((X + X // 2, 2, 2 * hc, dh), bf),
            pltpu.VMEM((n, w), bf),
            pltpu.VMEM((heads, n, LN), f32),
            pltpu.VMEM((heads, n, LN), f32),
            pltpu.VMEM((heads, n, dh), f32),
            pltpu.VMEM((T, n, w), bf),
            D((2, 9)), D((2, 9)), D((4, n // R)), D((4, n // R)), D((2,)), D, D((2,)),
        ],
        compiler_params=pltpu.CompilerParams(vmem_limit_bytes=61 * 2 ** 20, collective_id=cid, has_side_effects=True),
        cost_estimate=pl.CostEstimate(flops=4 * n * w * keys + 2 * n * d * (w + 2 * dh), bytes_accessed=4 * keys * dh,
                                      transcendentals=n * heads * keys),
        name="attention",
    )(x, cos, sin, kh, vh, wq, wk, wv, g)


def mlp_kernel(T, layer, attn_ref, x_ref, wo_ref, g_ref, wg_ref, wu_ref, wd_ref, out_ref,
               acc, ring, H, U, wdb, RA, RB, RD, RU, XF, xm, st, strv,
               ags, agr, rss, rsr, sts, strs, lsem, wsem, wosem, dsem, hsem):
    n, d = XF.shape
    dt = d // T
    KP = dt // LN
    NP = T * KP
    NG = NP // 4
    F = U.shape[1]
    FP = F // LN
    t = lax.axis_index("tp")
    up = lax.rem(t + 1, T)
    dn = lax.rem(t + 3, T)
    op = lax.rem(t + 2, T)
    hf = n // 2
    ALL, A, B = pl.ds(0, n), pl.ds(0, hf), pl.ds(hf, hf)

    barrier = pltpu.get_barrier_semaphore()
    for dev in (up, dn, op):
        pl.semaphore_signal(barrier, inc=1, device_id={"tp": dev}, device_id_type=MESH)

    def rcopy(src, dst, ss, rs, dev):
        return pltpu.make_async_remote_copy(src_ref=src, dst_ref=dst, send_sem=ss, recv_sem=rs,
                                            device_id={"tp": dev}, device_id_type=MESH)

    def pos_of(kind, k):
        return {'own': k, 'up': KP + 2 * k, 'dn': KP + 2 * k + 1, 'op': 3 * KP + k}[kind]

    order = [None] * NP
    for kind in ('own', 'up', 'dn', 'op'):
        for k in range(KP):
            order[pos_of(kind, k)] = (kind, k)
    owner_of = {'own': t, 'up': up, 'dn': dn, 'op': op}

    def hloc(kind, owner, k, rows):
        p = pos_of(kind, k)
        return H.at[p // 4, rows, pl.ds((p % 4) * LN, LN)]

    def xloc(kind, owner, k, rows):
        return XF.at[rows, pl.ds(pl.multiple_of(owner * dt + k * LN, LN), LN)]

    class Gather:
        def __init__(self, loc):
            self.loc = loc

        def c_up(self, k):
            return rcopy(self.loc('own', t, k, ALL), self.loc('dn', t, k, ALL), ags.at[0, k], agr.at[0, k], up)

        def c_dn(self, k):
            return rcopy(self.loc('own', t, k, ALL), self.loc('up', t, k, ALL), ags.at[1, k], agr.at[1, k], dn)

        def r_up(self, k):
            return rcopy(self.loc('dn', dn, k, A), self.loc('op', dn, k, A), ags.at[2, k], agr.at[2, k], up)

        def r_dn(self, k):
            return rcopy(self.loc('up', up, k, B), self.loc('op', up, k, B), ags.at[3, k], agr.at[3, k], dn)

        def send(self, k):
            self.c_up(k).start()
            self.c_dn(k).start()

        def wait(self, kind, k):
            if kind == 'dn':
                rcopy(self.loc('dn', dn, k, ALL), self.loc('dn', dn, k, ALL), ags.at[0, k], agr.at[0, k], up).wait_recv()
                self.r_up(k).start()
            elif kind == 'up':
                rcopy(self.loc('up', up, k, ALL), self.loc('up', up, k, ALL), ags.at[1, k], agr.at[1, k], dn).wait_recv()
                self.r_dn(k).start()
            elif kind == 'op':
                rcopy(self.loc('op', op, k, A), self.loc('op', op, k, A), ags.at[2, k], agr.at[2, k], up).wait_recv()
                rcopy(self.loc('op', op, k, B), self.loc('op', op, k, B), ags.at[3, k], agr.at[3, k], dn).wait_recv()

        def done(self):
            for k in range(KP):
                self.c_up(k).wait_send()
                self.c_dn(k).wait_send()
                self.r_up(k).wait_send()
                self.r_dn(k).wait_send()

    gh = Gather(hloc)
    gx = Gather(xloc)

    def wait_group(gather, j):
        for kind, k in order[4 * j:4 * j + 4]:
            gather.wait(kind, k)

    def h_in(p):
        kind, k = order[p]
        return pltpu.make_async_copy(attn_ref.at[owner_of[kind], :, pl.ds(k * LN, LN)], hloc(kind, None, k, ALL), hsem.at[p // 4])

    for p in range(NP):
        h_in(p).start()
    xin = pltpu.make_async_copy(x_ref.at[:, pl.ds(pl.multiple_of(t * dt, LN), dt)], xm, lsem.at[1])
    xin.start()

    per = F // dt
    SR = wo_ref.shape[4]
    NS = wo_ref.shape[0]

    def wo_copy(p, s):
        kind, k = order[p]
        j = p // 4
        return pltpu.make_async_copy(
            wo_ref.at[s, owner_of[kind], layer, k],
            ring.at[j // per, pl.ds((p % 4) * LN + s * SR, SR), pl.ds((j % per) * dt, dt)], wosem.at[j])

    for p in range(NP):
        for s in range(NS):
            wo_copy(p, s).start()

    def w_copy(i, q, slot):
        p = (i // 2) * 4 + q
        own = p < KP
        pair = jnp.logical_and(p >= KP, p < 3 * KP)
        k = jnp.where(own, p, jnp.where(pair, (p - KP) // 2, p - 3 * KP))
        who = jnp.where(own, t, jnp.where(pair, jnp.where(lax.rem(p - KP, 2) == 0, up, dn), op))
        row = pl.multiple_of(who * dt + k * LN, LN)
        return row

    def w_start(i, slot):
        for q in range(4):
            row = w_copy(i, q, slot)
            dst = ring.at[slot, pl.ds(q * LN, LN), :]

            @pl.when(lax.rem(i, 2) == 0)
            def _():
                pltpu.make_async_copy(wg_ref.at[layer, pl.ds(row, LN), :], dst, wsem.at[slot]).start()

            @pl.when(lax.rem(i, 2) == 1)
            def _():
                pltpu.make_async_copy(wu_ref.at[layer, pl.ds(row, LN), :], dst, wsem.at[slot]).start()

    def w_wait(slot):
        pltpu.make_async_copy(wg_ref.at[layer, pl.ds(0, 4 * LN), :], ring.at[slot], wsem.at[slot]).wait()

    NSLOT = ring.shape[0]
    free = list(range((NG + per - 1) // per, NSLOT))
    for s in free:
        w_start(jnp.int32(s), s)

    def zero(j, c):
        acc[j] = jnp.zeros(acc.shape[1:], acc.dtype)
        return c

    lax.fori_loop(0, 2 * FP, zero, 0)

    def wo_step(j, c):
        for jj in range(NG):
            @pl.when(j == jj)
            def _():
                for q in range(4):
                    h_in(4 * jj + q).wait()
                for q in range(4):
                    for s in range(NS):
                        wo_copy(4 * jj + q, s).wait()
        w = ring[j // per, :, pl.ds(pl.multiple_of(lax.rem(j, per) * dt, LN), dt)]
        r = mm(H[j], w)
        for k in range(KP):
            acc[k] += r[:, k * LN:(k + 1) * LN]
        return c

    lax.fori_loop(0, NG, wo_step, 0)
    for s in range(min(NSLOT, 2 * NG)):
        if s not in free:
            w_start(jnp.int32(s), s)
    xin.wait()
    ss = jnp.zeros((n, LN), jnp.float32)
    for k in range(KP):
        v = xm[:, k * LN:(k + 1) * LN] + acc[k].astype(jnp.bfloat16)
        xm[:, k * LN:(k + 1) * LN] = v
        vf = v.astype(jnp.float32)
        ss = ss + vf * vf
        acc[k] = jnp.zeros(acc.shape[1:], acc.dtype)
    sb = jnp.broadcast_to(jnp.sum(ss, axis=1, keepdims=True), (n, LN))
    st[...] = jnp.swapaxes(sb, 0, 1)[:8]

    pl.semaphore_wait(barrier, 3)

    def s_copy(j, dev):
        return rcopy(st, strv.at[j], sts.at[j], strs.at[j], dev)

    peers = ((0, up), (1, dn), (2, op))
    for j, dev in peers:
        s_copy(j, dev).start()
    for j, dev in peers:
        s_copy(j, dev).wait_recv()
    tot = st[...] + strv[0] + strv[1] + strv[2]
    r8 = lax.rsqrt(tot / d + EPS)
    rb = jnp.swapaxes(jnp.concatenate([r8] * (LN // 8), axis=0), 0, 1)
    for k in range(KP):
        gk = g_ref[0, pl.ds(pl.multiple_of(t * dt + k * LN, LN), LN)].astype(jnp.float32)
        hv = (xm[:, k * LN:(k + 1) * LN].astype(jnp.float32) * rb * gk[None, :]).astype(jnp.bfloat16)
        H[k // 4, :, (k % 4) * LN:(k % 4 + 1) * LN] = hv
    for k in range(KP):
        gh.send(k)
    for j, dev in peers:
        s_copy(j, dev).wait_send()

    def gu_step(i, c):
        j = i // 2
        slot = lax.rem(i, NSLOT)
        for jj in range(NG):
            @pl.when(i == 2 * jj)
            def _():
                wait_group(gh, jj)
        w_wait(slot)
        base = lax.rem(i, 2) * FP
        for f in range(0, FP, 4):
            m = min(4, FP - f)
            r = mm(H[j], ring[slot, :, f * LN:(f + m) * LN])
            for q in range(m):
                acc[base + f + q] += r[:, q * LN:(q + 1) * LN]

        @pl.when(i + NSLOT < 2 * NG)
        def _():
            w_start(i + NSLOT, slot)
        return c

    def d_col(p):
        c = p // KP
        who = jnp.where(c == 0, op, jnp.where(c == 1, up, jnp.where(c == 2, dn, t)))
        return pl.multiple_of(who * dt + lax.rem(p, KP) * LN, LN)

    def d_start(i, slot):
        for q in range(2):
            pltpu.make_async_copy(wd_ref.at[layer, :, pl.ds(d_col(2 * i + q), LN)],
                                  wdb.at[slot, :, pl.ds(q * LN, LN)], dsem.at[slot]).start()

    def d_wait(slot):
        pltpu.make_async_copy(wd_ref.at[layer, :, pl.ds(0, 2 * LN)], wdb.at[slot], dsem.at[slot]).wait()

    d_start(jnp.int32(0), 0)
    d_start(jnp.int32(1), 1)
    lax.fori_loop(0, 2 * NG, gu_step, 0)

    def silu(f, c):
        a = acc[f].astype(jnp.bfloat16).astype(jnp.float32)
        b = acc[FP + f].astype(jnp.bfloat16).astype(jnp.float32)
        U[:, pl.ds(pl.multiple_of(f * LN, LN), LN)] = (a * (1.0 / (1.0 + jnp.exp(-a))) * b).astype(jnp.bfloat16)
        return c

    lax.fori_loop(0, FP, silu, 0)
    gh.done()

    def c_opA(k):
        return rcopy(acc.at[k, A, :], RA.at[k], rss.at[0, k], rsr.at[0, k], up)

    def c_opB(k):
        return rcopy(acc.at[k, B, :], RB.at[k], rss.at[1, k], rsr.at[1, k], dn)

    def c_upB(k):
        return rcopy(acc.at[KP + k, B, :], RD.at[k, B, :], rss.at[2, k], rsr.at[2, k], up)

    def c_dnA(k):
        return rcopy(acc.at[2 * KP + k, A, :], RU.at[k, A, :], rss.at[3, k], rsr.at[3, k], dn)

    def c_upA(k):
        return rcopy(acc.at[KP + k, A, :], RD.at[k, A, :], rss.at[4, k], rsr.at[4, k], up)

    def c_dnB(k):
        return rcopy(acc.at[2 * KP + k, B, :], RU.at[k, B, :], rss.at[5, k], rsr.at[5, k], dn)

    def rs_send(p):
        c = p // KP
        k = lax.rem(p, KP)

        @pl.when(c == 0)
        def _():
            c_opA(k).start()
            c_opB(k).start()

        @pl.when(c == 1)
        def _():
            c_upB(k).start()

        @pl.when(c == 2)
        def _():
            c_dnA(k).start()

    def down(i, c):
        slot = lax.rem(i, 2)
        d_wait(slot)

        @pl.when(i > 0)
        def _():
            rs_send(2 * i - 2)
            rs_send(2 * i - 1)

        r = mm(U[...], wdb[slot])
        for q in range(2):
            acc[2 * i + q] = r[:, q * LN:(q + 1) * LN]

        @pl.when(i + 2 < NP // 2)
        def _():
            d_start(i + 2, slot)
        return c

    lax.fori_loop(0, NP // 2, down, 0)

    def add(k, c):
        c_opA(k).wait_recv()
        acc[KP + k, 0:hf, :] += RA[k]
        c_upA(k).start()
        c_opB(k).wait_recv()
        acc[2 * KP + k, hf:n, :] += RB[k]
        c_dnB(k).start()
        return c

    lax.fori_loop(0, KP, add, 0)

    for k in range(KP):
        c_upB(k).wait_recv()
        c_dnA(k).wait_recv()
        c_upA(k).wait_recv()
        c_dnB(k).wait_recv()
        s = acc[3 * KP + k] + RD[k] + RU[k]
        v = xm[:, k * LN:(k + 1) * LN] + s.astype(jnp.bfloat16)
        XF[:, pl.ds(pl.multiple_of(t * dt + k * LN, LN), LN)] = v
        gx.send(k)
    for k in range(KP):
        gx.wait('up', k)
        gx.wait('dn', k)
    for k in range(KP):
        gx.wait('op', k)
    o = pltpu.make_async_copy(XF, out_ref, lsem.at[0])
    o.start()
    gx.done()
    for k in range(KP):
        for cp in (c_opA, c_opB, c_upB, c_dnA, c_upA, c_dnB):
            cp(k).wait_send()
    o.wait()


def mlp(T, layer, attn, x, wo_g, g, wg, wu, wd, cid):
    n, d = x.shape
    F = wg.shape[2]
    dt = d // T
    KP = dt // LN
    FP = F // LN
    hf = n // 2
    NG = T * KP // 4
    f32, bf = jnp.float32, jnp.bfloat16
    anyspec = pl.BlockSpec(memory_space=pltpu.HBM)
    D = pltpu.SemaphoreType.DMA
    return pl.pallas_call(
        functools.partial(mlp_kernel, T, layer),
        out_shape=jax.ShapeDtypeStruct((n, d), bf),
        in_specs=[anyspec, anyspec, anyspec, pl.BlockSpec(memory_space=pltpu.VMEM), anyspec, anyspec, anyspec],
        out_specs=anyspec,
        scratch_shapes=[
            pltpu.VMEM((2 * FP, n, LN), f32),
            pltpu.VMEM((3, 4 * LN, F), bf),
            pltpu.VMEM((NG, n, 4 * LN), bf),
            pltpu.VMEM((n, F), bf),
            pltpu.VMEM((2, F, 2 * LN), bf),
            pltpu.VMEM((KP, hf, LN), f32),
            pltpu.VMEM((KP, hf, LN), f32),
            pltpu.VMEM((KP, n, LN), f32),
            pltpu.VMEM((KP, n, LN), f32),
            pltpu.VMEM((n, d), bf),
            pltpu.VMEM((n, dt), bf),
            pltpu.VMEM((8, n), f32),
            pltpu.VMEM((3, 8, n), f32),
            D((4, KP)), D((4, KP)), D((6, KP)), D((6, KP)), D((3,)), D((3,)),
            D((2,)), D((3,)), D((NG,)), D((2,)), D((NG,)),
        ],
        compiler_params=pltpu.CompilerParams(vmem_limit_bytes=61 * 2 ** 20, collective_id=cid, has_side_effects=True),
        cost_estimate=pl.CostEstimate(flops=2 * n * d * (3 * F + dt), bytes_accessed=2 * d * (3 * F + dt), transcendentals=n * F),
        name="mlp",
    )(attn, x, wo_g, g, wg, wu, wd)


def solution(mesh):
    sp = mesh.shape['sp']
    tp = mesh.shape['tp']
    row = ('dp', 'sp')
    kv_spec = P(None, row, 'tp', None)
    col = P(None, None, 'tp')
    rowsplit = P(None, 'tp', None)

    def body(x, pos, k_hist, v_hist, wq, wk, wv, wo, wg, wu, wd, g1, g2):
        n, d = x.shape
        layers, hc, kvl, dh = k_hist.shape
        dt = d // tp
        tt, ss = lax.axis_index('tp'), lax.axis_index('sp')
        kp = dt // LN
        sr = LN // sp
        wr = lax.dynamic_index_in_dim(wo.reshape(layers, kp, sp, sr, d), ss, axis=2, keepdims=False)

        def wcols(t):
            return lax.dynamic_slice_in_dim(wr, t * dt, dt, axis=3)

        parts = jnp.zeros((tp,) + wcols(0).shape, wo.dtype)
        parts = lax.dynamic_update_index_in_dim(parts, wcols(tt), tt, 0)
        for j in range(1, tp):
            got = lax.ppermute(wcols(lax.rem(tt + j, tp)), 'tp', [(i, (i + j) % tp) for i in range(tp)])
            parts = lax.dynamic_update_index_in_dim(parts, got, lax.rem(tt + tp - j, tp), 0)
        wo_g = lax.all_gather(parts, 'sp', axis=0)
        kh, vh = k_hist.reshape(layers, hc, dh), v_hist.reshape(layers, hc, dh)
        half = dh // 2
        inv = ROPE_THETA ** (-(jnp.arange(half, dtype=jnp.float32) * (2.0 / dh)))
        ang = pos.astype(jnp.float32)[:, None] * inv
        cos, sin = jnp.cos(ang), jnp.sin(ang)
        cos = jnp.concatenate([cos, cos], axis=1)
        sin = jnp.concatenate([-sin, sin], axis=1)
        ks, vs = [], []
        for l in range(layers):
            attn, k, v = attention(tp, sp, l, x, cos, sin, kh, vh, wq, wk, wv, g1[l:l + 1], 2 * l)
            ks.append(k.reshape(n, kvl, dh))
            vs.append(v.reshape(n, kvl, dh))
            x = mlp(tp, l, attn, x, wo_g, g2[l:l + 1], wg, wu, wd, 2 * l + 1)
        return x, jnp.stack(ks), jnp.stack(vs)

    in_specs = (P(row, None), P(row), kv_spec, kv_spec, col, col, col, rowsplit, col, col, rowsplit, P(), P())
    out_specs = (P(row, None), kv_spec, kv_spec)
    return jax.shard_map(body, mesh=mesh, in_specs=in_specs, out_specs=out_specs, check_vma=False)
```

```python
import functools

import jax
import jax.numpy as jnp
from jax import lax
from jax.experimental import pallas as pl
from jax.experimental.pallas import tpu as pltpu
from jax.sharding import PartitionSpec as P

EPS = 1e-5
ROPE_THETA = 500000.0
LOG2E = 1.4426950408889634
MESH = pl.DeviceIdType.MESH
LN = 128


def mm(a, b):
    return jnp.dot(a, b, preferred_element_type=jnp.float32)


def attn_kernel(T, SP, layer, x_ref, cos_ref, sin_ref, kh_ref, vh_ref, wq_ref, wk_ref, wv_ref, wo_ref, g_ref, g2_ref,
                ho_ref, xo_ref, ko_ref, vo_ref,
                xb, wb, kv, qb, m_ref, l_ref, acc_ref, ga, wob, xm, hb, st, strv,
                kvs, kvr, gas, gar, wys, wyr, sts, strs, lsem, hsem, wsem):
    n, d = xb.shape
    w = qb.shape[1]
    dh = kv.shape[3]
    heads = w // dh
    X = SP // 2
    C = kv.shape[2]
    hc = C // 2
    dt = w
    nt = 4
    R = n // nt
    scale = dh ** -0.5 * LOG2E
    me = lax.axis_index("sp")
    t = lax.axis_index("tp")
    c = lax.rem(me, 2)
    xx = me // 2
    lx, rx, ox = lax.rem(xx + X - 1, X), lax.rem(xx + 1, X), lax.rem(xx + 2, X)
    left, right, part = lx * 2 + c, rx * 2 + c, xx * 2 + 1 - c
    up, dn, far = lax.rem(t + 1, T), lax.rem(t + T - 1, T), lax.rem(t + 2, T)

    barrier = pltpu.get_barrier_semaphore()
    for dev in ({"sp": left}, {"sp": right}, {"sp": part}, {"tp": up}, {"tp": dn}, {"tp": far}):
        pl.semaphore_signal(barrier, inc=1, device_id=dev, device_id_type=MESH)

    def hist_in(j):
        return pltpu.make_async_copy((kh_ref, vh_ref)[j].at[layer], kv.at[xx, j, pl.ds(c * hc, hc), :], hsem)

    for j in range(2):
        hist_in(j).start()
    xin = pltpu.make_async_copy(x_ref, xb, lsem.at[0])
    xin.start()
    win = [pltpu.make_async_copy(wk_ref.at[layer], wb.at[:, 0:dh], wsem.at[0]),
           pltpu.make_async_copy(wv_ref.at[layer], wb.at[:, dh:2 * dh], wsem.at[0]),
           pltpu.make_async_copy(wq_ref.at[layer], wb.at[:, 2 * dh:], wsem.at[1])]
    for cp in win:
        cp.start()

    def wo_cols(dev):
        return wo_ref.at[layer, :, me, :, pl.ds(pl.multiple_of(dev * dt, LN), dt)]

    wo_own = pltpu.make_async_copy(wo_cols(t), wob.at[t, :, me], wsem.at[2])
    wo_own.start()
    xcol = pltpu.make_async_copy(x_ref.at[:, pl.ds(pl.multiple_of(t * dt, LN), dt)], xm, lsem.at[1])
    xcol.start()
    peers = ((0, up, dn), (1, dn, up), (2, far, far))

    def wo_tx(j, dev):
        return pltpu.make_async_remote_copy(src_ref=wo_cols(dev), dst_ref=wob.at[t, :, me], send_sem=wys.at[j],
                                            recv_sem=wyr.at[j], device_id={"tp": dev}, device_id_type=MESH)

    def wo_rx(j, src):
        pltpu.make_async_remote_copy(src_ref=wob.at[src, :, me], dst_ref=wob.at[src, :, me], send_sem=wys.at[j],
                                     recv_sem=wyr.at[j], device_id={"tp": src}, device_id_type=MESH).wait_recv()

    def region(kind, chip, core, half):
        if kind == 2:
            if half is None:
                return wob.at[:, :, chip * 2 + core]
            return wob.at[pl.ds(half * (T // 2), T // 2), :, chip * 2 + core]
        if kind == 0:
            blk, base, ln = chip, core * hc, hc
        else:
            blk, base, ln = X + chip // 2, lax.rem(chip, 2) * (2 * n) + core * n, n
        if half is not None:
            ln = ln // 2
            base = base + half * ln
        return kv.at[blk, :, pl.ds(pl.multiple_of(base, ln), ln), :]

    sent = [(xx, c, None, right), (xx, c, None, left), (xx, c, None, part), (lx, c, 0, right), (rx, c, 1, left),
            (lx, c, None, part), (rx, c, None, part), (ox, c, 0, part), (ox, c, 1, part)]
    got = [(lx, c, None), (rx, c, None), (xx, 1 - c, None), (ox, c, 0), (ox, c, 1),
           (lx, 1 - c, None), (rx, 1 - c, None), (ox, 1 - c, 0), (ox, 1 - c, 1)]

    def tx(kind, i):
        chip, core, half, dev = sent[i]
        r = region(kind, chip, core, half)
        return pltpu.make_async_remote_copy(src_ref=r, dst_ref=r, send_sem=kvs.at[kind, i], recv_sem=kvr.at[kind, i],
                                            device_id={"sp": dev}, device_id_type=MESH)

    def rx_wait(kind, i):
        chip, core, half = got[i]
        r = region(kind, chip, core, half)
        pltpu.make_async_remote_copy(src_ref=r, dst_ref=r, send_sem=kvs.at[kind, i], recv_sem=kvr.at[kind, i],
                                     device_id={"sp": part}, device_id_type=MESH).wait_recv()

    def send_own(kind):
        for i in (0, 1, 2):
            tx(kind, i).start()

    def pass_near(kind):
        rx_wait(kind, 0)
        tx(kind, 3).start()
        tx(kind, 5).start()
        rx_wait(kind, 1)
        tx(kind, 4).start()
        tx(kind, 6).start()

    def pass_far(kind):
        rx_wait(kind, 3)
        tx(kind, 7).start()
        rx_wait(kind, 4)
        tx(kind, 8).start()

    pl.semaphore_wait(barrier, 6)
    for j in range(2):
        hist_in(j).wait()
    send_own(0)
    for j, dev, _ in peers:
        wo_tx(j, dev).start()

    xin.wait()
    g = g_ref[...].astype(jnp.float32)
    NR = min(32, n)

    def norm(i, carry):
        rows = pl.ds(pl.multiple_of(i * NR, NR), NR)
        xf = xb[rows, :].astype(jnp.float32)
        r = lax.rsqrt(jnp.sum(xf * xf, axis=1, keepdims=True) / d + EPS)
        xb[rows, :] = (xf * r * g).astype(jnp.bfloat16)
        return carry

    lax.fori_loop(0, n // NR, norm, 0)

    def rope(a):
        a = a.astype(jnp.bfloat16).astype(jnp.float32)
        return (a * cos_ref[...] + pltpu.roll(a, dh // 2, 1) * sin_ref[...]).astype(jnp.bfloat16)

    win[0].wait()
    win[1].wait()
    r = mm(xb[...], wb[:, :2 * dh])
    own = pl.ds(pl.multiple_of(lax.rem(xx, 2) * (2 * n) + c * n, n), n)
    kv[X + xx // 2, 0, own, :] = rope(r[:, :dh])
    kv[X + xx // 2, 1, own, :] = r[:, dh:].astype(jnp.bfloat16)
    win[2].wait()

    def qpair(i, carry):
        @pl.when(i == 1)
        def _():
            send_own(1)

        r = mm(xb[...], wb[:, pl.ds(pl.multiple_of((i + 1) * 2 * dh, 2 * dh), 2 * dh)])
        for j in range(2):
            qb[:, pl.ds(pl.multiple_of((2 * i + j) * dh, dh), dh)] = rope(r[:, j * dh:(j + 1) * dh])
        return carry

    lax.fori_loop(0, heads // 2, qpair, 0)
    if heads // 2 < 2:
        send_own(1)
    if heads % 2:
        qb[:, (heads - 1) * dh:] = rope(mm(xb[...], wb[:, (heads + 1) * dh:]))

    def kv_out(j):
        return pltpu.make_async_copy(kv.at[X + xx // 2, j, own, :], (ko_ref, vo_ref)[j], hsem)

    for j in range(2):
        kv_out(j).start()

    def init(i, carry):
        rows = pl.ds(pl.multiple_of(i * R, R), R)
        for h in range(heads):
            m_ref[h, rows, :] = jnp.full((R, LN), -1e30, jnp.float32)
            l_ref[h, rows, :] = jnp.zeros((R, LN), jnp.float32)
            acc_ref[h, rows, :] = jnp.zeros((R, dh), jnp.float32)
        return carry

    lax.fori_loop(0, nt, init, 0)

    def unit(tile, blk, mask):
        rows = pl.ds(pl.multiple_of(tile * R, R), R)

        def qk(h):
            return lax.dot_general(qb[rows, h * dh:(h + 1) * dh], kv[blk, 0], (((1,), (1,)), ((), ())),
                                   preferred_element_type=jnp.float32)

        def pv(h, p, alpha):
            acc_ref[h, rows, :] = acc_ref[h, rows, :] * alpha + mm(p, kv[blk, 1])

        s = qk(0)
        pend = None
        for h in range(heads):
            s_next = qk(h + 1) if h + 1 < heads else None
            if pend is not None:
                pv(*pend)
            if mask is not None:
                s = jnp.where(mask, s, -jnp.inf)
            m_old = m_ref[h, rows, :]
            m_new = jnp.maximum(m_old, jnp.max(s, axis=1, keepdims=True) * scale)
            alpha = jnp.exp2(m_old - m_new)
            p = jnp.exp2(s * scale - m_new[:, :1])
            ls = p[:, :LN]
            for j in range(1, C // LN):
                ls = ls + p[:, j * LN:(j + 1) * LN]
            l_ref[h, rows, :] = l_ref[h, rows, :] * alpha + ls
            m_ref[h, rows, :] = m_new
            pend = (h, p.astype(jnp.bfloat16), alpha)
            s = s_next
        pv(*pend)

    hR = R // 2

    def gx(i, tile):
        base = pl.multiple_of(tile * R, R)
        owner, off, ln, dev = ((t, 0, R, up), (t, 0, R, dn), (dn, 0, hR, up), (up, hR, hR, dn))[i]
        ref = ga.at[owner, pl.ds(pl.multiple_of(base + off, hR), ln), :]
        return pltpu.make_async_remote_copy(src_ref=ref, dst_ref=ref, send_sem=gas.at[i, tile], recv_sem=gar.at[i, tile],
                                            device_id={"tp": dev}, device_id_type=MESH)

    def g_wait(i, tile):
        base = pl.multiple_of(tile * R, R)
        owner, off, ln = ((dn, 0, R), (up, 0, R), (far, 0, hR), (far, hR, hR))[i]
        ref = ga.at[owner, pl.ds(pl.multiple_of(base + off, hR), ln), :]
        pltpu.make_async_remote_copy(src_ref=ref, dst_ref=ref, send_sem=gas.at[i, tile], recv_sem=gar.at[i, tile],
                                     device_id={"tp": up}, device_id_type=MESH).wait_recv()

    def g_pass(tile):
        g_wait(0, tile)
        gx(2, tile).start()
        g_wait(1, tile)
        gx(3, tile).start()

    def finish(tile):
        rows = pl.ds(pl.multiple_of(tile * R, R), R)
        for h in range(heads):
            l = jnp.sum(l_ref[h, rows, :], axis=1, keepdims=True)
            ga[t, rows, h * dh:(h + 1) * dh] = (acc_ref[h, rows, :] / l).astype(jnp.bfloat16)

    def tile_rows(tile):
        return pl.ds(pl.multiple_of(tile * R, R), R)

    def s_copy(j, dev, tile):
        return pltpu.make_async_remote_copy(src_ref=st.at[tile], dst_ref=strv.at[j, tile], send_sem=sts.at[j, tile],
                                            recv_sem=strs.at[j, tile], device_id={"tp": dev}, device_id_type=MESH)

    def wo_tile(tile):
        g_wait(2, tile)
        g_wait(3, tile)
        rows = tile_rows(tile)
        a = jnp.concatenate([ga[j, rows, :] for j in range(T)], axis=1)
        y = mm(a, wob[...].reshape(d, dt))
        v = xm[rows, :] + y.astype(jnp.bfloat16)
        xm[rows, :] = v
        vf = v.astype(jnp.float32)
        sb = jnp.broadcast_to(jnp.sum(vf * vf, axis=1, keepdims=True), (R, LN))
        st[tile] = jnp.swapaxes(sb, 0, 1)[:8]
        for j, dev, _ in peers:
            s_copy(j, dev, tile).start()

    def h_tile(tile):
        rows = tile_rows(tile)
        for j, dev, _ in peers:
            s_copy(j, dev, tile).wait_recv()
        tot = st[tile] + strv[0, tile] + strv[1, tile] + strv[2, tile]
        r8 = lax.rsqrt(tot / d + EPS)
        rb = jnp.swapaxes(jnp.concatenate([r8] * (LN // 8), axis=0), 0, 1)
        for k in range(dt // LN):
            cols = slice(k * LN, (k + 1) * LN)
            gk = g2_ref[0:1, pl.ds(pl.multiple_of(t * dt + k * LN, LN), LN)].astype(jnp.float32)
            hb[rows, cols] = (xm[rows, cols].astype(jnp.float32) * rb * gk).astype(jnp.bfloat16)

    rx_wait(0, 2)
    first = 3 * nt
    per = 1 + xx // 2
    total = first + nt * per

    def near(kind):
        pass_near(kind)
        if kind == 1:
            wo_own.wait()
            for j, _, src in peers:
                wo_rx(j, src)
            send_own(2)

    points = ((2, near, 0), (nt, near, 1), (2 * nt - 1, pass_far, 0), (2 * nt, pass_far, 1), (first + 2, near, 2))

    def post(stage):
        @pl.when(jnp.logical_and(stage >= 1, stage <= nt))
        def _():
            g_pass(stage - 1)

        @pl.when(stage == 2)
        def _():
            pass_far(2)
            for gid in (2, 5, 6, 7, 8):
                rx_wait(2, gid)
            xcol.wait()

        @pl.when(jnp.logical_and(stage >= 2, stage <= nt + 1))
        def _():
            wo_tile(stage - 2)

        @pl.when(stage >= 3)
        def _():
            h_tile(stage - 3)

    def step(i, carry):
        for at, fn, kind in points:
            @pl.when(i == at)
            def _():
                fn(kind)

        for chip_at, gid in ((nt, 5), (2 * nt, 6)):
            @pl.when(i == chip_at)
            def _():
                rx_wait(0, gid)

        @pl.when(i == first)
        def _():
            rx_wait(0, 7)
            rx_wait(0, 8)
            for gid in (2, 5, 6, 7, 8):
                rx_wait(1, gid)

        late = i >= first
        i2 = jnp.maximum(i - first, 0)
        m = lax.rem(i2, per)
        tile = jnp.where(late, i2 // per, lax.rem(i, nt))
        early = jnp.where(i < nt, xx, jnp.where(i < 2 * nt, lx, rx))
        blk = jnp.where(late, jnp.where(m == 0, ox, X + m - 1), early)
        live = i < total
        last = jnp.logical_and(jnp.logical_and(late, live), m == per - 1)

        @pl.when(live)
        def _():
            unit(tile, blk, None)

        @pl.when(last)
        def _():
            off = lax.rem(xx, 2) * (2 * n) + c * n + tile * R
            row = lax.broadcasted_iota(jnp.int32, (R, C), 0) + off
            unit(tile, X + xx // 2, lax.broadcasted_iota(jnp.int32, (R, C), 1) <= row)
            finish(tile)
            gx(0, tile).start()
            gx(1, tile).start()

        @pl.when(jnp.logical_or(last, jnp.logical_not(live)))
        def _():
            post(jnp.where(live, tile, nt + i - total))
        return carry

    lax.fori_loop(0, total + 3, step, 0)
    o1 = pltpu.make_async_copy(hb, ho_ref, lsem.at[0])
    o2 = pltpu.make_async_copy(xm, xo_ref, lsem.at[1])
    o1.start()
    o2.start()
    for tile in range(nt):
        for i in range(4):
            gx(i, tile).wait_send()
        for j, dev, _ in peers:
            s_copy(j, dev, tile).wait_send()
    for j, dev, _ in peers:
        wo_tx(j, dev).wait_send()
    for kind in range(3):
        for i in range(9):
            tx(kind, i).wait_send()
    for j in range(2):
        kv_out(j).wait()
    o1.wait()
    o2.wait()


def attention(T, SP, layer, x, cos, sin, kh, vh, wq, wk, wv, wo, g, g2, cid):
    n, d = x.shape
    w = wq.shape[2]
    hc, dh = kh.shape[1], kh.shape[2]
    heads = w // dh
    X = SP // 2
    assert 2 * hc == 4 * n and wk.shape[2] == dh and w * T == d
    R = n // 4
    f32, bf = jnp.float32, jnp.bfloat16
    hbm = pl.BlockSpec(memory_space=pltpu.HBM)
    vm = pl.BlockSpec(memory_space=pltpu.VMEM)
    D = pltpu.SemaphoreType.DMA
    keys = SP * (hc + n // 2)
    return pl.pallas_call(
        functools.partial(attn_kernel, T, SP, layer),
        out_shape=[jax.ShapeDtypeStruct((n, w), bf), jax.ShapeDtypeStruct((n, w), bf),
                   jax.ShapeDtypeStruct((n, dh), bf), jax.ShapeDtypeStruct((n, dh), bf)],
        in_specs=[hbm, vm, vm, hbm, hbm, hbm, hbm, hbm, hbm, vm, vm],
        out_specs=[hbm, hbm, hbm, hbm],
        scratch_shapes=[
            pltpu.VMEM((n, d), bf),
            pltpu.VMEM((d, w + 2 * dh), bf),
            pltpu.VMEM((X + X // 2, 2, 2 * hc, dh), bf),
            pltpu.VMEM((n, w), bf),
            pltpu.VMEM((heads, n, LN), f32),
            pltpu.VMEM((heads, n, LN), f32),
            pltpu.VMEM((heads, n, dh), f32),
            pltpu.VMEM((T, n, w), bf),
            pltpu.VMEM((T, w // LN, SP, LN // SP, w), bf),
            pltpu.VMEM((n, w), bf),
            pltpu.VMEM((n, w), bf),
            pltpu.VMEM((4, 8, R), f32),
            pltpu.VMEM((3, 4, 8, R), f32),
            D((3, 9)), D((3, 9)), D((4, 4)), D((4, 4)), D((3,)), D((3,)), D((3, 4)), D((3, 4)), D((2,)), D, D((3,)),
        ],
        compiler_params=pltpu.CompilerParams(vmem_limit_bytes=61 * 2 ** 20, collective_id=cid, has_side_effects=True),
        cost_estimate=pl.CostEstimate(flops=4 * n * w * keys + 2 * n * d * (w + 2 * dh), bytes_accessed=4 * keys * dh,
                                      transcendentals=n * heads * keys),
        name="attention",
    )(x, cos, sin, kh, vh, wq, wk, wv, wo.reshape(wo.shape[0], w // LN, SP, LN // SP, d), g, g2)


def mlp_kernel(T, layer, h_ref, x_ref, wg_ref, wu_ref, wd_ref, out_ref,
               acc, ring, H, U, wdb, RA, RB, RD, RU, XF, xm,
               ags, agr, rss, rsr, lsem, wsem, dsem):
    n, d = XF.shape
    dt = d // T
    KP = dt // LN
    NP = T * KP
    NG = NP // 4
    F = U.shape[1]
    FP = F // LN
    t = lax.axis_index("tp")
    up = lax.rem(t + 1, T)
    dn = lax.rem(t + 3, T)
    op = lax.rem(t + 2, T)
    hf = n // 2
    ALL, A, B = pl.ds(0, n), pl.ds(0, hf), pl.ds(hf, hf)

    barrier = pltpu.get_barrier_semaphore()
    for dev in (up, dn, op):
        pl.semaphore_signal(barrier, inc=1, device_id={"tp": dev}, device_id_type=MESH)

    def rcopy(src, dst, ss, rs, dev):
        return pltpu.make_async_remote_copy(src_ref=src, dst_ref=dst, send_sem=ss, recv_sem=rs,
                                            device_id={"tp": dev}, device_id_type=MESH)

    def pos_of(kind, k):
        return {'own': k, 'up': KP + 2 * k, 'dn': KP + 2 * k + 1, 'op': 3 * KP + k}[kind]

    order = [None] * NP
    for kind in ('own', 'up', 'dn', 'op'):
        for k in range(KP):
            order[pos_of(kind, k)] = (kind, k)
    owner_of = {'own': t, 'up': up, 'dn': dn, 'op': op}

    def hloc(kind, owner, k, rows):
        p = pos_of(kind, k)
        return H.at[p // 4, rows, pl.ds((p % 4) * LN, LN)]

    def xloc(kind, owner, k, rows):
        return XF.at[rows, pl.ds(pl.multiple_of(owner * dt + k * LN, LN), LN)]

    class Gather:
        def __init__(self, loc):
            self.loc = loc

        def c_up(self, k):
            return rcopy(self.loc('own', t, k, ALL), self.loc('dn', t, k, ALL), ags.at[0, k], agr.at[0, k], up)

        def c_dn(self, k):
            return rcopy(self.loc('own', t, k, ALL), self.loc('up', t, k, ALL), ags.at[1, k], agr.at[1, k], dn)

        def r_up(self, k):
            return rcopy(self.loc('dn', dn, k, A), self.loc('op', dn, k, A), ags.at[2, k], agr.at[2, k], up)

        def r_dn(self, k):
            return rcopy(self.loc('up', up, k, B), self.loc('op', up, k, B), ags.at[3, k], agr.at[3, k], dn)

        def send(self, k):
            self.c_up(k).start()
            self.c_dn(k).start()

        def wait(self, kind, k):
            if kind == 'dn':
                rcopy(self.loc('dn', dn, k, ALL), self.loc('dn', dn, k, ALL), ags.at[0, k], agr.at[0, k], up).wait_recv()
                self.r_up(k).start()
            elif kind == 'up':
                rcopy(self.loc('up', up, k, ALL), self.loc('up', up, k, ALL), ags.at[1, k], agr.at[1, k], dn).wait_recv()
                self.r_dn(k).start()
            elif kind == 'op':
                rcopy(self.loc('op', op, k, A), self.loc('op', op, k, A), ags.at[2, k], agr.at[2, k], up).wait_recv()
                rcopy(self.loc('op', op, k, B), self.loc('op', op, k, B), ags.at[3, k], agr.at[3, k], dn).wait_recv()

        def done(self):
            for k in range(KP):
                self.c_up(k).wait_send()
                self.c_dn(k).wait_send()
                self.r_up(k).wait_send()
                self.r_dn(k).wait_send()

    gh = Gather(hloc)
    gx = Gather(xloc)

    def wait_group(gather, j):
        for kind, k in order[4 * j:4 * j + 4]:
            gather.wait(kind, k)

    def h_in(k):
        return pltpu.make_async_copy(h_ref.at[:, pl.ds(k * LN, LN)], hloc('own', t, k, ALL), lsem.at[0])

    for k in range(KP):
        h_in(k).start()
    xin = pltpu.make_async_copy(x_ref, xm, lsem.at[1])
    xin.start()

    def w_copy(i, q, slot):
        p = (i // 2) * 4 + q
        own = p < KP
        pair = jnp.logical_and(p >= KP, p < 3 * KP)
        k = jnp.where(own, p, jnp.where(pair, (p - KP) // 2, p - 3 * KP))
        who = jnp.where(own, t, jnp.where(pair, jnp.where(lax.rem(p - KP, 2) == 0, up, dn), op))
        row = pl.multiple_of(who * dt + k * LN, LN)
        return row

    def w_start(i, slot):
        for q in range(4):
            row = w_copy(i, q, slot)
            dst = ring.at[slot, pl.ds(q * LN, LN), :]

            @pl.when(lax.rem(i, 2) == 0)
            def _():
                pltpu.make_async_copy(wg_ref.at[layer, pl.ds(row, LN), :], dst, wsem.at[slot]).start()

            @pl.when(lax.rem(i, 2) == 1)
            def _():
                pltpu.make_async_copy(wu_ref.at[layer, pl.ds(row, LN), :], dst, wsem.at[slot]).start()

    def w_wait(slot):
        pltpu.make_async_copy(wg_ref.at[layer, pl.ds(0, 4 * LN), :], ring.at[slot], wsem.at[slot]).wait()

    NSLOT = ring.shape[0]
    for s in range(NSLOT):
        w_start(jnp.int32(s), s)
    for k in range(KP):
        h_in(k).wait()
    pl.semaphore_wait(barrier, 3)
    for k in range(KP):
        gh.send(k)

    def zero(j, c):
        acc[j] = jnp.zeros(acc.shape[1:], acc.dtype)
        return c

    lax.fori_loop(0, 2 * FP, zero, 0)

    def gu_step(i, c):
        j = i // 2
        slot = lax.rem(i, NSLOT)
        for jj in range(NG):
            @pl.when(i == 2 * jj)
            def _():
                wait_group(gh, jj)
        w_wait(slot)
        base = lax.rem(i, 2) * FP
        for f in range(0, FP, 4):
            m = min(4, FP - f)
            r = mm(H[j], ring[slot, :, f * LN:(f + m) * LN])
            for q in range(m):
                acc[base + f + q] += r[:, q * LN:(q + 1) * LN]

        @pl.when(i + NSLOT < 2 * NG)
        def _():
            w_start(i + NSLOT, slot)
        return c

    def d_col(p):
        c = p // KP
        who = jnp.where(c == 0, op, jnp.where(c == 1, up, jnp.where(c == 2, dn, t)))
        return pl.multiple_of(who * dt + lax.rem(p, KP) * LN, LN)

    def d_start(i, slot):
        for q in range(2):
            pltpu.make_async_copy(wd_ref.at[layer, :, pl.ds(d_col(2 * i + q), LN)],
                                  wdb.at[slot, :, pl.ds(q * LN, LN)], dsem.at[slot]).start()

    def d_wait(slot):
        pltpu.make_async_copy(wd_ref.at[layer, :, pl.ds(0, 2 * LN)], wdb.at[slot], dsem.at[slot]).wait()

    d_start(jnp.int32(0), 0)
    d_start(jnp.int32(1), 1)
    lax.fori_loop(0, 2 * NG, gu_step, 0)

    def silu(f, c):
        a = acc[f].astype(jnp.bfloat16).astype(jnp.float32)
        b = acc[FP + f].astype(jnp.bfloat16).astype(jnp.float32)
        U[:, pl.ds(pl.multiple_of(f * LN, LN), LN)] = (a * (1.0 / (1.0 + jnp.exp(-a))) * b).astype(jnp.bfloat16)
        return c

    lax.fori_loop(0, FP, silu, 0)
    gh.done()

    def c_opA(k):
        return rcopy(acc.at[k, A, :], RA.at[k], rss.at[0, k], rsr.at[0, k], up)

    def c_opB(k):
        return rcopy(acc.at[k, B, :], RB.at[k], rss.at[1, k], rsr.at[1, k], dn)

    def c_upB(k):
        return rcopy(acc.at[KP + k, B, :], RD.at[k, B, :], rss.at[2, k], rsr.at[2, k], up)

    def c_dnA(k):
        return rcopy(acc.at[2 * KP + k, A, :], RU.at[k, A, :], rss.at[3, k], rsr.at[3, k], dn)

    def c_upA(k):
        return rcopy(acc.at[KP + k, A, :], RD.at[k, A, :], rss.at[4, k], rsr.at[4, k], up)

    def c_dnB(k):
        return rcopy(acc.at[2 * KP + k, B, :], RU.at[k, B, :], rss.at[5, k], rsr.at[5, k], dn)

    def rs_send(p):
        c = p // KP
        k = lax.rem(p, KP)

        @pl.when(c == 0)
        def _():
            c_opA(k).start()
            c_opB(k).start()

        @pl.when(c == 1)
        def _():
            c_upB(k).start()

        @pl.when(c == 2)
        def _():
            c_dnA(k).start()

    def down(i, c):
        slot = lax.rem(i, 2)
        d_wait(slot)

        @pl.when(i > 0)
        def _():
            rs_send(2 * i - 2)
            rs_send(2 * i - 1)

        r = mm(U[...], wdb[slot])
        for q in range(2):
            acc[2 * i + q] = r[:, q * LN:(q + 1) * LN]

        @pl.when(i + 2 < NP // 2)
        def _():
            d_start(i + 2, slot)
        return c

    lax.fori_loop(0, NP // 2, down, 0)

    def add(k, c):
        c_opA(k).wait_recv()
        acc[KP + k, 0:hf, :] += RA[k]
        c_upA(k).start()
        c_opB(k).wait_recv()
        acc[2 * KP + k, hf:n, :] += RB[k]
        c_dnB(k).start()
        return c

    lax.fori_loop(0, KP, add, 0)

    xin.wait()
    for k in range(KP):
        c_upB(k).wait_recv()
        c_dnA(k).wait_recv()
        c_upA(k).wait_recv()
        c_dnB(k).wait_recv()
        s = acc[3 * KP + k] + RD[k] + RU[k]
        v = xm[:, k * LN:(k + 1) * LN] + s.astype(jnp.bfloat16)
        XF[:, pl.ds(pl.multiple_of(t * dt + k * LN, LN), LN)] = v
        gx.send(k)
    for k in range(KP):
        gx.wait('up', k)
        gx.wait('dn', k)
    for k in range(KP):
        gx.wait('op', k)
    o = pltpu.make_async_copy(XF, out_ref, lsem.at[0])
    o.start()
    gx.done()
    for k in range(KP):
        for cp in (c_opA, c_opB, c_upB, c_dnA, c_upA, c_dnB):
            cp(k).wait_send()
    o.wait()


def mlp(T, layer, h, x, wg, wu, wd, cid):
    n, dt = x.shape
    F = wg.shape[2]
    d = dt * T
    KP = dt // LN
    FP = F // LN
    hf = n // 2
    NG = T * KP // 4
    f32, bf = jnp.float32, jnp.bfloat16
    anyspec = pl.BlockSpec(memory_space=pltpu.HBM)
    D = pltpu.SemaphoreType.DMA
    return pl.pallas_call(
        functools.partial(mlp_kernel, T, layer),
        out_shape=jax.ShapeDtypeStruct((n, d), bf),
        in_specs=[anyspec] * 5,
        out_specs=anyspec,
        scratch_shapes=[
            pltpu.VMEM((2 * FP, n, LN), f32),
            pltpu.VMEM((3, 4 * LN, F), bf),
            pltpu.VMEM((NG, n, 4 * LN), bf),
            pltpu.VMEM((n, F), bf),
            pltpu.VMEM((2, F, 2 * LN), bf),
            pltpu.VMEM((KP, hf, LN), f32),
            pltpu.VMEM((KP, hf, LN), f32),
            pltpu.VMEM((KP, n, LN), f32),
            pltpu.VMEM((KP, n, LN), f32),
            pltpu.VMEM((n, d), bf),
            pltpu.VMEM((n, dt), bf),
            D((4, KP)), D((4, KP)), D((6, KP)), D((6, KP)), D((2,)), D((3,)), D((2,)),
        ],
        compiler_params=pltpu.CompilerParams(vmem_limit_bytes=61 * 2 ** 20, collective_id=cid, has_side_effects=True),
        cost_estimate=pl.CostEstimate(flops=6 * n * d * F, bytes_accessed=6 * d * F, transcendentals=n * F),
        name="mlp",
    )(h, x, wg, wu, wd)


def solution(mesh):
    sp = mesh.shape['sp']
    tp = mesh.shape['tp']
    row = ('dp', 'sp')
    kv_spec = P(None, row, 'tp', None)
    col = P(None, None, 'tp')
    rowsplit = P(None, 'tp', None)

    def body(x, pos, k_hist, v_hist, wq, wk, wv, wo, wg, wu, wd, g1, g2):
        n, d = x.shape
        layers, hc, kvl, dh = k_hist.shape
        kh, vh = k_hist.reshape(layers, hc, dh), v_hist.reshape(layers, hc, dh)
        half = dh // 2
        inv = ROPE_THETA ** (-(jnp.arange(half, dtype=jnp.float32) * (2.0 / dh)))
        ang = pos.astype(jnp.float32)[:, None] * inv
        cos, sin = jnp.cos(ang), jnp.sin(ang)
        cos = jnp.concatenate([cos, cos], axis=1)
        sin = jnp.concatenate([-sin, sin], axis=1)
        ks, vs = [], []
        for l in range(layers):
            h, xm, k, v = attention(tp, sp, l, x, cos, sin, kh, vh, wq, wk, wv, wo, g1[l:l + 1], g2[l:l + 1], 2 * l)
            ks.append(k.reshape(n, kvl, dh))
            vs.append(v.reshape(n, kvl, dh))
            x = mlp(tp, l, h, xm, wg, wu, wd, 2 * l + 1)
        return x, jnp.stack(ks), jnp.stack(vs)

    in_specs = (P(row, None), P(row), kv_spec, kv_spec, col, col, col, rowsplit, col, col, rowsplit, P(), P())
    out_specs = (P(row, None), kv_spec, kv_spec)
    return jax.shard_map(body, mesh=mesh, in_specs=in_specs, out_specs=out_specs, check_vma=False)
```

```python
import functools

import jax
import jax.numpy as jnp
from jax import lax
from jax.experimental import pallas as pl
from jax.experimental.pallas import tpu as pltpu
from jax.sharding import PartitionSpec as P

EPS = 1e-5
ROPE_THETA = 500000.0
LOG2E = 1.4426950408889634
MESH = pl.DeviceIdType.MESH
LN = 128


def mm(a, b):
    return jnp.dot(a, b, preferred_element_type=jnp.float32)


def attn_kernel(T, SP, layer, x_ref, cos_ref, sin_ref, kh_ref, vh_ref, wq_ref, wk_ref, wv_ref, wo_ref, g_ref, g2_ref,
                ho_ref, xo_ref, ko_ref, vo_ref,
                xb, wb, kb, vt, vs, qb, m_ref, l_ref, acc_ref, ga, wob, xm, hb, st, strv,
                kvs, kvr, gas, gar, wys, wyr, sts, strs, lsem, hsem, wsem):
    n, d = xb.shape
    w = qb.shape[1]
    dh = kb.shape[2]
    heads = w // dh
    X = SP // 2
    C = kb.shape[1]
    hc = C // 2
    dt = w
    nt = 2
    R = n // nt
    NS = 2
    SR = R // NS
    scale = dh ** -0.5 * LOG2E
    me = lax.axis_index("sp")
    t = lax.axis_index("tp")
    c = lax.rem(me, 2)
    xx = me // 2
    lx, rx, ox = lax.rem(xx + X - 1, X), lax.rem(xx + 1, X), lax.rem(xx + 2, X)
    left, right, part = lx * 2 + c, rx * 2 + c, xx * 2 + 1 - c
    up, dn, far = lax.rem(t + 1, T), lax.rem(t + T - 1, T), lax.rem(t + 2, T)

    barrier = pltpu.get_barrier_semaphore()
    for dev in ({"sp": left}, {"sp": right}, {"sp": part}, {"tp": up}, {"tp": dn}, {"tp": far}):
        pl.semaphore_signal(barrier, inc=1, device_id=dev, device_id_type=MESH)

    hown = pl.ds(pl.multiple_of(c * hc, hc), hc)
    hist_in = (pltpu.make_async_copy(kh_ref.at[layer], kb.at[xx, hown, :], hsem.at[0]),
               pltpu.make_async_copy(vh_ref.at[layer], vs, hsem.at[1]))
    for cp in hist_in:
        cp.start()
    xin = pltpu.make_async_copy(x_ref, xb, lsem.at[0])
    xin.start()
    win = [pltpu.make_async_copy(wk_ref.at[layer], wb.at[:, 0:dh], wsem.at[0]),
           pltpu.make_async_copy(wv_ref.at[layer], wb.at[:, dh:2 * dh], wsem.at[0]),
           pltpu.make_async_copy(wq_ref.at[layer], wb.at[:, 2 * dh:], wsem.at[1])]
    for cp in win:
        cp.start()

    def wo_cols(dev):
        return wo_ref.at[layer, :, me, :, pl.ds(pl.multiple_of(dev * dt, LN), dt)]

    wo_own = pltpu.make_async_copy(wo_cols(t), wob.at[t, :, me], wsem.at[2])
    wo_own.start()
    xcol = pltpu.make_async_copy(x_ref.at[:, pl.ds(pl.multiple_of(t * dt, LN), dt)], xm, lsem.at[1])
    xcol.start()
    peers = ((0, up, dn), (1, dn, up), (2, far, far))

    def wo_tx(j, dev):
        return pltpu.make_async_remote_copy(src_ref=wo_cols(dev), dst_ref=wob.at[t, :, me], send_sem=wys.at[j],
                                            recv_sem=wyr.at[j], device_id={"tp": dev}, device_id_type=MESH)

    def wo_rx(j, src):
        pltpu.make_async_remote_copy(src_ref=wob.at[src, :, me], dst_ref=wob.at[src, :, me], send_sem=wys.at[j],
                                     recv_sem=wyr.at[j], device_id={"tp": src}, device_id_type=MESH).wait_recv()

    def region(kind, chip, core, half):
        if kind == 2:
            if half is None:
                return wob.at[:, :, chip * 2 + core]
            return wob.at[pl.ds(half * (T // 2), T // 2), :, chip * 2 + core]
        if kind % 3 == 0:
            blk, base, ln = chip, core * hc, hc
        else:
            blk, base, ln = X + chip // 2, lax.rem(chip, 2) * (2 * n) + core * n, n
        if half is not None:
            ln = ln // 2
            base = base + half * ln
        part_ = pl.ds(pl.multiple_of(base, ln), ln)
        return kb.at[blk, part_, :] if kind < 3 else vt.at[blk, :, part_]

    sent = [(xx, c, None, right), (xx, c, None, left), (xx, c, None, part), (lx, c, 0, right), (rx, c, 1, left),
            (lx, c, None, part), (rx, c, None, part), (ox, c, 0, part), (ox, c, 1, part)]
    got = [(lx, c, None), (rx, c, None), (xx, 1 - c, None), (ox, c, 0), (ox, c, 1),
           (lx, 1 - c, None), (rx, 1 - c, None), (ox, 1 - c, 0), (ox, 1 - c, 1)]

    def tx(kind, i):
        chip, core, half, dev = sent[i]
        r = region(kind, chip, core, half)
        return pltpu.make_async_remote_copy(src_ref=r, dst_ref=r, send_sem=kvs.at[kind, i], recv_sem=kvr.at[kind, i],
                                            device_id={"sp": dev}, device_id_type=MESH)

    def rx_wait(kind, i):
        chip, core, half = got[i]
        r = region(kind, chip, core, half)
        pltpu.make_async_remote_copy(src_ref=r, dst_ref=r, send_sem=kvs.at[kind, i], recv_sem=kvr.at[kind, i],
                                     device_id={"sp": part}, device_id_type=MESH).wait_recv()

    def send_own(kind):
        for i in (0, 1, 2):
            tx(kind, i).start()

    def pass_near(kind):
        rx_wait(kind, 0)
        tx(kind, 3).start()
        tx(kind, 5).start()
        rx_wait(kind, 1)
        tx(kind, 4).start()
        tx(kind, 6).start()

    def pass_far(kind):
        rx_wait(kind, 3)
        tx(kind, 7).start()
        rx_wait(kind, 4)
        tx(kind, 8).start()

    pl.semaphore_wait(barrier, 6)
    hist_in[0].wait()
    send_own(0)
    hist_in[1].wait()
    vt[xx, :, hown] = jnp.swapaxes(vs[...].astype(jnp.float32), 0, 1).astype(jnp.bfloat16)
    send_own(3)
    for j, dev, _ in peers:
        wo_tx(j, dev).start()

    xin.wait()
    g = g_ref[...].astype(jnp.float32)
    NR = min(32, n)

    def norm(i, carry):
        rows = pl.ds(pl.multiple_of(i * NR, NR), NR)
        xf = xb[rows, :].astype(jnp.float32)
        r = lax.rsqrt(jnp.sum(xf * xf, axis=1, keepdims=True) / d + EPS)
        xb[rows, :] = (xf * r * g).astype(jnp.bfloat16)
        return carry

    lax.fori_loop(0, n // NR, norm, 0)

    def rope(a):
        a = a.astype(jnp.bfloat16).astype(jnp.float32)
        return (a * cos_ref[...] + pltpu.roll(a, dh // 2, 1) * sin_ref[...]).astype(jnp.bfloat16)

    win[0].wait()
    win[1].wait()
    own = pl.ds(pl.multiple_of(lax.rem(xx, 2) * (2 * n) + c * n, n), n)

    def qkv_pair(i, carry):
        @pl.when(i == 1)
        def _():
            win[2].wait()

        @pl.when(i == 2)
        def _():
            send_own(1)
            send_own(4)

        h0 = jnp.minimum(2 * i - 2, heads - 2)
        r = mm(xb[...], wb[:, pl.ds(pl.multiple_of((h0 + 2) * dh, dh), 2 * dh)])

        @pl.when(i == 0)
        def _():
            kb[X + xx // 2, own, :] = rope(r[:, :dh])
            vs[0:n, :] = r[:, dh:].astype(jnp.bfloat16)
            vt[X + xx // 2, :, own] = jnp.swapaxes(r[:, dh:], 0, 1).astype(jnp.bfloat16)

        @pl.when(i > 0)
        def _():
            for j in range(2):
                qb[:, pl.ds(pl.multiple_of((h0 + j) * dh, dh), dh)] = rope(r[:, j * dh:(j + 1) * dh])
        return carry

    lax.fori_loop(0, 1 + (heads + 1) // 2, qkv_pair, 0)

    kv_out = (pltpu.make_async_copy(kb.at[X + xx // 2, own, :], ko_ref, hsem.at[0]),
              pltpu.make_async_copy(vs.at[0:n, :], vo_ref, hsem.at[1]))
    for cp in kv_out:
        cp.start()

    m_ref[...] = jnp.full(m_ref.shape, -1e30, jnp.float32)
    l_ref[...] = jnp.zeros_like(l_ref)

    def init(h, carry):
        acc_ref[h] = jnp.zeros(acc_ref.shape[1:], jnp.float32)
        return carry

    lax.fori_loop(0, heads, init, 0)

    def unit(tile, blk, off, cn, mask):
        rows = pl.ds(pl.multiple_of(tile * R, R), R)
        keys = pl.ds(off, cn)

        def qk(h):
            return lax.dot_general(kb[blk, keys, :], qb[rows, h * dh:(h + 1) * dh], (((1,), (1,)), ((), ())),
                                   preferred_element_type=jnp.float32)

        def pv(h, p, alpha):
            acc_ref[h, :, rows] = acc_ref[h, :, rows] * alpha + mm(vt[blk, :, keys], p)

        s = qk(0)
        pend = None
        for h in range(heads):
            s_next = qk(h + 1) if h + 1 < heads else None
            if pend is not None:
                pv(*pend)
            if mask is not None:
                s = jnp.where(mask, s, -jnp.inf)
            m_old = m_ref[h, :, rows]
            m_new = jnp.maximum(m_old, jnp.max(s, axis=0, keepdims=True) * scale)
            alpha = jnp.exp2(m_old - m_new)
            p = jnp.exp2(s * scale - m_new)
            l_ref[h, :, rows] = l_ref[h, :, rows] * alpha + jnp.sum(p.reshape(cn // 8, 8, R), axis=0)
            m_ref[h, :, rows] = m_new
            pend = (h, p.astype(jnp.bfloat16), alpha)
            s = s_next
        pv(*pend)

    hR = SR // 2

    def gx(i, sub):
        base = pl.multiple_of(sub * SR, SR)
        owner, off, ln, dev = ((t, 0, SR, up), (t, 0, SR, dn), (dn, 0, hR, up), (up, hR, hR, dn))[i]
        ref = ga.at[owner, pl.ds(pl.multiple_of(base + off, hR), ln), :]
        return pltpu.make_async_remote_copy(src_ref=ref, dst_ref=ref, send_sem=gas.at[i, sub], recv_sem=gar.at[i, sub],
                                            device_id={"tp": dev}, device_id_type=MESH)

    def g_wait(i, sub):
        base = pl.multiple_of(sub * SR, SR)
        owner, off, ln = ((dn, 0, SR), (up, 0, SR), (far, 0, hR), (far, hR, hR))[i]
        ref = ga.at[owner, pl.ds(pl.multiple_of(base + off, hR), ln), :]
        pltpu.make_async_remote_copy(src_ref=ref, dst_ref=ref, send_sem=gas.at[i, sub], recv_sem=gar.at[i, sub],
                                     device_id={"tp": up}, device_id_type=MESH).wait_recv()

    def g_pass(sub):
        g_wait(0, sub)
        gx(2, sub).start()
        g_wait(1, sub)
        gx(3, sub).start()

    def finish(tile):
        rows = pl.ds(pl.multiple_of(tile * R, R), R)
        for h in range(heads):
            l = jnp.sum(l_ref[h, :, rows], axis=0, keepdims=True)
            ga[t, rows, h * dh:(h + 1) * dh] = jnp.swapaxes(acc_ref[h, :, rows] / l, 0, 1).astype(jnp.bfloat16)

    def s_copy(j, dev, sub):
        return pltpu.make_async_remote_copy(src_ref=st.at[sub], dst_ref=strv.at[j, sub], send_sem=sts.at[j, sub],
                                            recv_sem=strs.at[j, sub], device_id={"tp": dev}, device_id_type=MESH)

    def wo_sub(sub):
        g_wait(2, sub)
        g_wait(3, sub)
        rows = pl.ds(pl.multiple_of(sub * SR, SR), SR)
        a = jnp.concatenate([ga[j, rows, :] for j in range(T)], axis=1)
        y = mm(a, wob[...].reshape(d, dt))
        v = xm[rows, :] + y.astype(jnp.bfloat16)
        xm[rows, :] = v
        vf = v.astype(jnp.float32)
        sb = jnp.broadcast_to(jnp.sum(vf * vf, axis=1, keepdims=True), (SR, LN))
        st[sub] = jnp.swapaxes(sb, 0, 1)[:8]
        for j, dev, _ in peers:
            s_copy(j, dev, sub).start()

    def h_sub(sub):
        rows = pl.ds(pl.multiple_of(sub * SR, SR), SR)
        for j, dev, _ in peers:
            s_copy(j, dev, sub).wait_recv()
        tot = st[sub] + strv[0, sub] + strv[1, sub] + strv[2, sub]
        r8 = lax.rsqrt(tot / d + EPS)
        rb = jnp.swapaxes(jnp.concatenate([r8] * (LN // 8), axis=0), 0, 1)
        for k in range(dt // LN):
            cols = slice(k * LN, (k + 1) * LN)
            gk = g2_ref[0:1, pl.ds(pl.multiple_of(t * dt + k * LN, LN), LN)].astype(jnp.float32)
            hb[rows, cols] = (xm[rows, cols].astype(jnp.float32) * rb * gk).astype(jnp.bfloat16)

    rx_wait(0, 2)
    rx_wait(3, 2)
    first = 3 * nt
    per = 1 + xx // 2
    total = first + nt * per

    def near(kind):
        pass_near(kind)
        pass_near(kind + 3)
        if kind == 1:
            wo_own.wait()
            for j, _, src in peers:
                wo_rx(j, src)
            send_own(2)

    def far_(kind):
        pass_far(kind)
        pass_far(kind + 3)

    points = ((1, near, 0), (2, near, 1), (4, far_, 0), (5, far_, 1), (first + per, pass_near, 2))

    def step(i, carry):
        for at, fn, kind in points:
            @pl.when(i == at)
            def _():
                fn(kind)

        for chip_at, gid in ((nt, 5), (2 * nt, 6)):
            @pl.when(i == chip_at)
            def _():
                rx_wait(0, gid)
                rx_wait(3, gid)

        @pl.when(i == first)
        def _():
            for kind in (0, 3):
                rx_wait(kind, 7)
                rx_wait(kind, 8)
            for kind in (1, 4):
                for gid in (2, 5, 6, 7, 8):
                    rx_wait(kind, gid)

        late = i >= first
        i2 = jnp.maximum(i - first, 0)
        m = lax.rem(i2, per)
        tile = jnp.where(late, i2 // per, lax.rem(i, nt))
        early = jnp.where(i < nt, xx, jnp.where(i < 2 * nt, lx, rx))
        blk = jnp.where(late, jnp.where(m == 0, ox, X + m - 1), early)
        last = jnp.logical_and(late, m == per - 1)
        unit(tile, blk, 0, C, None)

        @pl.when(last)
        def _():
            @pl.when(tile == 1)
            def _():
                g_pass(0)

            @pl.when(lax.rem(xx, 2) == 1)
            def _():
                unit(tile, X + xx // 2, 0, hc, None)

            row = lax.broadcasted_iota(jnp.int32, (hc, R), 1) + c * n + tile * R
            unit(tile, X + xx // 2, pl.multiple_of(lax.rem(xx, 2) * hc, hc), hc,
                 lax.broadcasted_iota(jnp.int32, (hc, R), 0) <= row)
            finish(tile)
            for sub in range(NS):
                gx(0, tile * NS + sub).start()
                gx(1, tile * NS + sub).start()
        return carry

    lax.fori_loop(0, total, step, 0)

    nsub = nt * NS
    g_pass(1)
    pass_far(2)
    for gid in (2, 5, 6, 7, 8):
        rx_wait(2, gid)
    xcol.wait()

    def tail(j, carry):
        @pl.when(j < nsub)
        def _():
            wo_sub(j)

        @pl.when(j + 2 < nsub)
        def _():
            g_pass(j + 2)

        @pl.when(j >= 1)
        def _():
            h_sub(j - 1)
        return carry

    lax.fori_loop(0, nsub + 1, tail, 0)
    o1 = pltpu.make_async_copy(hb, ho_ref, lsem.at[0])
    o2 = pltpu.make_async_copy(xm, xo_ref, lsem.at[1])
    o1.start()
    o2.start()
    for sub in range(nt * NS):
        for i in range(4):
            gx(i, sub).wait_send()
        for j, dev, _ in peers:
            s_copy(j, dev, sub).wait_send()
    for j, dev, _ in peers:
        wo_tx(j, dev).wait_send()
    for kind in range(5):
        for i in range(9):
            tx(kind, i).wait_send()
    for cp in kv_out:
        cp.wait()
    o1.wait()
    o2.wait()


def attention(T, SP, layer, x, cos, sin, kh, vh, wq, wk, wv, wo, g, g2, cid):
    n, d = x.shape
    w = wq.shape[2]
    hc, dh = kh.shape[1], kh.shape[2]
    heads = w // dh
    X = SP // 2
    assert 2 * hc == 4 * n and wk.shape[2] == dh and w * T == d
    nt = 2
    R = n // nt
    f32, bf = jnp.float32, jnp.bfloat16
    hbm = pl.BlockSpec(memory_space=pltpu.HBM)
    vm = pl.BlockSpec(memory_space=pltpu.VMEM)
    D = pltpu.SemaphoreType.DMA
    keys = SP * (hc + n // 2)
    return pl.pallas_call(
        functools.partial(attn_kernel, T, SP, layer),
        out_shape=[jax.ShapeDtypeStruct((n, w), bf), jax.ShapeDtypeStruct((n, w), bf),
                   jax.ShapeDtypeStruct((n, dh), bf), jax.ShapeDtypeStruct((n, dh), bf)],
        in_specs=[hbm, vm, vm, hbm, hbm, hbm, hbm, hbm, hbm, vm, vm],
        out_specs=[hbm, hbm, hbm, hbm],
        scratch_shapes=[
            pltpu.VMEM((n, d), bf),
            pltpu.VMEM((d, w + 2 * dh), bf),
            pltpu.VMEM((X + X // 2, 2 * hc, dh), bf),
            pltpu.VMEM((X + X // 2, dh, 2 * hc), bf),
            pltpu.VMEM((hc, dh), bf),
            pltpu.VMEM((n, w), bf),
            pltpu.VMEM((heads, 1, n), f32),
            pltpu.VMEM((heads, 8, n), f32),
            pltpu.VMEM((heads, dh, n), f32),
            pltpu.VMEM((T, n, w), bf),
            pltpu.VMEM((T, w // LN, SP, LN // SP, w), bf),
            pltpu.VMEM((n, w), bf),
            pltpu.VMEM((n, w), bf),
            pltpu.VMEM((4, 8, n // 4), f32),
            pltpu.VMEM((3, 4, 8, n // 4), f32),
            D((5, 9)), D((5, 9)), D((4, 4)), D((4, 4)), D((3,)), D((3,)), D((3, 4)), D((3, 4)), D((2,)), D((2,)), D((3,)),
        ],
        compiler_params=pltpu.CompilerParams(vmem_limit_bytes=61 * 2 ** 20, collective_id=cid, has_side_effects=True),
        cost_estimate=pl.CostEstimate(flops=4 * n * w * keys + 2 * n * d * (w + 2 * dh), bytes_accessed=4 * keys * dh,
                                      transcendentals=n * heads * keys),
        name="attention",
    )(x, cos, sin, kh, vh, wq, wk, wv, wo.reshape(wo.shape[0], w // LN, SP, LN // SP, d), g, g2)


def mlp_kernel(T, layer, h_ref, x_ref, wg_ref, wu_ref, wd_ref, out_ref,
               acc, ring, H, U, wdb, RA, RB, RD, RU, XF, xm,
               ags, agr, rss, rsr, lsem, wsem, dsem):
    n, d = XF.shape
    dt = d // T
    KP = dt // LN
    NP = T * KP
    NG = NP // 4
    F = U.shape[1]
    FP = F // LN
    t = lax.axis_index("tp")
    up = lax.rem(t + 1, T)
    dn = lax.rem(t + 3, T)
    op = lax.rem(t + 2, T)
    hf = n // 2
    ALL, A, B = pl.ds(0, n), pl.ds(0, hf), pl.ds(hf, hf)

    barrier = pltpu.get_barrier_semaphore()
    for dev in (up, dn, op):
        pl.semaphore_signal(barrier, inc=1, device_id={"tp": dev}, device_id_type=MESH)

    def rcopy(src, dst, ss, rs, dev):
        return pltpu.make_async_remote_copy(src_ref=src, dst_ref=dst, send_sem=ss, recv_sem=rs,
                                            device_id={"tp": dev}, device_id_type=MESH)

    def pos_of(kind, k):
        return {'own': k, 'up': KP + 2 * k, 'dn': KP + 2 * k + 1, 'op': 3 * KP + k}[kind]

    order = [None] * NP
    for kind in ('own', 'up', 'dn', 'op'):
        for k in range(KP):
            order[pos_of(kind, k)] = (kind, k)
    owner_of = {'own': t, 'up': up, 'dn': dn, 'op': op}

    def hloc(kind, owner, k, rows):
        p = pos_of(kind, k)
        return H.at[p // 4, rows, pl.ds((p % 4) * LN, LN)]

    def xloc(kind, owner, k, rows):
        return XF.at[rows, pl.ds(pl.multiple_of(owner * dt + k * LN, LN), LN)]

    class Gather:
        def __init__(self, loc):
            self.loc = loc

        def c_up(self, k):
            return rcopy(self.loc('own', t, k, ALL), self.loc('dn', t, k, ALL), ags.at[0, k], agr.at[0, k], up)

        def c_dn(self, k):
            return rcopy(self.loc('own', t, k, ALL), self.loc('up', t, k, ALL), ags.at[1, k], agr.at[1, k], dn)

        def r_up(self, k):
            return rcopy(self.loc('dn', dn, k, A), self.loc('op', dn, k, A), ags.at[2, k], agr.at[2, k], up)

        def r_dn(self, k):
            return rcopy(self.loc('up', up, k, B), self.loc('op', up, k, B), ags.at[3, k], agr.at[3, k], dn)

        def send(self, k):
            self.c_up(k).start()
            self.c_dn(k).start()

        def wait(self, kind, k):
            if kind == 'dn':
                rcopy(self.loc('dn', dn, k, ALL), self.loc('dn', dn, k, ALL), ags.at[0, k], agr.at[0, k], up).wait_recv()
                self.r_up(k).start()
            elif kind == 'up':
                rcopy(self.loc('up', up, k, ALL), self.loc('up', up, k, ALL), ags.at[1, k], agr.at[1, k], dn).wait_recv()
                self.r_dn(k).start()
            elif kind == 'op':
                rcopy(self.loc('op', op, k, A), self.loc('op', op, k, A), ags.at[2, k], agr.at[2, k], up).wait_recv()
                rcopy(self.loc('op', op, k, B), self.loc('op', op, k, B), ags.at[3, k], agr.at[3, k], dn).wait_recv()

        def done(self):
            for k in range(KP):
                self.c_up(k).wait_send()
                self.c_dn(k).wait_send()
                self.r_up(k).wait_send()
                self.r_dn(k).wait_send()

    gh = Gather(hloc)
    gx = Gather(xloc)

    def wait_group(gather, j):
        for kind, k in order[4 * j:4 * j + 4]:
            gather.wait(kind, k)

    def h_in(k):
        return pltpu.make_async_copy(h_ref.at[:, pl.ds(k * LN, LN)], hloc('own', t, k, ALL), lsem.at[0])

    for k in range(KP):
        h_in(k).start()
    xin = pltpu.make_async_copy(x_ref, xm, lsem.at[1])
    xin.start()

    def w_copy(i, q, slot):
        p = (i // 2) * 4 + q
        own = p < KP
        pair = jnp.logical_and(p >= KP, p < 3 * KP)
        k = jnp.where(own, p, jnp.where(pair, (p - KP) // 2, p - 3 * KP))
        who = jnp.where(own, t, jnp.where(pair, jnp.where(lax.rem(p - KP, 2) == 0, up, dn), op))
        row = pl.multiple_of(who * dt + k * LN, LN)
        return row

    def w_start(i, slot):
        for q in range(4):
            row = w_copy(i, q, slot)
            dst = ring.at[slot, pl.ds(q * LN, LN), :]

            @pl.when(lax.rem(i, 2) == 0)
            def _():
                pltpu.make_async_copy(wg_ref.at[layer, pl.ds(row, LN), :], dst, wsem.at[slot]).start()

            @pl.when(lax.rem(i, 2) == 1)
            def _():
                pltpu.make_async_copy(wu_ref.at[layer, pl.ds(row, LN), :], dst, wsem.at[slot]).start()

    def w_wait(slot):
        pltpu.make_async_copy(wg_ref.at[layer, pl.ds(0, 4 * LN), :], ring.at[slot], wsem.at[slot]).wait()

    NSLOT = ring.shape[0]
    for s in range(NSLOT):
        w_start(jnp.int32(s), s)
    for k in range(KP):
        h_in(k).wait()
    pl.semaphore_wait(barrier, 3)
    for k in range(KP):
        gh.send(k)

    def zero(j, c):
        acc[j] = jnp.zeros(acc.shape[1:], acc.dtype)
        return c

    lax.fori_loop(0, 2 * FP, zero, 0)

    def gu_step(i, c):
        j = i // 2
        slot = lax.rem(i, NSLOT)
        for jj in range(NG):
            @pl.when(i == 2 * jj)
            def _():
                wait_group(gh, jj)
        w_wait(slot)
        base = lax.rem(i, 2) * FP
        for f in range(0, FP, 4):
            m = min(4, FP - f)
            r = mm(H[j], ring[slot, :, f * LN:(f + m) * LN])
            for q in range(m):
                acc[base + f + q] += r[:, q * LN:(q + 1) * LN]

        @pl.when(i + NSLOT < 2 * NG)
        def _():
            w_start(i + NSLOT, slot)
        return c

    def d_col(p):
        c = p // KP
        who = jnp.where(c == 0, op, jnp.where(c == 1, up, jnp.where(c == 2, dn, t)))
        return pl.multiple_of(who * dt + lax.rem(p, KP) * LN, LN)

    def d_start(i, slot):
        for q in range(2):
            pltpu.make_async_copy(wd_ref.at[layer, :, pl.ds(d_col(2 * i + q), LN)],
                                  wdb.at[slot, :, pl.ds(q * LN, LN)], dsem.at[slot]).start()

    def d_wait(slot):
        pltpu.make_async_copy(wd_ref.at[layer, :, pl.ds(0, 2 * LN)], wdb.at[slot], dsem.at[slot]).wait()

    d_start(jnp.int32(0), 0)
    d_start(jnp.int32(1), 1)
    lax.fori_loop(0, 2 * NG, gu_step, 0)

    def silu(f, c):
        a = acc[f].astype(jnp.bfloat16).astype(jnp.float32)
        b = acc[FP + f].astype(jnp.bfloat16).astype(jnp.float32)
        U[:, pl.ds(pl.multiple_of(f * LN, LN), LN)] = (a * (1.0 / (1.0 + jnp.exp(-a))) * b).astype(jnp.bfloat16)
        return c

    lax.fori_loop(0, FP, silu, 0)
    gh.done()

    def c_opA(k):
        return rcopy(acc.at[k, A, :], RA.at[k], rss.at[0, k], rsr.at[0, k], up)

    def c_opB(k):
        return rcopy(acc.at[k, B, :], RB.at[k], rss.at[1, k], rsr.at[1, k], dn)

    def c_upB(k):
        return rcopy(acc.at[KP + k, B, :], RD.at[k, B, :], rss.at[2, k], rsr.at[2, k], up)

    def c_dnA(k):
        return rcopy(acc.at[2 * KP + k, A, :], RU.at[k, A, :], rss.at[3, k], rsr.at[3, k], dn)

    def c_upA(k):
        return rcopy(acc.at[KP + k, A, :], RD.at[k, A, :], rss.at[4, k], rsr.at[4, k], up)

    def c_dnB(k):
        return rcopy(acc.at[2 * KP + k, B, :], RU.at[k, B, :], rss.at[5, k], rsr.at[5, k], dn)

    def rs_send(p):
        c = p // KP
        k = lax.rem(p, KP)

        @pl.when(c == 0)
        def _():
            c_opA(k).start()
            c_opB(k).start()

        @pl.when(c == 1)
        def _():
            c_upB(k).start()

        @pl.when(c == 2)
        def _():
            c_dnA(k).start()

    def down(i, c):
        slot = lax.rem(i, 2)
        d_wait(slot)

        @pl.when(i > 0)
        def _():
            rs_send(2 * i - 2)
            rs_send(2 * i - 1)

        r = mm(U[...], wdb[slot])
        for q in range(2):
            acc[2 * i + q] = r[:, q * LN:(q + 1) * LN]

        @pl.when(i + 2 < NP // 2)
        def _():
            d_start(i + 2, slot)
        return c

    lax.fori_loop(0, NP // 2, down, 0)

    def add(k, c):
        c_opA(k).wait_recv()
        acc[KP + k, 0:hf, :] += RA[k]
        c_upA(k).start()
        c_opB(k).wait_recv()
        acc[2 * KP + k, hf:n, :] += RB[k]
        c_dnB(k).start()
        return c

    lax.fori_loop(0, KP, add, 0)

    xin.wait()

    def total(k, c):
        c_upB(k).wait_recv()
        c_dnA(k).wait_recv()
        c_upA(k).wait_recv()
        c_dnB(k).wait_recv()
        s = acc[3 * KP + k] + RD[k] + RU[k]
        v = xm[:, pl.ds(pl.multiple_of(k * LN, LN), LN)] + s.astype(jnp.bfloat16)
        XF[:, pl.ds(pl.multiple_of(t * dt + k * LN, LN), LN)] = v
        gx.send(k)
        return c

    lax.fori_loop(0, KP, total, 0)

    def near(k, c):
        gx.wait('up', k)
        gx.wait('dn', k)
        return c

    lax.fori_loop(0, KP, near, 0)

    def far(k, c):
        gx.wait('op', k)
        return c

    lax.fori_loop(0, KP, far, 0)
    o = pltpu.make_async_copy(XF, out_ref, lsem.at[0])
    o.start()

    def sent(k, c):
        for cp in (gx.c_up, gx.c_dn, gx.r_up, gx.r_dn, c_opA, c_opB, c_upB, c_dnA, c_upA, c_dnB):
            cp(k).wait_send()
        return c

    lax.fori_loop(0, KP, sent, 0)
    o.wait()


def mlp(T, layer, h, x, wg, wu, wd, cid):
    n, dt = x.shape
    F = wg.shape[2]
    d = dt * T
    KP = dt // LN
    FP = F // LN
    hf = n // 2
    NG = T * KP // 4
    f32, bf = jnp.float32, jnp.bfloat16
    anyspec = pl.BlockSpec(memory_space=pltpu.HBM)
    D = pltpu.SemaphoreType.DMA
    return pl.pallas_call(
        functools.partial(mlp_kernel, T, layer),
        out_shape=jax.ShapeDtypeStruct((n, d), bf),
        in_specs=[anyspec] * 5,
        out_specs=anyspec,
        scratch_shapes=[
            pltpu.VMEM((2 * FP, n, LN), f32),
            pltpu.VMEM((3, 4 * LN, F), bf),
            pltpu.VMEM((NG, n, 4 * LN), bf),
            pltpu.VMEM((n, F), bf),
            pltpu.VMEM((2, F, 2 * LN), bf),
            pltpu.VMEM((KP, hf, LN), f32),
            pltpu.VMEM((KP, hf, LN), f32),
            pltpu.VMEM((KP, n, LN), f32),
            pltpu.VMEM((KP, n, LN), f32),
            pltpu.VMEM((n, d), bf),
            pltpu.VMEM((n, dt), bf),
            D((4, KP)), D((4, KP)), D((6, KP)), D((6, KP)), D((2,)), D((3,)), D((2,)),
        ],
        compiler_params=pltpu.CompilerParams(vmem_limit_bytes=61 * 2 ** 20, collective_id=cid, has_side_effects=True),
        cost_estimate=pl.CostEstimate(flops=6 * n * d * F, bytes_accessed=6 * d * F, transcendentals=n * F),
        name="mlp",
    )(h, x, wg, wu, wd)


def solution(mesh):
    sp = mesh.shape['sp']
    tp = mesh.shape['tp']
    row = ('dp', 'sp')
    kv_spec = P(None, row, 'tp', None)
    col = P(None, None, 'tp')
    rowsplit = P(None, 'tp', None)

    def body(x, pos, k_hist, v_hist, wq, wk, wv, wo, wg, wu, wd, g1, g2):
        n, d = x.shape
        layers, hc, kvl, dh = k_hist.shape
        kh, vh = k_hist.reshape(layers, hc, dh), v_hist.reshape(layers, hc, dh)
        half = dh // 2
        inv = ROPE_THETA ** (-(jnp.arange(half, dtype=jnp.float32) * (2.0 / dh)))
        ang = pos.astype(jnp.float32)[:, None] * inv
        cos, sin = jnp.cos(ang), jnp.sin(ang)
        cos = jnp.concatenate([cos, cos], axis=1)
        sin = jnp.concatenate([-sin, sin], axis=1)
        ks, vs = [], []
        for l in range(layers):
            h, xm, k, v = attention(tp, sp, l, x, cos, sin, kh, vh, wq, wk, wv, wo, g1[l:l + 1], g2[l:l + 1], 2 * l)
            ks.append(k.reshape(n, kvl, dh))
            vs.append(v.reshape(n, kvl, dh))
            x = mlp(tp, l, h, xm, wg, wu, wd, 2 * l + 1)
        return x, jnp.stack(ks), jnp.stack(vs)

    in_specs = (P(row, None), P(row), kv_spec, kv_spec, col, col, col, rowsplit, col, col, rowsplit, P(), P())
    out_specs = (P(row, None), kv_spec, kv_spec)
    return jax.shard_map(body, mesh=mesh, in_specs=in_specs, out_specs=out_specs, check_vma=False)
```

```python
import functools

import jax
import jax.numpy as jnp
from jax import lax
from jax.experimental import pallas as pl
from jax.experimental.pallas import tpu as pltpu
from jax.sharding import PartitionSpec as P

EPS = 1e-5
ROPE_THETA = 500000.0
LOG2E = 1.4426950408889634
MESH = pl.DeviceIdType.MESH
LN = 128
VMEM_LIMIT = 61 * 2 ** 20


def mm(a, b):
    return jnp.dot(a, b, preferred_element_type=jnp.float32)


def attn_kernel(T, SP, layer, x_ref, cos_ref, sin_ref, kh_ref, vh_ref, wq_ref, wk_ref, wv_ref, wo_ref, g_ref, g2_ref,
                ho_ref, xo_ref, ko_ref, vo_ref,
                xb, wb, kb, vt, vs, qb, m_ref, l_ref, acc_ref, ga, wob, xm, hb, st, strv,
                kvs, kvr, gas, gar, wys, wyr, sts, strs, lsem, hsem, wsem):
    n, d = xb.shape
    w = qb.shape[1]
    dh = kb.shape[2]
    heads = w // dh
    X = SP // 2
    C = kb.shape[1]
    hc = C // 2
    dt = w
    nt = 2
    R = n // nt
    NS = 2
    SR = R // NS
    scale = dh ** -0.5 * LOG2E
    me = lax.axis_index("sp")
    t = lax.axis_index("tp")
    c = lax.rem(me, 2)
    xx = me // 2
    lx, rx, ox = lax.rem(xx + X - 1, X), lax.rem(xx + 1, X), lax.rem(xx + 2, X)
    left, right, part = lx * 2 + c, rx * 2 + c, xx * 2 + 1 - c
    up, dn, far = lax.rem(t + 1, T), lax.rem(t + T - 1, T), lax.rem(t + 2, T)

    barrier = pltpu.get_barrier_semaphore()
    for dev in ({"sp": left}, {"sp": right}, {"sp": part}, {"tp": up}, {"tp": dn}, {"tp": far}):
        pl.semaphore_signal(barrier, inc=1, device_id=dev, device_id_type=MESH)

    hown = pl.ds(pl.multiple_of(c * hc, hc), hc)
    hist_in = (pltpu.make_async_copy(kh_ref.at[layer], kb.at[xx, hown, :], hsem.at[0]),
               pltpu.make_async_copy(vh_ref.at[layer], vs, hsem.at[1]))
    for cp in hist_in:
        cp.start()
    xin = pltpu.make_async_copy(x_ref, xb, lsem.at[0])
    xin.start()
    win = [pltpu.make_async_copy(wk_ref.at[layer], wb.at[:, 0:dh], wsem.at[0]),
           pltpu.make_async_copy(wv_ref.at[layer], wb.at[:, dh:2 * dh], wsem.at[0]),
           pltpu.make_async_copy(wq_ref.at[layer], wb.at[:, 2 * dh:], wsem.at[1])]
    for cp in win:
        cp.start()

    def wo_cols(dev):
        return wo_ref.at[layer, :, me, :, pl.ds(pl.multiple_of(dev * dt, LN), dt)]

    wo_own = pltpu.make_async_copy(wo_cols(t), wob.at[t, :, me], wsem.at[2])
    wo_own.start()
    xcol = pltpu.make_async_copy(x_ref.at[:, pl.ds(pl.multiple_of(t * dt, LN), dt)], xm, lsem.at[1])
    xcol.start()
    peers = [(j, *e) for j, e in enumerate(((up, dn), (dn, up), (far, far)))]

    def wo_tx(j, dev):
        return pltpu.make_async_remote_copy(src_ref=wo_cols(dev), dst_ref=wob.at[t, :, me], send_sem=wys.at[j],
                                            recv_sem=wyr.at[j], device_id={"tp": dev}, device_id_type=MESH)

    def wo_rx(j, src):
        pltpu.make_async_remote_copy(src_ref=wob.at[src, :, me], dst_ref=wob.at[src, :, me], send_sem=wys.at[j],
                                     recv_sem=wyr.at[j], device_id={"tp": src}, device_id_type=MESH).wait_recv()

    def region(kind, chip, core, half=None):
        if kind == 2:
            if half is None:
                return wob.at[:, :, chip * 2 + core]
            return wob.at[pl.ds(half * (T // 2), T // 2), :, chip * 2 + core]
        if kind % 3 == 0:
            blk, base, ln = chip, core * hc, hc
        else:
            blk, base, ln = X + chip // 2, lax.rem(chip, 2) * (2 * n) + core * n, n
        if half is not None:
            ln = ln // 2
            base = base + half * ln
        part_ = pl.ds(pl.multiple_of(base, ln), ln)
        return kb.at[blk, part_, :] if kind < 3 else vt.at[blk, :, part_]

    whole, other = None, 1 - c
    relayed = (2, 5, 6, 7, 8)
    sent = [(xx, c, whole, right), (xx, c, whole, left), (xx, c, whole, part), (lx, c, 0, right), (rx, c, 1, left),
            (lx, c, whole, part), (rx, c, whole, part), (ox, c, 0, part), (ox, c, 1, part)]
    got = [(lx, c, whole), (rx, c, whole), (xx, other, whole), (ox, c, 0), (ox, c, 1),
           (lx, other, whole), (rx, other, whole), (ox, other, 0), (ox, other, 1)]

    def tx(kind, i):
        chip, core, half, dev = sent[i]
        r = region(kind, chip, core, half)
        return pltpu.make_async_remote_copy(src_ref=r, dst_ref=r, send_sem=kvs.at[kind, i], recv_sem=kvr.at[kind, i],
                                            device_id={"sp": dev}, device_id_type=MESH)

    def rx_wait(kind, i):
        chip, core, half = got[i]
        r = region(kind, chip, core, half)
        pltpu.make_async_remote_copy(src_ref=r, dst_ref=r, send_sem=kvs.at[kind, i], recv_sem=kvr.at[kind, i],
                                     device_id={"sp": part}, device_id_type=MESH).wait_recv()

    def send_own(kind):
        for i in (0, 1, 2):
            tx(kind, i).start()

    def pass_near(kind):
        rx_wait(kind, 0)
        tx(kind, 3).start()
        tx(kind, 5).start()
        rx_wait(kind, 1)
        tx(kind, 4).start()
        tx(kind, 6).start()

    def pass_far(kind):
        rx_wait(kind, 3)
        tx(kind, 7).start()
        rx_wait(kind, 4)
        tx(kind, 8).start()

    pl.semaphore_wait(barrier, 6)
    hist_in[0].wait()
    send_own(0)
    hist_in[1].wait()
    vt[xx, :, hown] = jnp.swapaxes(vs[...].astype(jnp.float32), 0, 1).astype(jnp.bfloat16)
    send_own(3)
    for j, dev, _ in peers:
        wo_tx(j, dev).start()

    xin.wait()
    g = g_ref[layer:layer + 1, :].astype(jnp.float32)
    NR = min(LN, n)

    def norm(i, carry):
        rows = pl.ds(pl.multiple_of(i * NR, NR), NR)
        xf = xb[rows, :].astype(jnp.float32)
        r = lax.rsqrt(jnp.sum(xf * xf, axis=1, keepdims=True) / d + EPS)
        xb[rows, :] = (xf * r * g).astype(jnp.bfloat16)
        return carry

    lax.fori_loop(0, n // NR, norm, 0)

    def rope(a):
        a = a.astype(jnp.bfloat16).astype(jnp.float32)
        return (a * cos_ref[...] + pltpu.roll(a, dh // 2, 1) * sin_ref[...]).astype(jnp.bfloat16)

    win[0].wait()
    win[1].wait()
    own = pl.ds(pl.multiple_of(lax.rem(xx, 2) * (2 * n) + c * n, n), n)

    def qkv_pair(i, carry):
        @pl.when(i == 1)
        def _():
            win[2].wait()

        @pl.when(i == 2)
        def _():
            send_own(1)
            send_own(4)

        h0 = jnp.minimum(2 * i - 2, heads - 2)
        r = mm(xb[...], wb[:, pl.ds(pl.multiple_of((h0 + 2) * dh, dh), 2 * dh)])

        @pl.when(i == 0)
        def _():
            kb[X + xx // 2, own, :] = rope(r[:, :dh])
            vs[0:n, :] = r[:, dh:].astype(jnp.bfloat16)
            vt[X + xx // 2, :, own] = jnp.swapaxes(r[:, dh:], 0, 1).astype(jnp.bfloat16)

        @pl.when(i > 0)
        def _():
            for j in range(2):
                qb[:, pl.ds(pl.multiple_of((h0 + j) * dh, dh), dh)] = rope(r[:, j * dh:(j + 1) * dh])
        return carry

    lax.fori_loop(0, 1 + (heads + 1) // 2, qkv_pair, 0)

    kv_out = (pltpu.make_async_copy(kb.at[X + xx // 2, own, :], ko_ref, hsem.at[0]),
              pltpu.make_async_copy(vs.at[0:n, :], vo_ref, hsem.at[1]))
    for cp in kv_out:
        cp.start()

    m_ref[...] = jnp.full(m_ref.shape, -1e30, jnp.float32)
    l_ref[...] = jnp.zeros_like(l_ref)

    def init(h, carry):
        acc_ref[h] = jnp.zeros(acc_ref.shape[1:], jnp.float32)
        return carry

    lax.fori_loop(0, heads, init, 0)

    def unit(tile, blk, off, cn, mask=None):
        rows = pl.ds(pl.multiple_of(tile * R, R), R)

        sn = C // 4
        chain = [(h, j * sn) for h in range(heads) for j in range(cn // sn)]

        def qk(h, j):
            return lax.dot_general(kb[blk, pl.ds(off + j, sn), :], qb[rows, h * dh:(h + 1) * dh], (((1,), (1,)), ((), ())),
                                   preferred_element_type=jnp.float32)

        def pv(h, j, p, alpha):
            acc_ref[h, :, rows] = acc_ref[h, :, rows] * alpha + mm(vt[blk, :, pl.ds(off + j, sn)], p)

        ahead = 2
        scores = [qk(*e) for e in chain[:ahead]]
        pend = []
        for i, (h, j) in enumerate(chain):
            if i + ahead < len(chain):
                scores.append(qk(*chain[i + ahead]))
            s = scores.pop(0)
            if len(pend) == ahead:
                pv(*pend.pop(0))
            if mask is not None:
                s = jnp.where(mask(j, sn), s, -jnp.inf)
            m_old = m_ref[h, :, rows]
            m_new = jnp.maximum(m_old, jnp.max(s, axis=0, keepdims=True) * scale)
            alpha = jnp.exp2(m_old - m_new)
            p = jnp.exp2(s * scale - m_new)
            l_ref[h, :, rows] = l_ref[h, :, rows] * alpha + jnp.sum(p.reshape(sn // 8, 8, R), axis=0)
            m_ref[h, :, rows] = m_new
            pend.append((h, j, p.astype(jnp.bfloat16), alpha))
        for e in pend:
            pv(*e)

    hR = SR // 2

    def gx(i, sub):
        base = pl.multiple_of(sub * SR, SR)
        owner, off, ln, dev = ((t, 0, SR, up), (t, 0, SR, dn), (dn, 0, hR, up), (up, hR, hR, dn))[i]
        ref = ga.at[owner, pl.ds(pl.multiple_of(base + off, hR), ln), :]
        return pltpu.make_async_remote_copy(src_ref=ref, dst_ref=ref, send_sem=gas.at[i, sub], recv_sem=gar.at[i, sub],
                                            device_id={"tp": dev}, device_id_type=MESH)

    def g_wait(i, sub):
        base = pl.multiple_of(sub * SR, SR)
        owner, off, ln = ((dn, 0, SR), (up, 0, SR), (far, 0, hR), (far, hR, hR))[i]
        ref = ga.at[owner, pl.ds(pl.multiple_of(base + off, hR), ln), :]
        pltpu.make_async_remote_copy(src_ref=ref, dst_ref=ref, send_sem=gas.at[i, sub], recv_sem=gar.at[i, sub],
                                     device_id={"tp": up}, device_id_type=MESH).wait_recv()

    def g_pass(sub):
        g_wait(0, sub)
        gx(2, sub).start()
        g_wait(1, sub)
        gx(3, sub).start()

    def finish(tile):
        rows = pl.ds(pl.multiple_of(tile * R, R), R)
        for h in range(heads):
            l = jnp.sum(l_ref[h, :, rows], axis=0, keepdims=True)
            ga[t, rows, h * dh:(h + 1) * dh] = jnp.swapaxes(acc_ref[h, :, rows] / l, 0, 1).astype(jnp.bfloat16)

    def s_copy(j, dev, sub):
        return pltpu.make_async_remote_copy(src_ref=st.at[sub], dst_ref=strv.at[j, sub], send_sem=sts.at[j, sub],
                                            recv_sem=strs.at[j, sub], device_id={"tp": dev}, device_id_type=MESH)

    def wo_sub(sub):
        g_wait(2, sub)
        g_wait(3, sub)
        rows = pl.ds(pl.multiple_of(sub * SR, SR), SR)
        a = jnp.concatenate([ga[j, rows, :] for j in range(T)], axis=1)
        y = mm(a, wob[...].reshape(d, dt))
        v = xm[rows, :] + y.astype(jnp.bfloat16)
        xm[rows, :] = v
        vf = v.astype(jnp.float32)
        sb = jnp.broadcast_to(jnp.sum(vf * vf, axis=1, keepdims=True), (SR, LN))
        st[sub] = jnp.swapaxes(sb, 0, 1)[:8]
        for j, dev, _ in peers:
            s_copy(j, dev, sub).start()

    def h_sub(sub):
        rows = pl.ds(pl.multiple_of(sub * SR, SR), SR)
        for j, dev, _ in peers:
            s_copy(j, dev, sub).wait_recv()
        tot = st[sub] + strv[0, sub] + strv[1, sub] + strv[2, sub]
        r8 = lax.rsqrt(tot / d + EPS)
        rb = jnp.swapaxes(jnp.concatenate([r8] * (LN // 8), axis=0), 0, 1)
        for k in range(dt // LN):
            cols = slice(k * LN, (k + 1) * LN)
            gk = g2_ref[layer:layer + 1, pl.ds(pl.multiple_of(t * dt + k * LN, LN), LN)].astype(jnp.float32)
            hb[rows, cols] = (xm[rows, cols].astype(jnp.float32) * rb * gk).astype(jnp.bfloat16)

    rx_wait(0, 2)
    rx_wait(3, 2)
    first = 3 * nt
    per = 1 + xx // 2
    total = first + nt * per

    def near(kind):
        pass_near(kind)
        pass_near(kind + 3)
        if kind == 1:
            wo_own.wait()
            for j, _, src in peers:
                wo_rx(j, src)
            send_own(2)

    def far_(kind):
        pass_far(kind)
        pass_far(kind + 3)

    points = ((1, near, 0), (2, near, 1), (4, far_, 0), (5, far_, 1), (first + per, pass_near, 2))

    def step(i, carry):
        for at, fn, kind in points:
            @pl.when(i == at)
            def _():
                fn(kind)

        for chip_at, gid in ((nt, 5), (2 * nt, 6)):
            @pl.when(i == chip_at)
            def _():
                rx_wait(0, gid)
                rx_wait(3, gid)

        @pl.when(i == first)
        def _():
            for kind in (0, 3):
                rx_wait(kind, 7)
                rx_wait(kind, 8)
            for kind in (1, 4):
                for gid in relayed:
                    rx_wait(kind, gid)

        late = i >= first
        i2 = jnp.maximum(i - first, 0)
        m = lax.rem(i2, per)
        tile = jnp.where(late, i2 // per, lax.rem(i, nt))
        early = jnp.where(i < nt, xx, jnp.where(i < 2 * nt, lx, rx))
        blk = jnp.where(late, jnp.where(m == 0, ox, X + m - 1), early)
        last = jnp.logical_and(late, m == per - 1)
        unit(tile, blk, 0, C)

        @pl.when(last)
        def _():
            @pl.when(tile == 1)
            def _():
                g_pass(0)

            @pl.when(lax.rem(xx, 2) == 1)
            def _():
                unit(tile, X + xx // 2, 0, hc)

            def causal(j, sn):
                row = lax.broadcasted_iota(jnp.int32, (sn, R), 1) + (c * n + tile * R - j)
                return lax.broadcasted_iota(jnp.int32, (sn, R), 0) <= row

            unit(tile, X + xx // 2, pl.multiple_of(lax.rem(xx, 2) * hc, hc), hc, causal)
            finish(tile)
            for sub in range(NS):
                gx(0, tile * NS + sub).start()
                gx(1, tile * NS + sub).start()
        return carry

    lax.fori_loop(0, total, step, 0)

    nsub = nt * NS
    g_pass(1)
    pass_far(2)
    for gid in relayed:
        rx_wait(2, gid)
    xcol.wait()

    def tail(j, carry):
        @pl.when(j < nsub)
        def _():
            wo_sub(j)

        @pl.when(j + 2 < nsub)
        def _():
            g_pass(j + 2)

        @pl.when(j >= 1)
        def _():
            h_sub(j - 1)
        return carry

    lax.fori_loop(0, nsub + 1, tail, 0)
    o1 = pltpu.make_async_copy(hb, ho_ref, lsem.at[0])
    o2 = pltpu.make_async_copy(xm, xo_ref, lsem.at[1])
    o1.start()
    o2.start()
    for sub in range(nt * NS):
        for i in range(4):
            gx(i, sub).wait_send()
        for j, dev, _ in peers:
            s_copy(j, dev, sub).wait_send()
    for j, dev, _ in peers:
        wo_tx(j, dev).wait_send()
    for kind in range(5):
        for i in range(len(sent)):
            tx(kind, i).wait_send()
    for cp in kv_out:
        cp.wait()
    o1.wait()
    o2.wait()


def attention(T, SP, layer, x, cos, sin, kh, vh, wq, wk, wv, wo, g, g2, cid):
    n, d = x.shape
    w = wq.shape[2]
    hc, dh = kh.shape[1], kh.shape[2]
    heads = w // dh
    X = SP // 2
    assert 2 * hc == 4 * n and wk.shape[2] == dh and w * T == d
    nt = 2
    R = n // nt
    f32, bf = jnp.float32, jnp.bfloat16
    hbm = pl.BlockSpec(memory_space=pltpu.HBM)
    vm = pl.BlockSpec(memory_space=pltpu.VMEM)
    D = pltpu.SemaphoreType.DMA
    return pl.pallas_call(
        functools.partial(attn_kernel, T, SP, layer),
        out_shape=[jax.ShapeDtypeStruct((n, w), bf), jax.ShapeDtypeStruct((n, w), bf),
                   jax.ShapeDtypeStruct((n, dh), bf), jax.ShapeDtypeStruct((n, dh), bf)],
        in_specs=[hbm, vm, vm, hbm, hbm, hbm, hbm, hbm, hbm, vm, vm],
        out_specs=[hbm, hbm, hbm, hbm],
        scratch_shapes=[
            pltpu.VMEM((n, d), bf),
            pltpu.VMEM((d, w + 2 * dh), bf),
            pltpu.VMEM((X + X // 2, 2 * hc, dh), bf),
            pltpu.VMEM((X + X // 2, dh, 2 * hc), bf),
            pltpu.VMEM((hc, dh), bf),
            pltpu.VMEM((n, w), bf),
            pltpu.VMEM((heads, 1, n), f32),
            pltpu.VMEM((heads, 8, n), f32),
            pltpu.VMEM((heads, dh, n), f32),
            pltpu.VMEM((T, n, w), bf),
            pltpu.VMEM((T, w // LN, SP, LN // SP, w), bf),
            pltpu.VMEM((n, w), bf),
            pltpu.VMEM((n, w), bf),
            pltpu.VMEM((4, 8, n // 4), f32),
            pltpu.VMEM((3, 4, 8, n // 4), f32),
            D((5, 9)), D((5, 9)), D((4, 4)), D((4, 4)), D((3,)), D((3,)), D((3, 4)), D((3, 4)), D((2,)), D((2,)), D((3,)),
        ],
        compiler_params=pltpu.CompilerParams(vmem_limit_bytes=VMEM_LIMIT, collective_id=cid, has_side_effects=True),
        name="attention",
    )(x, cos, sin, kh, vh, wq, wk, wv, wo.reshape(wo.shape[0], w // LN, SP, LN // SP, d), g, g2)


def mlp_kernel(T, layer, h_ref, x_ref, wg_ref, wu_ref, wd_ref, out_ref,
               acc, PS, ring, H, U, wdb, RA, RB, RD, RU, XF, xm,
               ags, agr, rss, rsr, lsem, wsem, dsem):
    n, d = XF.shape
    dt = d // T
    KP = dt // LN
    NP = T * KP
    NG = NP // 4
    F = U.shape[1]
    FP = F // LN
    hn = n // 2
    qn = hn // 2
    NSLOT = ring.shape[0]
    ND = wdb.shape[0]
    SUB = 2 * NG
    TL = NP // 2
    t = lax.axis_index("tp")
    up = lax.rem(t + 1, T)
    dn = lax.rem(t + 3, T)
    op = lax.rem(t + 2, T)

    barrier = pltpu.get_barrier_semaphore()
    for dev in (up, dn, op):
        pl.semaphore_signal(barrier, inc=1, device_id={"tp": dev}, device_id_type=MESH)

    def rcopy(src, dst, ss, rs, dev):
        return pltpu.make_async_remote_copy(src_ref=src, dst_ref=dst, send_sem=ss, recv_sem=rs,
                                            device_id={"tp": dev}, device_id_type=MESH)

    def pos_of(kind, k):
        return {'own': k, 'up': KP + 2 * k, 'dn': KP + 2 * k + 1, 'op': 3 * KP + k}[kind]

    order = [None] * NP
    for kind in ('own', 'up', 'dn', 'op'):
        for k in range(KP):
            order[pos_of(kind, k)] = (kind, k)

    def rows_of(base, part=None):
        if part is None:
            return pl.ds(base if isinstance(base, int) else pl.multiple_of(base, hn), hn)
        return pl.ds(base + part * qn if isinstance(base, int) else pl.multiple_of(base + part * qn, qn), qn)

    def hloc(kind, owner, k, half, part=None):
        p = pos_of(kind, k)
        return H.at[half, p // 4, rows_of(0, part), pl.ds((p % 4) * LN, LN)]

    def xloc(kind, owner, k, half, part):
        return XF.at[rows_of(half * hn, part), pl.ds(pl.multiple_of(owner * dt + k * LN, LN), LN)]

    class Gather:
        def __init__(self, loc, half):
            self.loc, self.half = loc, half

        def copy(self, i, k, kind, there, owner, dev, part=None):
            h = self.half
            return rcopy(self.loc(kind, owner, k, h, part), self.loc(there, owner, k, h, part), ags.at[h, i, k], agr.at[h, i, k], dev)

        def c_up(self, k):
            return self.copy(0, k, 'own', 'dn', t, up)

        def c_dn(self, k):
            return self.copy(1, k, 'own', 'up', t, dn)

        def r_up(self, k):
            return self.copy(2, k, 'dn', 'op', dn, up, 0)

        def r_dn(self, k):
            return self.copy(3, k, 'up', 'op', up, dn, 1)

        def send(self, k):
            self.c_up(k).start()
            self.c_dn(k).start()

        def wait(self, kind, k):
            if kind == 'dn':
                self.copy(0, k, kind, kind, dn, up).wait_recv()
                self.r_up(k).start()
            elif kind == 'up':
                self.copy(1, k, kind, kind, up, dn).wait_recv()
                self.r_dn(k).start()
            elif kind == 'op':
                self.copy(2, k, kind, kind, op, up, 0).wait_recv()
                self.copy(3, k, kind, kind, op, dn, 1).wait_recv()

        def sent(self, k):
            for cp in (self.c_up, self.c_dn, self.r_up, self.r_dn):
                cp(k).wait_send()

    def h_in(half, k):
        return pltpu.make_async_copy(h_ref.at[pl.ds(half * hn, hn), pl.ds(k * LN, LN)], hloc('own', t, k, half), lsem.at[half])

    for half in range(2):
        for k in range(KP):
            h_in(half, k).start()
    xin = pltpu.make_async_copy(x_ref, xm, lsem.at[2])
    xin.start()

    def w_start(gi):
        i = lax.rem(gi, SUB)
        slot = lax.rem(gi, NSLOT)
        for q in range(4):
            p = (i // 2) * 4 + q
            own = p < KP
            pair = jnp.logical_and(p >= KP, p < 3 * KP)
            k = jnp.where(own, p, jnp.where(pair, (p - KP) // 2, p - 3 * KP))
            who = jnp.where(own, t, jnp.where(pair, jnp.where(lax.rem(p - KP, 2) == 0, up, dn), op))
            row = pl.multiple_of(who * dt + k * LN, LN)
            dst = ring.at[slot, pl.ds(q * LN, LN), :]

            @pl.when(lax.rem(i, 2) == 0)
            def _():
                pltpu.make_async_copy(wg_ref.at[layer, pl.ds(row, LN), :], dst, wsem.at[slot]).start()

            @pl.when(lax.rem(i, 2) == 1)
            def _():
                pltpu.make_async_copy(wu_ref.at[layer, pl.ds(row, LN), :], dst, wsem.at[slot]).start()

    def w_wait(slot):
        pltpu.make_async_copy(wg_ref.at[layer, pl.ds(0, 4 * LN), :], ring.at[slot], wsem.at[slot]).wait()

    def d_col(p):
        c = p // KP
        who = jnp.where(c == 0, op, jnp.where(c == 1, up, jnp.where(c == 2, dn, t)))
        return pl.multiple_of(who * dt + lax.rem(p, KP) * LN, LN)

    def d_start(gi):
        i = lax.rem(gi, TL)
        slot = lax.rem(gi, ND)
        for q in range(2):
            pltpu.make_async_copy(wd_ref.at[layer, :, pl.ds(d_col(2 * i + q), LN)],
                                  wdb.at[slot, :, pl.ds(q * LN, LN)], dsem.at[slot]).start()

    def d_wait(slot):
        pltpu.make_async_copy(wd_ref.at[layer, :, pl.ds(0, 2 * LN)], wdb.at[slot], dsem.at[slot]).wait()

    for s in range(NSLOT):
        w_start(jnp.int32(s))
    for k in range(KP):
        h_in(0, k).wait()
    pl.semaphore_wait(barrier, 3)
    for k in range(KP):
        Gather(hloc, 0).send(k)
    for k in range(KP):
        h_in(1, k).wait()

    def zero(j, c):
        acc[j] = jnp.zeros(acc.shape[1:], acc.dtype)
        return c

    lax.fori_loop(0, 2 * FP, zero, 0)
    for s in range(ND):
        d_start(jnp.int32(s))

    class Scatter:
        def __init__(self, half):
            self.half = half

        def copy(self, i, k, piece, part, dst, dev):
            h = self.half
            return rcopy(PS.at[h, piece, rows_of(0, part), :], dst, rss.at[h, i, k], rsr.at[h, i, k], dev)

        def opA(self, k):
            return self.copy(0, k, k, 0, RA.at[self.half, k], up)

        def opB(self, k):
            return self.copy(1, k, k, 1, RB.at[self.half, k], dn)

        def upB(self, k):
            return self.copy(2, k, KP + k, 1, RD.at[self.half, k, rows_of(0, 1), :], up)

        def dnA(self, k):
            return self.copy(3, k, 2 * KP + k, 0, RU.at[self.half, k, rows_of(0, 0), :], dn)

        def upA(self, k):
            return self.copy(4, k, KP + k, 0, RD.at[self.half, k, rows_of(0, 0), :], up)

        def dnB(self, k):
            return self.copy(5, k, 2 * KP + k, 1, RU.at[self.half, k, rows_of(0, 1), :], dn)

        def send(self, p):
            c = p // KP
            k = lax.rem(p, KP)

            @pl.when(c == 0)
            def _():
                self.opA(k).start()
                self.opB(k).start()

            @pl.when(c == 1)
            def _():
                self.upB(k).start()

            @pl.when(c == 2)
            def _():
                self.dnA(k).start()

        def add(self, k, c):
            h = self.half
            self.opA(k).wait_recv()
            PS[h, KP + k, 0:qn, :] += RA[h, k]
            self.upA(k).start()
            self.opB(k).wait_recv()
            PS[h, 2 * KP + k, qn:hn, :] += RB[h, k]
            self.dnB(k).start()
            return c

        def total(self, k, c):
            h = self.half
            for cp in (self.upB, self.dnA, self.upA, self.dnB):
                cp(k).wait_recv()
            s = PS[h, 3 * KP + k] + RD[h, k] + RU[h, k]
            rows = rows_of(h * hn)
            v = xm[rows, pl.ds(pl.multiple_of(k * LN, LN), LN)] + s.astype(jnp.bfloat16)
            XF[rows, pl.ds(pl.multiple_of(t * dt + k * LN, LN), LN)] = v
            Gather(xloc, h).send(k)
            return c

        def near(self, k, c):
            Gather(xloc, self.half).wait('up', k)
            Gather(xloc, self.half).wait('dn', k)
            return c

        def far(self, k, c):
            Gather(xloc, self.half).wait('op', k)
            return c

        def sent(self, k, c):
            Gather(xloc, self.half).sent(k)
            for cp in (self.opA, self.opB, self.upB, self.dnA, self.upA, self.dnB):
                cp(k).wait_send()
            return c

    first, second = Scatter(0), Scatter(1)

    def each(fn):
        lax.fori_loop(0, KP, fn, 0)

    later = [(0, min(2 * g, SUB - 1), (lambda k: lambda: Gather(hloc, 1).send(k))(k)) for k, g in
             zip(range(KP), (2, 3, 3, 4, 4, 5, 6))]
    later += [(1, 0, xin.wait), (1, 1, lambda: each(first.add)), (1, SUB - 2, lambda: each(first.total))]

    def half_step(half, carry):
        gh = Gather(hloc, half)
        rsh = Scatter(half)

        def gu_step(i, c):
            j = i // 2
            gi = half * SUB + i
            slot = lax.rem(gi, NSLOT)
            for jj in range(NG):
                @pl.when(i == 2 * jj)
                def _():
                    for kind, k in order[4 * jj:4 * jj + 4]:
                        gh.wait(kind, k)
            for hh, at, fn in later:
                @pl.when(jnp.logical_and(half == hh, i == at))
                def _():
                    fn()
            w_wait(slot)
            base = lax.rem(i, 2) * FP
            for f in range(0, FP, 4):
                m = min(4, FP - f)
                r = mm(H[half, j], ring[slot, :, f * LN:(f + m) * LN])
                for q in range(m):
                    acc[base + f + q] += r[:, q * LN:(q + 1) * LN]

            @pl.when(gi + NSLOT < 2 * SUB)
            def _():
                w_start(gi + NSLOT)
            return c

        lax.fori_loop(0, SUB, gu_step, 0)

        def silu(f, c):
            a = acc[f].astype(jnp.bfloat16).astype(jnp.float32)
            b = acc[FP + f].astype(jnp.bfloat16).astype(jnp.float32)
            U[:, pl.ds(pl.multiple_of(f * LN, LN), LN)] = (a * (1.0 / (1.0 + jnp.exp(-a))) * b).astype(jnp.bfloat16)
            acc[f] = jnp.zeros(acc.shape[1:], acc.dtype)
            acc[FP + f] = jnp.zeros(acc.shape[1:], acc.dtype)
            return c

        lax.fori_loop(0, FP, silu, 0)
        for k in range(KP):
            gh.sent(k)

        def tile(i, c):
            gi = half * TL + i
            slot = lax.rem(gi, ND)

            @pl.when(jnp.logical_and(half == 1, i == min(4, TL - 1)))
            def _():
                each(first.near)

            d_wait(slot)

            @pl.when(i > 0)
            def _():
                rsh.send(2 * i - 2)
                rsh.send(2 * i - 1)

            r = mm(U[...], wdb[slot])
            for q in range(2):
                PS[half, 2 * i + q] = r[:, q * LN:(q + 1) * LN]

            @pl.when(gi + ND < 2 * TL)
            def _():
                d_start(gi + ND)
            return c

        lax.fori_loop(0, TL, tile, 0)
        return carry

    lax.fori_loop(0, 2, half_step, 0)
    each(second.add)
    each(first.far)
    each(second.total)
    each(second.near)
    each(second.far)
    o = pltpu.make_async_copy(XF, out_ref, lsem.at[0])
    o.start()
    each(first.sent)
    each(second.sent)
    o.wait()


def mlp(T, layer, h, x, wg, wu, wd, cid):
    n, dt = x.shape
    F = wg.shape[2]
    d = dt * T
    KP = dt // LN
    FP = F // LN
    hn = n // 2
    NG = T * KP // 4
    f32, bf = jnp.float32, jnp.bfloat16
    anyspec = pl.BlockSpec(memory_space=pltpu.HBM)
    D = pltpu.SemaphoreType.DMA
    return pl.pallas_call(
        functools.partial(mlp_kernel, T, layer),
        out_shape=jax.ShapeDtypeStruct((n, d), bf),
        in_specs=[anyspec] * 5,
        out_specs=anyspec,
        scratch_shapes=[
            pltpu.VMEM((2 * FP, hn, LN), f32),
            pltpu.VMEM((2, T * KP, hn, LN), f32),
            pltpu.VMEM((3, 4 * LN, F), bf),
            pltpu.VMEM((2, NG, hn, 4 * LN), bf),
            pltpu.VMEM((hn, F), bf),
            pltpu.VMEM((3, F, 2 * LN), bf),
            pltpu.VMEM((2, KP, hn // 2, LN), f32),
            pltpu.VMEM((2, KP, hn // 2, LN), f32),
            pltpu.VMEM((2, KP, hn, LN), f32),
            pltpu.VMEM((2, KP, hn, LN), f32),
            pltpu.VMEM((n, d), bf),
            pltpu.VMEM((n, dt), bf),
            D((2, 4, KP)), D((2, 4, KP)), D((2, 6, KP)), D((2, 6, KP)), D((3,)), D((3,)), D((3,)),
        ],
        compiler_params=pltpu.CompilerParams(vmem_limit_bytes=VMEM_LIMIT, collective_id=cid, has_side_effects=True),
        name="mlp",
    )(h, x, wg, wu, wd)


def solution(mesh):
    sp = mesh.shape['sp']
    tp = mesh.shape['tp']
    row = ('dp', 'sp')
    kv_spec = P(None, row, 'tp', None)
    col = P(None, None, 'tp')
    rowsplit = P(None, 'tp', None)

    def body(x, pos, k_hist, v_hist, wq, wk, wv, wo, wg, wu, wd, g1, g2):
        n, d = x.shape
        layers, hc, kvl, dh = k_hist.shape
        kh, vh = k_hist.reshape(layers, hc, dh), v_hist.reshape(layers, hc, dh)
        lane = jnp.arange(dh)
        inv = ROPE_THETA ** (-((lane % (dh // 2)).astype(jnp.float32) * (2.0 / dh)))
        ang = pos.astype(jnp.float32)[:, None] * inv
        cos = jnp.cos(ang)
        sin = jnp.sin(ang) * jnp.where(lane < dh // 2, -1.0, 1.0)
        ks, vs = [], []
        for l in range(layers):
            h, xm, k, v = attention(tp, sp, l, x, cos, sin, kh, vh, wq, wk, wv, wo, g1, g2, 2 * l)
            ks.append(k.reshape(n, kvl, dh))
            vs.append(v.reshape(n, kvl, dh))
            x = mlp(tp, l, h, xm, wg, wu, wd, 2 * l + 1)
        return x, jnp.stack(ks), jnp.stack(vs)

    in_specs = (P(row, None), P(row), kv_spec, kv_spec, col, col, col, rowsplit, col, col, rowsplit, P(), P())
    out_specs = (P(row, None), kv_spec, kv_spec)
    return jax.shard_map(body, mesh=mesh, in_specs=in_specs, out_specs=out_specs, check_vma=False)
```

```python
import functools

import jax
import jax.numpy as jnp
from jax import lax
from jax.experimental import pallas as pl
from jax.experimental.pallas import tpu as pltpu
from jax.sharding import PartitionSpec as P

EPS = 1e-5
ROPE_THETA = 500000.0
LOG2E = 1.4426950408889634
MESH = pl.DeviceIdType.MESH
LN = 128
VMEM_LIMIT = 61 * 2 ** 20


def mm(a, b):
    return jnp.dot(a, b, preferred_element_type=jnp.float32)


def attn_kernel(T, SP, layer, x_ref, cos_ref, sin_ref, kh_ref, vh_ref, wq_ref, wk_ref, wv_ref, wo_ref, g_ref, g2_ref,
                ho_ref, xo_ref, ko_ref, vo_ref,
                xb, wb, kb, vt, vs, qb, m_ref, l_ref, acc_ref, ga, wob, xm, hb, st, strv,
                kvs, kvr, gas, gar, wys, wyr, sts, strs, lsem, hsem, wsem):
    n, d = xb.shape
    w = qb.shape[1]
    dh = kb.shape[2]
    heads = w // dh
    X = SP // 2
    C = kb.shape[1]
    hc = C // 2
    dt = w
    nt = 2
    R = n // nt
    NS = 2
    SR = R // NS
    scale = dh ** -0.5 * LOG2E
    me = lax.axis_index("sp")
    t = lax.axis_index("tp")
    c = lax.rem(me, 2)
    xx = me // 2
    lx, rx, ox = lax.rem(xx + X - 1, X), lax.rem(xx + 1, X), lax.rem(xx + 2, X)
    left, right, part = lx * 2 + c, rx * 2 + c, xx * 2 + 1 - c
    up, dn, far = lax.rem(t + 1, T), lax.rem(t + T - 1, T), lax.rem(t + 2, T)

    barrier = pltpu.get_barrier_semaphore()
    for dev in ({"sp": left}, {"sp": right}, {"sp": part}, {"tp": up}, {"tp": dn}, {"tp": far}):
        pl.semaphore_signal(barrier, inc=1, device_id=dev, device_id_type=MESH)

    hown = pl.ds(pl.multiple_of(c * hc, hc), hc)
    hist_in = (pltpu.make_async_copy(kh_ref.at[layer], kb.at[xx, hown, :], hsem.at[0]),
               pltpu.make_async_copy(vh_ref.at[layer], vs, hsem.at[1]))
    for cp in hist_in:
        cp.start()
    xin = pltpu.make_async_copy(x_ref, xb, lsem.at[0])
    xin.start()
    win = [pltpu.make_async_copy(wk_ref.at[layer], wb.at[:, 0:dh], wsem.at[0]),
           pltpu.make_async_copy(wv_ref.at[layer], wb.at[:, dh:2 * dh], wsem.at[0]),
           pltpu.make_async_copy(wq_ref.at[layer], wb.at[:, 2 * dh:], wsem.at[1])]
    for cp in win:
        cp.start()

    def wo_cols(dev):
        return wo_ref.at[layer, :, me, :, pl.ds(pl.multiple_of(dev * dt, LN), dt)]

    wo_own = pltpu.make_async_copy(wo_cols(t), wob.at[t, :, me], wsem.at[2])
    wo_own.start()
    xcol = pltpu.make_async_copy(x_ref.at[:, pl.ds(pl.multiple_of(t * dt, LN), dt)], xm, lsem.at[1])
    xcol.start()
    peers = [(j, *e) for j, e in enumerate(((up, dn), (dn, up), (far, far)))]

    def wo_tx(j, dev):
        return pltpu.make_async_remote_copy(src_ref=wo_cols(dev), dst_ref=wob.at[t, :, me], send_sem=wys.at[j],
                                            recv_sem=wyr.at[j], device_id={"tp": dev}, device_id_type=MESH)

    def wo_rx(j, src):
        pltpu.make_async_remote_copy(src_ref=wob.at[src, :, me], dst_ref=wob.at[src, :, me], send_sem=wys.at[j],
                                     recv_sem=wyr.at[j], device_id={"tp": src}, device_id_type=MESH).wait_recv()

    def region(kind, chip, core, half=None):
        if kind == 2:
            if half is None:
                return wob.at[:, :, chip * 2 + core]
            return wob.at[pl.ds(half * (T // 2), T // 2), :, chip * 2 + core]
        if kind % 3 == 0:
            blk, base, ln = chip, core * hc, hc
        else:
            blk, base, ln = X + chip // 2, lax.rem(chip, 2) * (2 * n) + core * n, n
        if half is not None:
            ln = ln // 2
            base = base + half * ln
        part_ = pl.ds(pl.multiple_of(base, ln), ln)
        return kb.at[blk, part_, :] if kind < 3 else vt.at[blk, :, part_]

    whole, other = None, 1 - c
    relayed = (2, 5, 6, 7, 8)
    sent = [(xx, c, whole, right), (xx, c, whole, left), (xx, c, whole, part), (lx, c, 0, right), (rx, c, 1, left),
            (lx, c, whole, part), (rx, c, whole, part), (ox, c, 0, part), (ox, c, 1, part)]
    got = [(lx, c, whole), (rx, c, whole), (xx, other, whole), (ox, c, 0), (ox, c, 1),
           (lx, other, whole), (rx, other, whole), (ox, other, 0), (ox, other, 1)]

    def tx(kind, i):
        chip, core, half, dev = sent[i]
        r = region(kind, chip, core, half)
        return pltpu.make_async_remote_copy(src_ref=r, dst_ref=r, send_sem=kvs.at[kind, i], recv_sem=kvr.at[kind, i],
                                            device_id={"sp": dev}, device_id_type=MESH)

    def rx_wait(kind, i):
        chip, core, half = got[i]
        r = region(kind, chip, core, half)
        pltpu.make_async_remote_copy(src_ref=r, dst_ref=r, send_sem=kvs.at[kind, i], recv_sem=kvr.at[kind, i],
                                     device_id={"sp": part}, device_id_type=MESH).wait_recv()

    def send_own(kind):
        for i in (0, 1, 2):
            tx(kind, i).start()

    def pass_near(kind):
        rx_wait(kind, 0)
        tx(kind, 3).start()
        tx(kind, 5).start()
        rx_wait(kind, 1)
        tx(kind, 4).start()
        tx(kind, 6).start()

    def pass_far(kind):
        rx_wait(kind, 3)
        tx(kind, 7).start()
        rx_wait(kind, 4)
        tx(kind, 8).start()

    pl.semaphore_wait(barrier, 6)
    hist_in[0].wait()
    send_own(0)
    hist_in[1].wait()
    vt[xx, :, hown] = jnp.swapaxes(vs[...].astype(jnp.float32), 0, 1).astype(jnp.bfloat16)
    send_own(3)
    for j, dev, _ in peers:
        wo_tx(j, dev).start()

    xin.wait()
    g = g_ref[layer:layer + 1, :].astype(jnp.float32)
    NR = min(LN, n)

    def norm(i, carry):
        rows = pl.ds(pl.multiple_of(i * NR, NR), NR)
        xf = xb[rows, :].astype(jnp.float32)
        r = lax.rsqrt(jnp.sum(xf * xf, axis=1, keepdims=True) / d + EPS)
        xb[rows, :] = (xf * r * g).astype(jnp.bfloat16)
        return carry

    lax.fori_loop(0, n // NR, norm, 0)

    def rope(a):
        a = a.astype(jnp.bfloat16).astype(jnp.float32)
        return (a * cos_ref[...] + pltpu.roll(a, dh // 2, 1) * sin_ref[...]).astype(jnp.bfloat16)

    win[0].wait()
    win[1].wait()
    own = pl.ds(pl.multiple_of(lax.rem(xx, 2) * (2 * n) + c * n, n), n)

    def qkv_pair(i, carry):
        @pl.when(i == 1)
        def _():
            win[2].wait()

        @pl.when(i == 2)
        def _():
            send_own(1)
            send_own(4)

        h0 = jnp.minimum(2 * i - 2, heads - 2)
        r = mm(xb[...], wb[:, pl.ds(pl.multiple_of((h0 + 2) * dh, dh), 2 * dh)])

        @pl.when(i == 0)
        def _():
            kb[X + xx // 2, own, :] = rope(r[:, :dh])
            vs[0:n, :] = r[:, dh:].astype(jnp.bfloat16)
            vt[X + xx // 2, :, own] = jnp.swapaxes(r[:, dh:], 0, 1).astype(jnp.bfloat16)

        @pl.when(i > 0)
        def _():
            for j in range(2):
                qb[:, pl.ds(pl.multiple_of((h0 + j) * dh, dh), dh)] = rope(r[:, j * dh:(j + 1) * dh])
        return carry

    lax.fori_loop(0, 1 + (heads + 1) // 2, qkv_pair, 0)

    kv_out = (pltpu.make_async_copy(kb.at[X + xx // 2, own, :], ko_ref, hsem.at[0]),
              pltpu.make_async_copy(vs.at[0:n, :], vo_ref, hsem.at[1]))
    for cp in kv_out:
        cp.start()

    m_ref[...] = jnp.full(m_ref.shape, -1e30, jnp.float32)
    l_ref[...] = jnp.zeros_like(l_ref)

    def init(h, carry):
        acc_ref[h] = jnp.zeros(acc_ref.shape[1:], jnp.float32)
        return carry

    lax.fori_loop(0, heads, init, 0)

    def unit(tile, blk, off, cn, mask=None):
        rows = pl.ds(pl.multiple_of(tile * R, R), R)

        sn = C // 4
        chain = [(h, j * sn) for h in range(heads) for j in range(cn // sn)]

        def qk(h, j):
            return lax.dot_general(kb[blk, pl.ds(off + j, sn), :], qb[rows, h * dh:(h + 1) * dh], (((1,), (1,)), ((), ())),
                                   preferred_element_type=jnp.float32)

        def pv(h, j, p, alpha):
            acc_ref[h, :, rows] = acc_ref[h, :, rows] * alpha + mm(vt[blk, :, pl.ds(off + j, sn)], p)

        ahead = 2
        scores = [qk(*e) for e in chain[:ahead]]
        pend = []
        for i, (h, j) in enumerate(chain):
            if i + ahead < len(chain):
                scores.append(qk(*chain[i + ahead]))
            s = scores.pop(0)
            if len(pend) == ahead:
                pv(*pend.pop(0))
            if mask is not None:
                s = jnp.where(mask(j, sn), s, -jnp.inf)
            m_old = m_ref[h, :, rows]
            m_new = jnp.maximum(m_old, jnp.max(s, axis=0, keepdims=True) * scale)
            alpha = jnp.exp2(m_old - m_new)
            p = jnp.exp2(s * scale - m_new)
            l_ref[h, :, rows] = l_ref[h, :, rows] * alpha + jnp.sum(p.reshape(sn // 8, 8, R), axis=0)
            m_ref[h, :, rows] = m_new
            pend.append((h, j, p.astype(jnp.bfloat16), alpha))
        for e in pend:
            pv(*e)

    hR = SR // 2

    def gx(i, sub):
        base = pl.multiple_of(sub * SR, SR)
        owner, off, ln, dev = ((t, 0, SR, up), (t, 0, SR, dn), (dn, 0, hR, up), (up, hR, hR, dn))[i]
        ref = ga.at[owner, pl.ds(pl.multiple_of(base + off, hR), ln), :]
        return pltpu.make_async_remote_copy(src_ref=ref, dst_ref=ref, send_sem=gas.at[i, sub], recv_sem=gar.at[i, sub],
                                            device_id={"tp": dev}, device_id_type=MESH)

    def g_wait(i, sub):
        base = pl.multiple_of(sub * SR, SR)
        owner, off, ln = ((dn, 0, SR), (up, 0, SR), (far, 0, hR), (far, hR, hR))[i]
        ref = ga.at[owner, pl.ds(pl.multiple_of(base + off, hR), ln), :]
        pltpu.make_async_remote_copy(src_ref=ref, dst_ref=ref, send_sem=gas.at[i, sub], recv_sem=gar.at[i, sub],
                                     device_id={"tp": up}, device_id_type=MESH).wait_recv()

    def g_pass(sub):
        g_wait(0, sub)
        gx(2, sub).start()
        g_wait(1, sub)
        gx(3, sub).start()

    def finish(tile):
        rows = pl.ds(pl.multiple_of(tile * R, R), R)
        for h in range(heads):
            l = jnp.sum(l_ref[h, :, rows], axis=0, keepdims=True)
            ga[t, rows, h * dh:(h + 1) * dh] = jnp.swapaxes(acc_ref[h, :, rows] / l, 0, 1).astype(jnp.bfloat16)

    def s_copy(j, dev, sub):
        return pltpu.make_async_remote_copy(src_ref=st.at[sub], dst_ref=strv.at[j, sub], send_sem=sts.at[j, sub],
                                            recv_sem=strs.at[j, sub], device_id={"tp": dev}, device_id_type=MESH)

    def wo_sub(sub):
        rows = pl.ds(pl.multiple_of(sub * SR, SR), SR)

        def part(j):
            return mm(ga[j, rows, :], wob[j].reshape(dt, dt))

        y = part(t) + part(up) + part(dn)
        g_wait(2, sub)
        g_wait(3, sub)
        y = y + part(far)
        v = xm[rows, :] + y.astype(jnp.bfloat16)
        xm[rows, :] = v
        vf = v.astype(jnp.float32)
        sb = jnp.broadcast_to(jnp.sum(vf * vf, axis=1, keepdims=True), (SR, LN))
        st[sub] = jnp.swapaxes(sb, 0, 1)[:8]
        for j, dev, _ in peers:
            s_copy(j, dev, sub).start()

    def h_sub(sub):
        rows = pl.ds(pl.multiple_of(sub * SR, SR), SR)
        for j, dev, _ in peers:
            s_copy(j, dev, sub).wait_recv()
        tot = st[sub] + strv[0, sub] + strv[1, sub] + strv[2, sub]
        r8 = lax.rsqrt(tot / d + EPS)
        rb = jnp.swapaxes(jnp.concatenate([r8] * (LN // 8), axis=0), 0, 1)
        for k in range(dt // LN):
            cols = slice(k * LN, (k + 1) * LN)
            gk = g2_ref[layer:layer + 1, pl.ds(pl.multiple_of(t * dt + k * LN, LN), LN)].astype(jnp.float32)
            hb[rows, cols] = (xm[rows, cols].astype(jnp.float32) * rb * gk).astype(jnp.bfloat16)

    rx_wait(0, 2)
    rx_wait(3, 2)
    first = 3 * nt
    per = 1 + xx // 2
    total = first + nt * per

    def near(kind):
        pass_near(kind)
        pass_near(kind + 3)
        if kind == 1:
            wo_own.wait()
            for j, _, src in peers:
                wo_rx(j, src)
            send_own(2)

    def far_(kind):
        pass_far(kind)
        pass_far(kind + 3)

    points = ((1, near, 0), (2, near, 1), (4, far_, 0), (5, far_, 1), (first + per, pass_near, 2))

    def step(i, carry):
        for at, fn, kind in points:
            @pl.when(i == at)
            def _():
                fn(kind)

        for chip_at, gid in ((nt, 5), (2 * nt, 6)):
            @pl.when(i == chip_at)
            def _():
                rx_wait(0, gid)
                rx_wait(3, gid)

        @pl.when(i == first)
        def _():
            for kind in (0, 3):
                rx_wait(kind, 7)
                rx_wait(kind, 8)
            for kind in (1, 4):
                for gid in relayed:
                    rx_wait(kind, gid)

        late = i >= first
        i2 = jnp.maximum(i - first, 0)
        m = lax.rem(i2, per)
        tile = jnp.where(late, i2 // per, lax.rem(i, nt))
        early = jnp.where(i < nt, xx, jnp.where(i < 2 * nt, lx, rx))
        blk = jnp.where(late, jnp.where(m == 0, ox, X + m - 1), early)
        last = jnp.logical_and(late, m == per - 1)
        unit(tile, blk, 0, C)

        @pl.when(last)
        def _():
            @pl.when(tile == 1)
            def _():
                g_pass(0)

            @pl.when(lax.rem(xx, 2) == 1)
            def _():
                unit(tile, X + xx // 2, 0, hc)

            def causal(j, sn):
                row = lax.broadcasted_iota(jnp.int32, (sn, R), 1) + (c * n + tile * R - j)
                return lax.broadcasted_iota(jnp.int32, (sn, R), 0) <= row

            unit(tile, X + xx // 2, pl.multiple_of(lax.rem(xx, 2) * hc, hc), hc, causal)
            finish(tile)
            for sub in range(NS):
                gx(0, tile * NS + sub).start()
                gx(1, tile * NS + sub).start()
        return carry

    lax.fori_loop(0, total, step, 0)

    nsub = nt * NS
    g_pass(1)
    pass_far(2)
    for gid in relayed:
        rx_wait(2, gid)
    xcol.wait()

    def tail(j, carry):
        @pl.when(j < nsub)
        def _():
            wo_sub(j)

        @pl.when(j + 2 < nsub)
        def _():
            g_pass(j + 2)

        @pl.when(j >= 1)
        def _():
            h_sub(j - 1)
        return carry

    lax.fori_loop(0, nsub + 1, tail, 0)
    o1 = pltpu.make_async_copy(hb, ho_ref, lsem.at[0])
    o2 = pltpu.make_async_copy(xm, xo_ref, lsem.at[1])
    o1.start()
    o2.start()
    for sub in range(nt * NS):
        for i in range(4):
            gx(i, sub).wait_send()
        for j, dev, _ in peers:
            s_copy(j, dev, sub).wait_send()
    for j, dev, _ in peers:
        wo_tx(j, dev).wait_send()
    for kind in range(5):
        for i in range(len(sent)):
            tx(kind, i).wait_send()
    for cp in kv_out:
        cp.wait()
    o1.wait()
    o2.wait()


def attention(T, SP, layer, x, cos, sin, kh, vh, wq, wk, wv, wo, g, g2, cid):
    n, d = x.shape
    w = wq.shape[2]
    hc, dh = kh.shape[1], kh.shape[2]
    heads = w // dh
    X = SP // 2
    assert 2 * hc == 4 * n and wk.shape[2] == dh and w * T == d
    nt = 2
    R = n // nt
    f32, bf = jnp.float32, jnp.bfloat16
    hbm = pl.BlockSpec(memory_space=pltpu.HBM)
    vm = pl.BlockSpec(memory_space=pltpu.VMEM)
    D = pltpu.SemaphoreType.DMA
    return pl.pallas_call(
        functools.partial(attn_kernel, T, SP, layer),
        out_shape=[jax.ShapeDtypeStruct((n, w), bf), jax.ShapeDtypeStruct((n, w), bf),
                   jax.ShapeDtypeStruct((n, dh), bf), jax.ShapeDtypeStruct((n, dh), bf)],
        in_specs=[hbm, vm, vm, hbm, hbm, hbm, hbm, hbm, hbm, vm, vm],
        out_specs=[hbm, hbm, hbm, hbm],
        scratch_shapes=[
            pltpu.VMEM((n, d), bf),
            pltpu.VMEM((d, w + 2 * dh), bf),
            pltpu.VMEM((X + X // 2, 2 * hc, dh), bf),
            pltpu.VMEM((X + X // 2, dh, 2 * hc), bf),
            pltpu.VMEM((hc, dh), bf),
            pltpu.VMEM((n, w), bf),
            pltpu.VMEM((heads, 1, n), f32),
            pltpu.VMEM((heads, 8, n), f32),
            pltpu.VMEM((heads, dh, n), f32),
            pltpu.VMEM((T, n, w), bf),
            pltpu.VMEM((T, w // LN, SP, LN // SP, w), bf),
            pltpu.VMEM((n, w), bf),
            pltpu.VMEM((n, w), bf),
            pltpu.VMEM((4, 8, n // 4), f32),
            pltpu.VMEM((3, 4, 8, n // 4), f32),
            D((5, 9)), D((5, 9)), D((4, 4)), D((4, 4)), D((3,)), D((3,)), D((3, 4)), D((3, 4)), D((2,)), D((2,)), D((3,)),
        ],
        compiler_params=pltpu.CompilerParams(vmem_limit_bytes=VMEM_LIMIT, collective_id=cid, has_side_effects=True),
        name="attention",
    )(x, cos, sin, kh, vh, wq, wk, wv, wo.reshape(wo.shape[0], w // LN, SP, LN // SP, d), g, g2)


def mlp_kernel(T, layer, h_ref, x_ref, wg_ref, wu_ref, wd_ref, out_ref,
               acc, PS, ring, H, U, wdb, RA, RB, RD, RU, XF, xm,
               ags, agr, rss, rsr, lsem, wsem, dsem):
    n, d = XF.shape
    dt = d // T
    KP = dt // LN
    NP = T * KP
    NG = NP // 4
    F = U.shape[1]
    FP = F // LN
    hn = n // 2
    qn = hn // 2
    NSLOT = ring.shape[0]
    ND = wdb.shape[0]
    SUB = 2 * NG
    TL = NP // 2
    t = lax.axis_index("tp")
    up = lax.rem(t + 1, T)
    dn = lax.rem(t + 3, T)
    op = lax.rem(t + 2, T)

    barrier = pltpu.get_barrier_semaphore()
    for dev in (up, dn, op):
        pl.semaphore_signal(barrier, inc=1, device_id={"tp": dev}, device_id_type=MESH)

    def rcopy(src, dst, ss, rs, dev):
        return pltpu.make_async_remote_copy(src_ref=src, dst_ref=dst, send_sem=ss, recv_sem=rs,
                                            device_id={"tp": dev}, device_id_type=MESH)

    def pos_of(kind, k):
        return {'own': k, 'up': KP + 2 * k, 'dn': KP + 2 * k + 1, 'op': 3 * KP + k}[kind]

    order = [None] * NP
    for kind in ('own', 'up', 'dn', 'op'):
        for k in range(KP):
            order[pos_of(kind, k)] = (kind, k)

    def rows_of(base, part=None):
        if part is None:
            return pl.ds(base if isinstance(base, int) else pl.multiple_of(base, hn), hn)
        return pl.ds(base + part * qn if isinstance(base, int) else pl.multiple_of(base + part * qn, qn), qn)

    def hloc(kind, owner, k, half, part=None):
        p = pos_of(kind, k)
        return H.at[half, p // 4, rows_of(0, part), pl.ds((p % 4) * LN, LN)]

    def xloc(kind, owner, k, half, part):
        return XF.at[rows_of(half * hn, part), pl.ds(pl.multiple_of(owner * dt + k * LN, LN), LN)]

    class Gather:
        def __init__(self, loc, half):
            self.loc, self.half = loc, half

        def copy(self, i, k, kind, there, owner, dev, part=None):
            h = self.half
            return rcopy(self.loc(kind, owner, k, h, part), self.loc(there, owner, k, h, part), ags.at[h, i, k], agr.at[h, i, k], dev)

        def c_up(self, k):
            return self.copy(0, k, 'own', 'dn', t, up)

        def c_dn(self, k):
            return self.copy(1, k, 'own', 'up', t, dn)

        def r_up(self, k):
            return self.copy(2, k, 'dn', 'op', dn, up, 0)

        def r_dn(self, k):
            return self.copy(3, k, 'up', 'op', up, dn, 1)

        def send(self, k):
            self.c_up(k).start()
            self.c_dn(k).start()

        def wait(self, kind, k):
            if kind == 'dn':
                self.copy(0, k, kind, kind, dn, up).wait_recv()
                self.r_up(k).start()
            elif kind == 'up':
                self.copy(1, k, kind, kind, up, dn).wait_recv()
                self.r_dn(k).start()
            elif kind == 'op':
                self.copy(2, k, kind, kind, op, up, 0).wait_recv()
                self.copy(3, k, kind, kind, op, dn, 1).wait_recv()

        def sent(self, k):
            for cp in (self.c_up, self.c_dn, self.r_up, self.r_dn):
                cp(k).wait_send()

    def h_in(half, k):
        return pltpu.make_async_copy(h_ref.at[pl.ds(half * hn, hn), pl.ds(k * LN, LN)], hloc('own', t, k, half), lsem.at[half])

    for half in range(2):
        for k in range(KP):
            h_in(half, k).start()
    xin = pltpu.make_async_copy(x_ref, xm, lsem.at[2])
    xin.start()

    def w_start(gi):
        i = lax.rem(gi, SUB)
        slot = lax.rem(gi, NSLOT)
        for q in range(4):
            p = (i // 2) * 4 + q
            own = p < KP
            pair = jnp.logical_and(p >= KP, p < 3 * KP)
            k = jnp.where(own, p, jnp.where(pair, (p - KP) // 2, p - 3 * KP))
            who = jnp.where(own, t, jnp.where(pair, jnp.where(lax.rem(p - KP, 2) == 0, up, dn), op))
            row = pl.multiple_of(who * dt + k * LN, LN)
            dst = ring.at[slot, pl.ds(q * LN, LN), :]

            @pl.when(lax.rem(i, 2) == 0)
            def _():
                pltpu.make_async_copy(wg_ref.at[layer, pl.ds(row, LN), :], dst, wsem.at[slot]).start()

            @pl.when(lax.rem(i, 2) == 1)
            def _():
                pltpu.make_async_copy(wu_ref.at[layer, pl.ds(row, LN), :], dst, wsem.at[slot]).start()

    def w_wait(slot):
        pltpu.make_async_copy(wg_ref.at[layer, pl.ds(0, 4 * LN), :], ring.at[slot], wsem.at[slot]).wait()

    def d_col(p):
        c = p // KP
        who = jnp.where(c == 0, op, jnp.where(c == 1, up, jnp.where(c == 2, dn, t)))
        return pl.multiple_of(who * dt + lax.rem(p, KP) * LN, LN)

    def d_start(gi):
        i = lax.rem(gi, TL)
        slot = lax.rem(gi, ND)
        for q in range(2):
            pltpu.make_async_copy(wd_ref.at[layer, :, pl.ds(d_col(2 * i + q), LN)],
                                  wdb.at[slot, :, pl.ds(q * LN, LN)], dsem.at[slot]).start()

    def d_wait(slot):
        pltpu.make_async_copy(wd_ref.at[layer, :, pl.ds(0, 2 * LN)], wdb.at[slot], dsem.at[slot]).wait()

    for s in range(NSLOT):
        w_start(jnp.int32(s))
    for k in range(KP):
        h_in(0, k).wait()
    pl.semaphore_wait(barrier, 3)
    for k in range(KP):
        Gather(hloc, 0).send(k)
    for k in range(KP):
        h_in(1, k).wait()

    def zero(j, c):
        acc[j] = jnp.zeros(acc.shape[1:], acc.dtype)
        return c

    lax.fori_loop(0, 2 * FP, zero, 0)
    for s in range(ND):
        d_start(jnp.int32(s))

    class Scatter:
        def __init__(self, half):
            self.half = half

        def copy(self, i, k, piece, part, dst, dev):
            h = self.half
            return rcopy(PS.at[h, piece, rows_of(0, part), :], dst, rss.at[h, i, k], rsr.at[h, i, k], dev)

        def opA(self, k):
            return self.copy(0, k, k, 0, RA.at[self.half, k], up)

        def opB(self, k):
            return self.copy(1, k, k, 1, RB.at[self.half, k], dn)

        def upB(self, k):
            return self.copy(2, k, KP + k, 1, RD.at[self.half, k, rows_of(0, 1), :], up)

        def dnA(self, k):
            return self.copy(3, k, 2 * KP + k, 0, RU.at[self.half, k, rows_of(0, 0), :], dn)

        def upA(self, k):
            return self.copy(4, k, KP + k, 0, RD.at[self.half, k, rows_of(0, 0), :], up)

        def dnB(self, k):
            return self.copy(5, k, 2 * KP + k, 1, RU.at[self.half, k, rows_of(0, 1), :], dn)

        def send(self, p):
            c = p // KP
            k = lax.rem(p, KP)

            @pl.when(c == 0)
            def _():
                self.opA(k).start()
                self.opB(k).start()

            @pl.when(c == 1)
            def _():
                self.upB(k).start()

            @pl.when(c == 2)
            def _():
                self.dnA(k).start()

        def add(self, k, c):
            h = self.half
            self.opA(k).wait_recv()
            PS[h, KP + k, 0:qn, :] += RA[h, k]
            self.upA(k).start()
            self.opB(k).wait_recv()
            PS[h, 2 * KP + k, qn:hn, :] += RB[h, k]
            self.dnB(k).start()
            return c

        def total(self, k, c):
            h = self.half
            for cp in (self.upB, self.dnA, self.upA, self.dnB):
                cp(k).wait_recv()
            s = PS[h, 3 * KP + k] + RD[h, k] + RU[h, k]
            rows = rows_of(h * hn)
            v = xm[rows, pl.ds(pl.multiple_of(k * LN, LN), LN)] + s.astype(jnp.bfloat16)
            XF[rows, pl.ds(pl.multiple_of(t * dt + k * LN, LN), LN)] = v
            Gather(xloc, h).send(k)
            return c

        def near(self, k, c):
            Gather(xloc, self.half).wait('up', k)
            Gather(xloc, self.half).wait('dn', k)
            return c

        def far(self, k, c):
            Gather(xloc, self.half).wait('op', k)
            return c

        def sent(self, k, c):
            Gather(xloc, self.half).sent(k)
            for cp in (self.opA, self.opB, self.upB, self.dnA, self.upA, self.dnB):
                cp(k).wait_send()
            return c

    first, second = Scatter(0), Scatter(1)

    def each(fn):
        lax.fori_loop(0, KP, fn, 0)

    later = [(0, min(2 * g, SUB - 1), (lambda k: lambda: Gather(hloc, 1).send(k))(k)) for k, g in
             zip(range(KP), (2, 3, 3, 4, 4, 5, 6))]
    later += [(1, 0, xin.wait), (1, 1, lambda: each(first.add)), (1, SUB - 2, lambda: each(first.total))]

    def half_step(half, carry):
        gh = Gather(hloc, half)
        rsh = Scatter(half)

        def gu_step(i, c):
            j = i // 2
            gi = half * SUB + i
            slot = lax.rem(gi, NSLOT)
            for jj in range(NG):
                @pl.when(i == 2 * jj)
                def _():
                    for kind, k in order[4 * jj:4 * jj + 4]:
                        gh.wait(kind, k)
            for hh, at, fn in later:
                @pl.when(jnp.logical_and(half == hh, i == at))
                def _():
                    fn()
            w_wait(slot)
            base = lax.rem(i, 2) * FP
            for f in range(0, FP, 4):
                m = min(4, FP - f)
                r = mm(H[half, j], ring[slot, :, f * LN:(f + m) * LN])
                for q in range(m):
                    acc[base + f + q] += r[:, q * LN:(q + 1) * LN]

            @pl.when(gi + NSLOT < 2 * SUB)
            def _():
                w_start(gi + NSLOT)
            return c

        lax.fori_loop(0, SUB, gu_step, 0)

        def silu(f, c):
            a = acc[f].astype(jnp.bfloat16).astype(jnp.float32)
            b = acc[FP + f].astype(jnp.bfloat16).astype(jnp.float32)
            U[:, pl.ds(pl.multiple_of(f * LN, LN), LN)] = (a * (1.0 / (1.0 + jnp.exp(-a))) * b).astype(jnp.bfloat16)
            acc[f] = jnp.zeros(acc.shape[1:], acc.dtype)
            acc[FP + f] = jnp.zeros(acc.shape[1:], acc.dtype)
            return c

        lax.fori_loop(0, FP, silu, 0)
        for k in range(KP):
            gh.sent(k)

        def tile(i, c):
            gi = half * TL + i
            slot = lax.rem(gi, ND)

            @pl.when(jnp.logical_and(half == 1, i == min(4, TL - 1)))
            def _():
                each(first.near)

            d_wait(slot)

            @pl.when(i > 0)
            def _():
                rsh.send(2 * i - 2)
                rsh.send(2 * i - 1)

            r = mm(U[...], wdb[slot])
            for q in range(2):
                PS[half, 2 * i + q] = r[:, q * LN:(q + 1) * LN]

            @pl.when(gi + ND < 2 * TL)
            def _():
                d_start(gi + ND)
            return c

        lax.fori_loop(0, TL, tile, 0)
        return carry

    lax.fori_loop(0, 2, half_step, 0)
    each(second.add)
    each(first.far)

    def out(half):
        rows = pl.ds(half * hn, hn)
        return pltpu.make_async_copy(XF.at[rows, :], out_ref.at[rows, :], lsem.at[half])

    out(0).start()
    each(second.total)
    each(second.near)
    each(second.far)
    out(1).start()
    each(first.sent)
    each(second.sent)
    out(0).wait()
    out(1).wait()


def mlp(T, layer, h, x, wg, wu, wd, cid):
    n, dt = x.shape
    F = wg.shape[2]
    d = dt * T
    KP = dt // LN
    FP = F // LN
    hn = n // 2
    NG = T * KP // 4
    f32, bf = jnp.float32, jnp.bfloat16
    anyspec = pl.BlockSpec(memory_space=pltpu.HBM)
    D = pltpu.SemaphoreType.DMA
    return pl.pallas_call(
        functools.partial(mlp_kernel, T, layer),
        out_shape=jax.ShapeDtypeStruct((n, d), bf),
        in_specs=[anyspec] * 5,
        out_specs=anyspec,
        scratch_shapes=[
            pltpu.VMEM((2 * FP, hn, LN), f32),
            pltpu.VMEM((2, T * KP, hn, LN), f32),
            pltpu.VMEM((3, 4 * LN, F), bf),
            pltpu.VMEM((2, NG, hn, 4 * LN), bf),
            pltpu.VMEM((hn, F), bf),
            pltpu.VMEM((3, F, 2 * LN), bf),
            pltpu.VMEM((2, KP, hn // 2, LN), f32),
            pltpu.VMEM((2, KP, hn // 2, LN), f32),
            pltpu.VMEM((2, KP, hn, LN), f32),
            pltpu.VMEM((2, KP, hn, LN), f32),
            pltpu.VMEM((n, d), bf),
            pltpu.VMEM((n, dt), bf),
            D((2, 4, KP)), D((2, 4, KP)), D((2, 6, KP)), D((2, 6, KP)), D((3,)), D((3,)), D((3,)),
        ],
        compiler_params=pltpu.CompilerParams(vmem_limit_bytes=VMEM_LIMIT, collective_id=cid, has_side_effects=True),
        name="mlp",
    )(h, x, wg, wu, wd)


def emit_kernel(x_ref, *refs):
    *kv_in, xo_ref, ko_ref, vo_ref, xb, kvb, xsem, ksem = refs
    layers = len(kv_in) // 2
    parts = xsem.shape[1]
    rows = x_ref.shape[0] // parts

    def x_copy(i, out):
        here = pl.ds(i * rows, rows)
        a, b = (xb, xo_ref) if out else (x_ref, xb)
        return pltpu.make_async_copy(a.at[here, :], b.at[here, :], xsem.at[int(out), i])

    def kv_copy(i, out):
        a, b = (kvb.at[i], (ko_ref, vo_ref)[i // layers].at[i % layers]) if out else (kv_in[i], kvb.at[i])
        return pltpu.make_async_copy(a, b, ksem.at[int(out), i])

    jobs = [(kv_copy, i) for i in range(len(kv_in))] + [(x_copy, i) for i in range(parts)]
    for fn, i in jobs:
        fn(i, False).start()
    for fn, i in jobs:
        fn(i, False).wait()
        fn(i, True).start()
    for fn, i in jobs:
        fn(i, True).wait()


def emit(x, ks, vs):
    n, dh = ks[0].shape
    parts = 8
    hbm = pl.BlockSpec(memory_space=pltpu.HBM)
    stack = jax.ShapeDtypeStruct((len(ks), n, dh), x.dtype)
    D = pltpu.SemaphoreType.DMA
    return pl.pallas_call(
        emit_kernel,
        out_shape=[jax.ShapeDtypeStruct(x.shape, x.dtype), stack, stack],
        in_specs=[hbm] * (1 + len(ks) + len(vs)),
        out_specs=[hbm] * 3,
        scratch_shapes=[pltpu.VMEM(x.shape, x.dtype), pltpu.VMEM((len(ks) + len(vs), n, dh), x.dtype),
                        D((2, parts)), D((2, len(ks) + len(vs)))],
        compiler_params=pltpu.CompilerParams(vmem_limit_bytes=VMEM_LIMIT),
        name="emit",
    )(x, *ks, *vs)


def solution(mesh):
    sp = mesh.shape['sp']
    tp = mesh.shape['tp']
    row = ('dp', 'sp')
    kv_spec = P(None, row, 'tp', None)
    col = P(None, None, 'tp')
    rowsplit = P(None, 'tp', None)

    def body(x, pos, k_hist, v_hist, wq, wk, wv, wo, wg, wu, wd, g1, g2):
        n, d = x.shape
        layers, hc, kvl, dh = k_hist.shape
        kh, vh = k_hist.reshape(layers, hc, dh), v_hist.reshape(layers, hc, dh)
        lane = jnp.arange(dh)
        inv = ROPE_THETA ** (-((lane % (dh // 2)).astype(jnp.float32) * (2.0 / dh)))
        ang = pos.astype(jnp.float32)[:, None] * inv
        cos = jnp.cos(ang)
        sin = jnp.sin(ang) * jnp.where(lane < dh // 2, -1.0, 1.0)
        ks, vs = [], []
        for l in range(layers):
            h, xm, k, v = attention(tp, sp, l, x, cos, sin, kh, vh, wq, wk, wv, wo, g1, g2, 2 * l)
            ks.append(k)
            vs.append(v)
            x = mlp(tp, l, h, xm, wg, wu, wd, 2 * l + 1)
        x, k, v = emit(x, ks, vs)
        return x, k.reshape(layers, n, kvl, dh), v.reshape(layers, n, kvl, dh)

    in_specs = (P(row, None), P(row), kv_spec, kv_spec, col, col, col, rowsplit, col, col, rowsplit, P(), P())
    out_specs = (P(row, None), kv_spec, kv_spec)
    return jax.shard_map(body, mesh=mesh, in_specs=in_specs, out_specs=out_specs, check_vma=False)
```
